32 devices in a mesh: grp: 2 (over y), ep: 4 (over z), tp: 2 (over x), mb: 2 (over core).
Axes of the slice: x: 2, y: 2, z: 4, core: 2. Of those that a mesh axis runs over, the one named last changes fastest.
Arguments:
- hidden: bfloat16 [256, 3584], P(('grp', 'ep', 'mb'), 'tp'), parts along dimension 0, may hold values from -12 to 12
- moe_gain: float32 [3584], P('tp'), may hold values from 0.1 to 1.9
- expert_ids: int32 [256, 8], P(('grp', 'ep', 'mb')), parts along dimension 0, may hold values from 0 to 7, as said below
- slots: int32 [256, 8], P(('grp', 'ep', 'mb')), parts along dimension 0, may hold values from 0 to 15, as said below
- affinity: float32 [256, 8], P(('grp', 'ep', 'mb')), parts along dimension 0, may hold values from 0.05 to 1
- w_gate: bfloat16 [8, 3584, 1024], P(('ep', 'mb'), None, 'tp'), may hold values from -0.09375 to 0.09375
- w_up: bfloat16 [8, 3584, 1024], P(('ep', 'mb'), None, 'tp'), may hold values from -0.09375 to 0.09375
- w_down: bfloat16 [8, 1024, 3584], P(('ep', 'mb'), 'tp'), may hold values from -0.1875 to 0.1875
- attn_gain: float32 [3584], P('tp'), may hold values from 0.1 to 1.9
- w_dkv: bfloat16 [3584, 576], P('tp'), may hold values from -0.09375 to 0.09375
- kv_gain: float32 [512], replicated, may hold values from 0.1 to 1.9
- queries: bfloat16 [256, 64, 576], P(('grp', 'ep', 'mb'), 'tp'), parts along dimension 0, may hold values from -36 to 36
- cache: bfloat16 [256, 128, 576], P(('grp', 'ep', 'mb'), 'tp'), parts along dimension 0, may hold values from -4 to 4
- lengths: int32 [256], P(('grp', 'ep', 'mb')), parts along dimension 0, may hold values from 2 to 128
Outputs:
- next_hidden: bfloat16 [256, 3584], P(('grp', 'ep', 'mb'), 'tp'), parts along dimension 0
- latent_out: bfloat16 [256, 64, 512], P(('grp', 'ep', 'mb'), 'tp'), parts along dimension 0
The draws below stay inside these ranges and needn't reach their ends.
There are 2 independent parts, one for each index of `grp`. The reference program is written for one: setup_inputs(seed, part) draws one part's arguments, and reference() takes and returns one part's arrays. A program takes and returns all parts, laid end to end along the dimension named above; an argument that names none is the same for every part. Nothing has to cross between parts.
Inputs may be any that keep to these rules, and one draw needn't show every extreme that they name: `expert_ids`: each row names 8 different experts; in every draw some expert is named by every token. slots[t, k] is the rank of the choice (t, k) among the choices of the same expert made by the 16 tokens of one device; these ranks are distinct and run from 0 upward. A choice whose slot is 8 or more is dropped.
All inputs are finite; a program needn't handle non-finite values.
Results may differ from the reference program's by a relative error of at most 0.017.
Values may be sent and summed in bfloat16 or wider, within the bound.
A program may use at most 128 MiB of HBM per device.

```python
import math
import jax
import jax.numpy as jnp
from jax import lax

D = 3584
H = 1024
HEADS = 64
LAT = 512
KVC = 576
TOP = 8
TOK_DEV = 16
KV = 128
CAP = 8
EXPERTS = 8
TOKENS = 128
N_TP = 2


def routing(key):
    base_key = jax.random.fold_in(key, 7)
    hot_expert = jax.random.randint(jax.random.fold_in(base_key, 1), (), 0, EXPERTS)
    expert_iota = jnp.arange(EXPERTS, dtype=jnp.int32)
    biases = jax.random.randint(jax.random.fold_in(base_key, 2), (EXPERTS,), 0, 4 * EXPERTS)
    biases = jnp.where(expert_iota == hot_expert, 16 * EXPERTS, biases)
    noise_int = jax.random.randint(jax.random.fold_in(base_key, 3), (TOKENS, EXPERTS), 0, 6 * EXPERTS)
    scores = (noise_int + biases[None, :]) * EXPERTS + expert_iota[None, :]
    chosen = lax.top_k(scores, TOP)[1].astype(jnp.int32)
    priority = jax.random.randint(jax.random.fold_in(base_key, 4), (TOKENS, TOP), 0, 4096) * (TOKENS * TOP)
    priority = priority + jnp.arange(TOKENS * TOP, dtype=jnp.int32).reshape(TOKENS, TOP)
    blocks = TOKENS // TOK_DEV
    block_ids = chosen.reshape(blocks, TOK_DEV * TOP)
    block_prio = priority.reshape(blocks, TOK_DEV * TOP)
    same_expert = block_ids[:, :, None] == block_ids[:, None, :]
    earlier = block_prio[:, None, :] < block_prio[:, :, None]
    ranks = jnp.sum((same_expert & earlier).astype(jnp.int32), -1)
    return (chosen, ranks.reshape(TOKENS, TOP).astype(jnp.int32))


def draw_expert_ids(key, part):
    return routing(key)[0]


def draw_slots(key, part):
    return routing(key)[1]


def cache_normal(key):
    return jnp.clip(jax.random.normal(jax.random.fold_in(key, 31), (TOKENS, KV, KVC), jnp.float32), -4.0, 4.0)


def draw_cache(key, part):
    values = cache_normal(key)
    return values.astype(jnp.bfloat16)


def draw_queries(key, part):
    values = jnp.clip(jax.random.normal(jax.random.fold_in(key, 34), (TOKENS, HEADS, KVC), jnp.float32), -4.0, 4.0)
    return values.astype(jnp.bfloat16)


def draw_hidden(key, part):
    column_scale = 0.6 + 1.2 * jnp.arange(D, dtype=jnp.float32) / D
    values = jnp.clip(jax.random.normal(jax.random.fold_in(key, 44), (TOKENS, D), jnp.float32), -4.0, 4.0) * column_scale[None, :]
    return jnp.clip(values, -12.0, 12.0).astype(jnp.bfloat16)


def set_ends(result, rng, smallest, top_value):
    dims = result.shape
    place = [jax.random.randint(jax.random.fold_in(rng, axis), (), 0, dims[axis]) for axis in range(len(dims))]
    result = result.at[tuple(place)].set(smallest)
    longest = dims.index(max(dims))
    place[longest] = (place[longest] + 1) % dims[longest]
    return result.at[tuple(place)].set(top_value)


def block_levels(key, shape, cuts, smallest, largest):
    level = 1.0
    for dim, parts in cuts:
        draws = jax.random.uniform(jax.random.fold_in(jax.random.fold_in(key, 6), dim), (parts,), jnp.float32, smallest / len(cuts), largest / len(cuts))
        level = level * jnp.repeat(jnp.exp(draws), shape[dim] // parts).reshape((-1,) + (1,) * (len(shape) - 1 - dim))
    return level


def centred(own_key, dims, spread, limit, cuts=(), kind=jnp.bfloat16):
    loudness = block_levels(own_key, dims, cuts, -0.22, 0.18) if cuts else 1.0
    array = jax.random.normal(own_key, dims, jnp.float32) * spread * loudness
    return jnp.minimum(jnp.maximum(array, -limit), limit).astype(kind)


def setup_inputs(seed: int = 0, part: int = 0) -> dict:
    splits = jax.random.split(jax.random.key(seed), 15)
    part_keys = jax.random.split(jax.random.fold_in(splits[14], part), 15)
    hidden = draw_hidden(jax.random.fold_in(jax.random.fold_in(splits[14], part), 71), part)
    moe_gain = jnp.clip(1.0 + 0.18 * jax.random.normal(splits[1], (D,), jnp.float32), 0.1, 1.9)
    expert_ids = draw_expert_ids(jax.random.fold_in(jax.random.fold_in(splits[14], part), 71), part)
    slots = draw_slots(jax.random.fold_in(jax.random.fold_in(splits[14], part), 71), part)
    affinity = jnp.clip(jnp.exp(math.log(1.0) - 2.9957323 * jax.random.uniform(part_keys[4], (TOKENS, TOP), jnp.float32) ** block_levels(part_keys[4], (TOKENS, TOP), ((0, 8),), -0.2, 0.2)), 0.05, 1.0)
    w_gate = centred(splits[5], (EXPERTS, D, H), D ** -0.5, 0.09375, ((0, 8), (2, 2)))
    w_up = centred(splits[6], (EXPERTS, D, H), D ** -0.5, 0.09375, ((0, 8), (2, 2)))
    w_down = centred(splits[7], (EXPERTS, H, D), H ** -0.5, 0.1875, ((0, 8), (1, 2)))
    attn_gain = jnp.clip(1.0 + 0.18 * jax.random.normal(splits[8], (D,), jnp.float32), 0.1, 1.9)
    w_dkv = centred(splits[9], (D, KVC), D ** -0.5, 0.09375, ((0, 2),))
    kv_gain = jnp.clip(1.0 + 0.18 * jax.random.normal(splits[10], (LAT,), jnp.float32), 0.1, 1.9)
    queries = draw_queries(jax.random.fold_in(jax.random.fold_in(splits[14], part), 71), part)
    cache = draw_cache(jax.random.fold_in(jax.random.fold_in(splits[14], part), 71), part)
    lengths = set_ends(jax.random.randint(part_keys[13], (TOKENS,), 2, KV + 1), jax.random.fold_in(part_keys[13], 1), 2, KV).astype(jnp.int32)
    return dict(hidden=hidden, moe_gain=moe_gain, expert_ids=expert_ids, slots=slots, affinity=affinity, w_gate=w_gate, w_up=w_up, w_down=w_down, attn_gain=attn_gain, w_dkv=w_dkv, kv_gain=kv_gain, queries=queries, cache=cache, lengths=lengths)


epsilon = 1e-06
route_scale = 2.5
score_scale = 192.0 ** (-0.5)

def root_norm(values, gain):
    return values * lax.rsqrt(lax.optimization_barrier(jnp.mean(values * values, -1, keepdims=True)) + epsilon) * gain

def rope_rotate(rope_part, position):
    half_rope = rope_part.shape[-1] // 2
    inv_freq = 10000.0 ** (-jnp.arange(half_rope, dtype=jnp.float32) / half_rope)
    angles = position[:, None] * inv_freq[None, :]
    cos_table = jnp.cos(angles)
    sin_table = jnp.sin(angles)
    first_half = rope_part[:, :half_rope]
    second_half = rope_part[:, half_rope:]
    return jnp.concatenate([first_half * cos_table - second_half * sin_table, first_half * sin_table + second_half * cos_table], 1)

def reference(hidden, moe_gain, expert_ids, slots, affinity, w_gate, w_up, w_down, attn_gain, w_dkv, kv_gain, queries, cache, lengths):
    hidden_wide = hidden.astype(jnp.float32)
    normed = root_norm(hidden_wide, moe_gain).astype(jnp.bfloat16)
    kept_rows = slots < CAP
    weight = route_scale * affinity / lax.optimization_barrier(jnp.sum(affinity, -1, keepdims=True)) * kept_rows.astype(jnp.float32)
    source = (jnp.arange(TOKENS, dtype=jnp.int32) // TOK_DEV)[:, None]
    flat_slot = ((expert_ids * EXPERTS + source) * CAP + jnp.minimum(slots, CAP - 1)).astype(jnp.int32)
    slot_count = EXPERTS * EXPERTS * CAP
    token_iota = jnp.broadcast_to(jnp.arange(TOKENS, dtype=jnp.int32)[:, None], (TOKENS, TOP))
    target = jnp.where(kept_rows, flat_slot, slot_count).astype(jnp.int32)
    token_of = jnp.full((slot_count,), TOKENS, jnp.int32).at[target].set(token_iota, mode='drop')
    padded = jnp.concatenate([normed, jnp.zeros((1, D), jnp.bfloat16)], 0)
    expert_rows = padded[token_of].reshape(EXPERTS, EXPERTS * CAP, D)

    def expert_block(operands):
        rows_in, gate_weight, up_weight, down_weight = operands
        gate_act = jnp.dot(rows_in, gate_weight, preferred_element_type=jnp.float32)
        up_act = jnp.dot(rows_in, up_weight, preferred_element_type=jnp.float32)
        units = (jax.nn.silu(gate_act) * up_act).astype(jnp.bfloat16)
        grouped = units.reshape(EXPERTS * CAP, N_TP, H // N_TP).astype(jnp.float32)
        down_groups = down_weight.reshape(N_TP, H // N_TP, D).astype(jnp.float32)
        partials = jnp.einsum('rth,thd->trd', grouped, down_groups)
        return lax.optimization_barrier(jnp.sum(partials.astype(jnp.bfloat16).astype(jnp.float32), 0))
    expert_out = lax.map(expert_block, (expert_rows, w_gate, w_up, w_down)).reshape(slot_count, D)
    picked = expert_out[jnp.where(kept_rows, flat_slot, 0).astype(jnp.int32)]
    moe_out = lax.optimization_barrier(jnp.sum(picked * weight[:, :, None], 1))
    next_hidden = (hidden_wide + moe_out).astype(jnp.bfloat16)
    normed_attn = root_norm(next_hidden.astype(jnp.float32), attn_gain).astype(jnp.bfloat16)
    down_kv = jnp.dot(normed_attn, w_dkv, preferred_element_type=jnp.float32)
    latent_part = root_norm(down_kv[:, :LAT], kv_gain)
    rope_part = rope_rotate(down_kv[:, LAT:], lengths.astype(jnp.float32))
    new_key = jnp.concatenate([latent_part, rope_part], 1).astype(jnp.bfloat16)
    query_wide = queries.astype(jnp.float32)
    cache_wide = cache.astype(jnp.float32)
    scores = jnp.einsum('bhc,bjc->bhj', query_wide, cache_wide) * score_scale
    live_mask = (jnp.arange(KV, dtype=jnp.int32)[None, :] < lengths[:, None])[:, None, :]
    scores = jnp.where(live_mask, scores, -1e+30)
    own_score = jnp.einsum('bhc,bc->bh', query_wide, new_key.astype(jnp.float32)) * score_scale
    peak_all = jnp.maximum(lax.optimization_barrier(jnp.max(scores, -1)), own_score)
    prob_live = jnp.where(live_mask, jnp.exp(scores - peak_all[:, :, None]), 0.0)
    own_prob = jnp.exp(own_score - peak_all)
    mass_total = lax.optimization_barrier(jnp.sum(prob_live, -1)) + own_prob
    numerator = jnp.einsum('bhj,bjc->bhc', prob_live.astype(jnp.bfloat16).astype(jnp.float32), cache_wide[:, :, :LAT])
    numerator = numerator + own_prob.astype(jnp.bfloat16).astype(jnp.float32)[:, :, None] * new_key[:, None, :LAT].astype(jnp.float32)
    latent_out = (numerator / mass_total[:, :, None]).astype(jnp.bfloat16)
    return (next_hidden, latent_out)
```

```python
import functools

import jax
import jax.numpy as jnp
from jax import lax
from jax.experimental import pallas as pl
from jax.experimental.pallas import tpu as pltpu
from jax.sharding import PartitionSpec as P

CAP = 8
GROUPS = 4
epsilon = 1e-06
route_scale = 2.5
score_scale = 192.0 ** (-0.5)
MESH = pl.DeviceIdType.MESH
F32 = jnp.float32
BF16 = jnp.bfloat16


def up(value, step):
    return -(-value // step) * step


def kernel(
    n_tp,
    n_ep,
    n_mb,
    hidden,
    moe_gain,
    ids,
    slots,
    affinity,
    w_gate,
    w_up,
    w_down,
    attn_gain,
    w_dkv,
    kv_gain,
    queries,
    cache,
    lengths,
    next_out,
    latent_out,
    hid_all,
    gain_all,
    send,
    arrived,
    wg,
    wu,
    wd,
    wk,
    ret_send,
    ret,
    tsum,
    rs_send,
    rs_recv,
    key_send,
    key_recv,
    q_buf,
    kv_buf,
    acc,
    peaks,
    masses,
    keys,
    load_sem,
    kv_load_sem,
    hid_ssem,
    hid_rsem,
    gain_ssem,
    gain_rsem,
    kv_ssem,
    kv_rsem,
    row_ssem,
    row_rsem,
    ret_ssem,
    ret_rsem,
    rs_ssem,
    rs_rsem,
    key_ssem,
    key_rsem,
):
    experts = n_ep * n_mb
    tokens, d_loc = hidden.shape
    d_all = d_loc * n_tp
    lat = kv_gain.shape[1]
    kvc = cache.shape[2]
    per_group = tokens // GROUPS
    tp = lax.axis_index("tp")
    me = lax.axis_index("ep") * n_mb + lax.axis_index("mb")

    def tp_id(step):
        return lax.rem(tp + step, n_tp)

    def ex_id(step):
        return lax.rem(me + step, experts)

    def ex_dev(index):
        return {"ep": index // n_mb, "mb": lax.rem(index, n_mb)}

    local = [
        pltpu.make_async_copy(hidden, hid_all.at[tp], load_sem.at[0]),
        pltpu.make_async_copy(queries, q_buf, load_sem.at[1]),
        pltpu.make_async_copy(w_gate.at[0], wg, load_sem.at[2]),
        pltpu.make_async_copy(w_up.at[0], wu, load_sem.at[3]),
        pltpu.make_async_copy(w_down.at[0], wd, load_sem.at[4]),
        pltpu.make_async_copy(w_dkv, wk, load_sem.at[5]),
    ]
    kv_load = pltpu.make_async_copy(cache, kv_buf.at[:, tp], kv_load_sem)
    local[0].start()
    gain_all[tp] = moe_gain[...].reshape(1, d_loc)

    barrier = pltpu.get_barrier_semaphore()
    for step in range(1, n_tp):
        pl.semaphore_signal(barrier, inc=1, device_id={"tp": tp_id(step)}, device_id_type=MESH)
    for step in range(1, experts):
        pl.semaphore_signal(barrier, inc=1, device_id=ex_dev(ex_id(step)), device_id_type=MESH)
    kept = slots[...] < CAP
    aff = affinity[...]
    weight = route_scale * aff / jnp.sum(aff, 0, keepdims=True) * kept.astype(F32)
    target = jnp.where(kept, ids[...] * CAP + slots[...], -1)
    rows = experts * CAP
    iota = lax.broadcasted_iota(jnp.int32, (rows, tokens), 0)
    dispatch = jnp.zeros((rows, tokens), F32)
    combine = jnp.zeros((rows, tokens), F32)
    for k in range(ids.shape[0]):
        match = target[k : k + 1] == iota
        dispatch = jnp.where(match, 1.0, dispatch)
        combine = jnp.where(match, weight[k : k + 1], combine)
    dispatch = dispatch.astype(BF16)
    combine = combine.T
    high = combine.astype(BF16)
    rest = combine - high.astype(F32)
    mid = rest.astype(BF16)
    low = (rest - mid.astype(F32)).astype(BF16)
    combine3 = jnp.concatenate([high, mid, low], 0)

    def pick(block):
        picked = jnp.dot(dispatch, hid_all[block], preferred_element_type=F32)
        send[:, block] = picked.reshape(experts, CAP, d_loc).astype(BF16)

    def ship(block, turn):
        for step in range(1, experts):
            peer = ex_id(step)
            copy = pltpu.make_async_remote_copy(
                src_ref=send.at[peer, block],
                dst_ref=arrived.at[me, block],
                send_sem=row_ssem.at[step, turn],
                recv_sem=row_rsem.at[me, block],
                device_id=ex_dev(peer),
                device_id_type=MESH,
            )
            copy.start()
            sends.append(copy)
        arrived[me, block] = send[me, block]

    local[0].wait()
    pick(tp)
    pl.semaphore_wait(barrier, n_tp - 1 + experts - 1)

    def tp_copy(src, dst, ssem, rsem, step):
        return pltpu.make_async_remote_copy(
            src_ref=src,
            dst_ref=dst,
            send_sem=ssem,
            recv_sem=rsem,
            device_id={"tp": tp_id(step)},
            device_id_type=MESH,
        )

    def arrival(dst, rsem):
        return pltpu.make_async_copy(dst, dst, rsem)

    sends = []
    for step in range(1, n_tp):
        for src, dst, ssem, rsem in (
            (hidden, hid_all, hid_ssem, hid_rsem),
            (gain_all.at[tp], gain_all, gain_ssem, gain_rsem),
        ):
            copy = tp_copy(src, dst.at[tp], ssem.at[step], rsem.at[tp], step)
            copy.start()
            sends.append(copy)
    ship(tp, 0)
    for g in range(GROUPS):
        span = pl.ds(g * per_group, per_group)
        for step in range(1, n_tp):
            copy = tp_copy(
                cache.at[span], kv_buf.at[span, tp], kv_ssem.at[step, g], kv_rsem.at[tp, g], step
            )
            copy.start()
            sends.append(copy)
    for copy in local[1:4]:
        copy.start()
    kv_load.start()
    for copy in local[4:]:
        copy.start()

    for step in range(1, n_tp):
        arrival(hid_all.at[tp_id(step)], hid_rsem.at[tp_id(step)]).wait()
        arrival(gain_all.at[tp_id(step)], gain_rsem.at[tp_id(step)]).wait()
    for turn in range(1, n_tp):
        pick(tp_id(turn))
        ship(tp_id(turn), turn)

    local[1].wait()
    kv_load.wait()
    heads = queries.shape[1]
    span_len = cache.shape[1]
    total_len = n_tp * span_len

    def attend(g):
        span = pl.ds(g * per_group, per_group)
        for step in range(1, n_tp):
            arrival(kv_buf.at[span, tp_id(step)], kv_rsem.at[tp_id(step), g]).wait()

        def body(i, carry):
            t = g * per_group + i
            block = kv_buf[t].reshape(total_len, kvc)
            scores = (
                lax.dot_general(
                    q_buf[t], block, (((1,), (1,)), ((), ())), preferred_element_type=F32
                )
                * score_scale
            )
            live = lax.broadcasted_iota(jnp.int32, (heads, total_len), 1) < lengths[t]
            scores = jnp.where(live, scores, -1e30)
            peak = jnp.max(scores, -1, keepdims=True)
            prob = jnp.where(live, jnp.exp(scores - peak), 0.0)
            mass = jnp.sum(prob, -1, keepdims=True)
            acc[t] = jnp.dot(prob.astype(BF16), block[:, :lat], preferred_element_type=F32)
            peaks[t] = jnp.broadcast_to(peak, (heads, 128))
            masses[t] = jnp.broadcast_to(mass, (heads, 128))
            return carry

        lax.fori_loop(0, per_group, body, 0)

    local[2].wait()
    local[3].wait()
    gate = jnp.zeros((rows, wg.shape[1]), F32)
    upper = jnp.zeros((rows, wg.shape[1]), F32)
    square = jnp.zeros((rows, 1), F32)
    for turn in range(n_tp):
        b = tp_id(turn)
        for step in range(1, experts):
            peer = ex_id(step)
            arrival(arrived.at[peer, b], row_rsem.at[peer, b]).wait()
        wide = arrived[:, b].astype(F32).reshape(rows, d_loc)
        square = square + jnp.sum(wide * wide, -1, keepdims=True)
        block = (wide * gain_all[b]).astype(BF16)
        deep = pl.ds(pl.multiple_of(b * d_loc, d_loc & -d_loc), d_loc)
        gate = gate + jnp.dot(block, wg[deep], preferred_element_type=F32)
        upper = upper + jnp.dot(block, wu[deep], preferred_element_type=F32)
    scale = lax.rsqrt(square / d_all + epsilon)
    gate = gate * scale
    upper = upper * scale
    units = (gate / (1.0 + jnp.exp(-gate)) * upper).astype(BF16)
    local[4].wait()
    width = 512 if d_all % 512 == 0 else 128
    aligned = d_loc % 128 == 0
    if aligned:
        width = next(w for w in (896, 512, 384, 256, 128) if d_loc % w == 0)
        pieces = [
            (pl.multiple_of(tp_id(turn) * d_loc, 128), d_loc) for turn in (*range(1, n_tp), 0)
        ]
    else:
        middle = d_all // width // 2 * width
        pieces = [(0, middle), (middle, d_all - middle)]

    def columns(start, size):
        return pl.ds(pl.multiple_of(start, 128), size)

    for h, (first, size) in enumerate(pieces):
        for c in range(0, size, width):
            part = jnp.dot(units, wd[:, columns(first + c, width)], preferred_element_type=F32)
            ret_send[:, :, columns(first + c, width)] = part.reshape(
                experts, CAP, width
            ).astype(BF16)
        for step in range(1, experts):
            peer = ex_id(step)
            copy = pltpu.make_async_remote_copy(
                src_ref=ret_send.at[peer, :, columns(first, size)],
                dst_ref=ret.at[me, :, columns(first, size)],
                send_sem=ret_ssem.at[step, h],
                recv_sem=ret_rsem.at[me, h],
                device_id=ex_dev(peer),
                device_id_type=MESH,
            )
            copy.start()
            sends.append(copy)
    ret[me] = ret_send[me]

    def exchange(step):
        copy = tp_copy(
            rs_send.at[tp_id(step)], rs_recv.at[tp], rs_ssem.at[step], rs_rsem.at[tp], step
        )
        copy.start()
        sends.append(copy)

    for h, (first, size) in enumerate(pieces):
        for step in range(1, experts):
            peer = ex_id(step)
            arrival(ret.at[peer, :, columns(first, size)], ret_rsem.at[peer, h]).wait()
        for c in range(0, size, width):
            block = ret[:, :, columns(first + c, width)].astype(F32)
            block = block.reshape(rows, width).astype(BF16)
            part = jnp.dot(combine3, block, preferred_element_type=F32)
            part = part[:tokens] + (part[tokens : 2 * tokens] + part[2 * tokens : 3 * tokens])
            if aligned:
                rs_send[tp_id(h + 1), :, c : c + width] = part.astype(BF16)
            else:
                tsum[:, columns(first + c, width)] = part
        if aligned and h < n_tp - 1:
            exchange(h + 1)
        if h == 0:
            for g in range(GROUPS // 2):
                attend(g)
    if not aligned:
        for p in range(n_tp):
            rs_send[p] = tsum[:, p * d_loc : (p + 1) * d_loc].astype(BF16)
        for step in range(1, n_tp):
            exchange(step)
    rs_recv[tp] = rs_send[tp]
    local[5].wait()
    for step in range(1, n_tp):
        arrival(rs_recv.at[tp_id(step)], rs_rsem.at[tp_id(step)]).wait()
    moe = rs_recv[0].astype(F32)
    for p in range(1, n_tp):
        moe = moe + rs_recv[p].astype(F32)
    next_hidden = (hid_all[tp].astype(F32) + moe).astype(BF16)
    next_out[...] = next_hidden
    next_wide = next_hidden.astype(F32)
    square = jnp.sum(next_wide * next_wide, -1, keepdims=True)
    scaled = (next_wide * attn_gain[...].reshape(1, d_loc)).astype(BF16)
    kvp = up(kvc, 128)
    if kvp > kvc:
        key_send[:, kvp - 128 : kvp] = jnp.zeros((tokens, 128), F32)
    key_send[:, :kvc] = lax.dot_general(
        scaled, wk[...], (((1,), (1,)), ((), ())), preferred_element_type=F32
    )
    key_send[:, kvp : kvp + 128] = jnp.broadcast_to(square, (tokens, 128))
    for step in range(1, n_tp):
        copy = tp_copy(key_send, key_recv.at[tp], key_ssem.at[step], key_rsem.at[tp], step)
        copy.start()
        sends.append(copy)
    key_recv[tp] = key_send[...]
    for g in range(GROUPS // 2, GROUPS):
        attend(g)

    half = (kvc - lat) // 2
    lane = lax.broadcasted_iota(jnp.int32, (tokens, 2 * half), 1)
    pair = jnp.where(lane < half, lane, lane - half).astype(F32)
    freq = jnp.exp(pair * (-9.210340371976184 / half))
    row_id = lax.broadcasted_iota(jnp.int32, (tokens, 2 * half), 0)
    place = jnp.zeros((tokens, 2 * half), F32)
    for t in range(tokens):
        place = jnp.where(row_id == t, lengths[t].astype(F32), place)
    angle = place * freq
    cos_table = jnp.cos(angle)
    sin_table = jnp.where(lane < half, -1.0, 1.0) * jnp.sin(angle)

    for step in range(1, n_tp):
        arrival(key_recv.at[tp_id(step)], key_rsem.at[tp_id(step)]).wait()
    total = key_recv[0]
    for p in range(1, n_tp):
        total = total + key_recv[p]
    down = total * lax.rsqrt(total[:, kvp : kvp + 1] / d_all + epsilon)
    latent = down[:, :lat]
    latent = (
        latent
        * lax.rsqrt(jnp.mean(latent * latent, -1, keepdims=True) + epsilon)
        * kv_gain[...]
    )
    rope = down[:, lat:kvc]
    swapped = jnp.concatenate([rope[:, half:], rope[:, :half]], 1)
    rope = rope * cos_table + swapped * sin_table
    keys[:, :lat] = latent.astype(BF16).astype(F32)
    keys[:, lat:kvc] = rope.astype(BF16).astype(F32)

    def finish(t, carry):
        key = keys[pl.ds(t, 1), :]
        own = jnp.sum(q_buf[t].astype(F32) * key, -1, keepdims=True) * score_scale
        peak = peaks[t][:, :1]
        mass = masses[t][:, :1]
        top = jnp.maximum(peak, own)
        factor = jnp.exp(peak - top)
        own_prob = jnp.exp(own - top)
        inverse = 1.0 / (mass * factor + own_prob)
        own_b = own_prob.astype(BF16).astype(F32)
        latent_out[t] = (acc[t] * (factor * inverse) + (own_b * inverse) * key[:, :lat]).astype(
            BF16
        )
        return carry

    lax.fori_loop(0, tokens, finish, 0)
    for copy in sends:
        copy.wait_send()


def solution(mesh):
    n_tp, n_ep, n_mb = mesh.shape["tp"], mesh.shape["ep"], mesh.shape["mb"]
    experts = n_ep * n_mb

    def local(
        hidden,
        moe_gain,
        expert_ids,
        slots,
        affinity,
        w_gate,
        w_up,
        w_down,
        attn_gain,
        w_dkv,
        kv_gain,
        queries,
        cache,
        lengths,
    ):
        tokens, d_loc = hidden.shape
        d_all = d_loc * n_tp
        heads, kvc = queries.shape[1:]
        span = cache.shape[1]
        lat = kv_gain.shape[0]
        hid_dim = w_gate.shape[2]
        wide = up(kvc, 128) + 128
        any_space = pl.BlockSpec(memory_space=pl.ANY)
        vmem = pl.BlockSpec(memory_space=pltpu.VMEM)
        smem = pl.BlockSpec(memory_space=pltpu.SMEM)
        dma = pltpu.SemaphoreType.DMA
        return pl.pallas_call(
            functools.partial(kernel, n_tp, n_ep, n_mb),
            out_shape=(
                pltpu.VMEM((tokens, d_loc), BF16),
                pltpu.VMEM((tokens, heads, lat), BF16),
            ),
            in_specs=[
                any_space,
                vmem,
                vmem,
                vmem,
                vmem,
                any_space,
                any_space,
                any_space,
                vmem,
                any_space,
                vmem,
                any_space,
                any_space,
                smem,
            ],
            out_specs=(vmem, vmem),
            scratch_shapes=[
                pltpu.VMEM((n_tp, tokens, d_loc), BF16),
                pltpu.VMEM((n_tp, 1, d_loc), F32),
                pltpu.VMEM((experts, n_tp, CAP, d_loc), BF16),
                pltpu.VMEM((experts, n_tp, CAP, d_loc), BF16),
                pltpu.VMEM((d_all, hid_dim), BF16),
                pltpu.VMEM((d_all, hid_dim), BF16),
                pltpu.VMEM((hid_dim, d_all), BF16),
                pltpu.VMEM((kvc, d_loc), BF16),
                pltpu.VMEM((experts, CAP, d_all), BF16),
                pltpu.VMEM((experts, CAP, d_all), BF16),
                pltpu.VMEM((tokens, d_all), F32),
                pltpu.VMEM((n_tp, tokens, d_loc), BF16),
                pltpu.VMEM((n_tp, tokens, d_loc), BF16),
                pltpu.VMEM((tokens, wide), F32),
                pltpu.VMEM((n_tp, tokens, wide), F32),
                pltpu.VMEM((tokens, heads, kvc), BF16),
                pltpu.VMEM((tokens, n_tp, span, kvc), BF16),
                pltpu.VMEM((tokens, heads, lat), F32),
                pltpu.VMEM((tokens, heads, 128), F32),
                pltpu.VMEM((tokens, heads, 128), F32),
                pltpu.VMEM((tokens, kvc), F32),
                dma((6,)),
                dma,
                dma((n_tp,)),
                dma((n_tp,)),
                dma((n_tp,)),
                dma((n_tp,)),
                dma((n_tp, GROUPS)),
                dma((n_tp, GROUPS)),
                dma((experts, n_tp)),
                dma((experts, n_tp)),
                dma((experts, max(2, n_tp))),
                dma((experts, max(2, n_tp))),
                dma((n_tp,)),
                dma((n_tp,)),
                dma((n_tp,)),
                dma((n_tp,)),
            ],
            compiler_params=pltpu.CompilerParams(
                collective_id=0, has_side_effects=True, vmem_limit_bytes=60 * 1024 * 1024
            ),
        )(
            hidden,
            moe_gain,
            expert_ids.T,
            slots.T,
            affinity.T,
            w_gate,
            w_up,
            w_down,
            attn_gain,
            w_dkv.T,
            kv_gain[None],
            queries,
            cache,
            lengths,
        )

    return jax.shard_map(
        local,
        mesh=mesh,
        in_specs=(
            P(("grp", "ep", "mb"), "tp"),
            P("tp"),
            P(("grp", "ep", "mb"), None),
            P(("grp", "ep", "mb"), None),
            P(("grp", "ep", "mb"), None),
            P(("ep", "mb"), None, "tp"),
            P(("ep", "mb"), None, "tp"),
            P(("ep", "mb"), "tp", None),
            P("tp"),
            P("tp", None),
            P(),
            P(("grp", "ep", "mb"), "tp", None),
            P(("grp", "ep", "mb"), "tp", None),
            P(("grp", "ep", "mb")),
        ),
        out_specs=(P(("grp", "ep", "mb"), "tp"), P(("grp", "ep", "mb"), "tp", None)),
        check_vma=False,
    )
```

```python
import functools

import jax
import jax.numpy as jnp
from jax import lax
from jax.experimental import pallas as pl
from jax.experimental.pallas import tpu as pltpu
from jax.sharding import PartitionSpec as P

CAP = 8
AHEAD = 3
epsilon = 1e-06
route_scale = 2.5
score_scale = 192.0 ** (-0.5)
STOPS = (2, 5, 10, 13)
MESH = pl.DeviceIdType.MESH
F32 = jnp.float32
BF16 = jnp.bfloat16


def up(value, step):
    return -(-value // step) * step


def split3(value, width):
    high = value.astype(BF16)
    rest = value - high.astype(F32)
    mid = rest.astype(BF16)
    low = (rest - mid.astype(F32)).astype(BF16)
    lane = lax.broadcasted_iota(jnp.int32, (value.shape[0], width), 1)
    parts = jnp.where(lane == 1, mid.astype(F32), jnp.where(lane == 2, low.astype(F32), 0.0))
    return jnp.where(lane == 0, high.astype(F32), parts).astype(BF16)


def kernel(
    n_tp,
    n_ep,
    n_mb,
    hidden,
    moe_gain,
    ids,
    slots,
    affinity,
    w_gate,
    w_up,
    w_down,
    attn_gain,
    w_dkv,
    kv_gain,
    queries,
    cache,
    lengths,
    next_out,
    latent_out,
    hid_all,
    gain_all,
    send,
    arrived,
    wg,
    wu,
    wd,
    wk,
    ret_send,
    ret,
    tsum,
    rs_send,
    rs_recv,
    key_send,
    key_recv,
    q_buf,
    kv_buf,
    acc,
    peaks,
    masses,
    keys,
    old_part,
    own_part,
    load_sem,
    kv_load_sem,
    hid_ssem,
    hid_rsem,
    gain_ssem,
    gain_rsem,
    kv_ssem,
    kv_rsem,
    row_ssem,
    row_rsem,
    ret_ssem,
    ret_rsem,
    rs_ssem,
    rs_rsem,
    key_ssem,
    key_rsem,
):
    experts = n_ep * n_mb
    tokens, d_loc = hidden.shape
    d_all = d_loc * n_tp
    lat = kv_gain.shape[1]
    kvc = cache.shape[2]
    tp = lax.axis_index("tp")
    me = lax.axis_index("ep") * n_mb + lax.axis_index("mb")

    def tp_id(step):
        return lax.rem(tp + step, n_tp)

    def ex_id(step):
        return lax.rem(me + step, experts)

    def ex_dev(index):
        return {"ep": index // n_mb, "mb": lax.rem(index, n_mb)}
    local = [
        pltpu.make_async_copy(hidden, hid_all.at[tp], load_sem.at[0]),
        pltpu.make_async_copy(queries, q_buf, load_sem.at[1]),
        pltpu.make_async_copy(w_gate.at[0], wg, load_sem.at[2]),
        pltpu.make_async_copy(w_up.at[0], wu, load_sem.at[3]),
        pltpu.make_async_copy(w_down.at[0], wd, load_sem.at[4]),
        pltpu.make_async_copy(w_dkv, wk, load_sem.at[5]),
    ]
    kv_load = pltpu.make_async_copy(cache, kv_buf.at[:, tp], kv_load_sem)
    local[0].start()
    kv_load.start()
    gain_all[tp] = moe_gain[...].reshape(1, d_loc)

    barrier = pltpu.get_barrier_semaphore()
    for step in range(1, n_tp):
        pl.semaphore_signal(barrier, inc=1, device_id={"tp": tp_id(step)}, device_id_type=MESH)
    for step in range(1, experts):
        pl.semaphore_signal(barrier, inc=1, device_id=ex_dev(ex_id(step)), device_id_type=MESH)
    kept = slots[...] < CAP
    aff = affinity[...]
    weight = route_scale * aff / jnp.sum(aff, 0, keepdims=True) * kept.astype(F32)
    target = jnp.where(kept, ids[...] * CAP + slots[...], -1)
    rows = experts * CAP
    iota = lax.broadcasted_iota(jnp.int32, (rows, tokens), 0)
    dispatch = jnp.zeros((rows, tokens), F32)
    combine = jnp.zeros((rows, tokens), F32)
    for k in range(ids.shape[0]):
        match = target[k : k + 1] == iota
        dispatch = jnp.where(match, 1.0, dispatch)
        combine = jnp.where(match, weight[k : k + 1], combine)
    dispatch = dispatch.astype(BF16)
    combine = combine.T
    high = combine.astype(BF16)
    rest = combine - high.astype(F32)
    mid = rest.astype(BF16)
    low = (rest - mid.astype(F32)).astype(BF16)
    combine3 = jnp.concatenate([high, mid, low], 0)

    def pick(block):
        picked = jnp.dot(dispatch, hid_all[block], preferred_element_type=F32)
        send[:, block] = picked.reshape(experts, CAP, d_loc).astype(BF16)

    def ship(block, turn):
        for step in range(1, experts):
            peer = ex_id(step)
            copy = pltpu.make_async_remote_copy(
                src_ref=send.at[peer, block],
                dst_ref=arrived.at[me, block],
                send_sem=row_ssem.at[step, turn],
                recv_sem=row_rsem.at[me, block],
                device_id=ex_dev(peer),
                device_id_type=MESH,
            )
            copy.start()
            sends.append(copy)
        arrived[me, block] = send[me, block]
    local[0].wait()
    pick(tp)
    kv_load.wait()
    for copy in local[1:]:
        copy.start()
    pl.semaphore_wait(barrier, n_tp - 1 + experts - 1)

    def tp_copy(src, dst, ssem, rsem, step):
        return pltpu.make_async_remote_copy(
            src_ref=src,
            dst_ref=dst,
            send_sem=ssem,
            recv_sem=rsem,
            device_id={"tp": tp_id(step)},
            device_id_type=MESH,
        )

    def arrival(dst, rsem):
        return pltpu.make_async_copy(dst, dst, rsem)
    sends = []
    for step in range(1, n_tp):
        for src, dst, ssem, rsem in (
            (hid_all.at[tp], hid_all, hid_ssem, hid_rsem),
            (gain_all.at[tp], gain_all, gain_ssem, gain_rsem),
        ):
            copy = tp_copy(src, dst.at[tp], ssem.at[step], rsem.at[tp], step)
            copy.start()
            sends.append(copy)
    ship(tp, 0)

    def cache_copy(t, step):
        return tp_copy(
            kv_buf.at[t, tp], kv_buf.at[t, tp], kv_ssem.at[step, t], kv_rsem.at[tp, t], step
        )

    def feed(t):
        for step in range(1, n_tp):
            cache_copy(t, step).start()

    for t in range(AHEAD):
        feed(t)
    for step in range(1, n_tp):
        arrival(hid_all.at[tp_id(step)], hid_rsem.at[tp_id(step)]).wait()
        arrival(gain_all.at[tp_id(step)], gain_rsem.at[tp_id(step)]).wait()
    for turn in range(1, n_tp):
        pick(tp_id(turn))
        ship(tp_id(turn), turn)

    local[1].wait()
    heads = queries.shape[1]
    span_len = cache.shape[1]
    total_len = n_tp * span_len

    def attend(first, last):
        def body(t, carry):
            for step in range(1, n_tp):
                arrival(kv_buf.at[t, tp_id(step)], kv_rsem.at[tp_id(step), t]).wait()

            @pl.when(t + AHEAD < tokens)
            def _():
                feed(t + AHEAD)

            block = kv_buf[t].reshape(total_len, kvc)
            scores = (
                lax.dot_general(
                    q_buf[t], block, (((1,), (1,)), ((), ())), preferred_element_type=F32
                )
                * score_scale
            )
            live = lax.broadcasted_iota(jnp.int32, (heads, total_len), 1) < lengths[t]
            scores = jnp.where(live, scores, -1e30)
            peak = jnp.max(scores, -1, keepdims=True)
            prob = jnp.where(live, jnp.exp(scores - peak), 0.0)
            mass = jnp.sum(prob, -1, keepdims=True)
            acc[t] = jnp.dot(prob.astype(BF16), block[:, :lat], preferred_element_type=F32)
            peaks[t] = jnp.broadcast_to(peak, (heads, 128))
            masses[t] = jnp.broadcast_to(mass, (heads, 128))
            return carry

        lax.fori_loop(first, last, body, 0)

    stops = [tokens * n // 16 for n in STOPS]
    attend(0, stops[0])
    local[2].wait()
    local[3].wait()
    gate = jnp.zeros((rows, wg.shape[1]), F32)
    upper = jnp.zeros((rows, wg.shape[1]), F32)
    square = jnp.zeros((rows, 1), F32)
    for turn in range(n_tp):
        b = tp_id(turn)
        if turn == n_tp - 1:
            attend(stops[0], stops[1])
        for step in range(1, experts):
            peer = ex_id(step)
            arrival(arrived.at[peer, b], row_rsem.at[peer, b]).wait()
        wide = arrived[:, b].astype(F32).reshape(rows, d_loc)
        square = square + jnp.sum(wide * wide, -1, keepdims=True)
        block = (wide * gain_all[b]).astype(BF16)
        deep = pl.ds(pl.multiple_of(b * d_loc, d_loc & -d_loc), d_loc)
        gate = gate + jnp.dot(block, wg[deep], preferred_element_type=F32)
        upper = upper + jnp.dot(block, wu[deep], preferred_element_type=F32)
    scale = lax.rsqrt(square / d_all + epsilon)
    gate = gate * scale
    upper = upper * scale
    units = (gate / (1.0 + jnp.exp(-gate)) * upper).astype(BF16)
    local[4].wait()
    width = 512 if d_all % 512 == 0 else 128
    aligned = d_loc % 128 == 0
    if aligned:
        width = next(w for w in (896, 512, 384, 256, 128) if d_loc % w == 0)
        pieces = [
            (pl.multiple_of(tp_id(turn) * d_loc, 128), d_loc) for turn in (*range(1, n_tp), 0)
        ]
    else:
        middle = d_all // width // 2 * width
        pieces = [(0, middle), (middle, d_all - middle)]

    def columns(start, size):
        return pl.ds(pl.multiple_of(start, 128), size)

    for h, (first, size) in enumerate(pieces):
        for c in range(0, size, width):
            part = jnp.dot(units, wd[:, columns(first + c, width)], preferred_element_type=F32)
            ret_send[:, :, columns(first + c, width)] = part.reshape(
                experts, CAP, width
            ).astype(BF16)
        for step in range(1, experts):
            peer = ex_id(step)
            copy = pltpu.make_async_remote_copy(
                src_ref=ret_send.at[peer, :, columns(first, size)],
                dst_ref=ret.at[me, :, columns(first, size)],
                send_sem=ret_ssem.at[step, h],
                recv_sem=ret_rsem.at[me, h],
                device_id=ex_dev(peer),
                device_id_type=MESH,
            )
            copy.start()
            sends.append(copy)
    ret[me] = ret_send[me]

    def exchange(step):
        copy = tp_copy(
            rs_send.at[tp_id(step)], rs_recv.at[tp], rs_ssem.at[step], rs_rsem.at[tp], step
        )
        copy.start()
        sends.append(copy)

    for h, (first, size) in enumerate(pieces):
        if h < 2:
            attend(stops[h + 1], stops[h + 2])
        for step in range(1, experts):
            peer = ex_id(step)
            arrival(ret.at[peer, :, columns(first, size)], ret_rsem.at[peer, h]).wait()
        for c in range(0, size, width):
            block = ret[:, :, columns(first + c, width)].astype(F32)
            block = block.reshape(rows, width).astype(BF16)
            part = jnp.dot(combine3, block, preferred_element_type=F32)
            part = part[:tokens] + (part[tokens : 2 * tokens] + part[2 * tokens : 3 * tokens])
            if aligned:
                rs_send[tp_id(h + 1), :, c : c + width] = part.astype(BF16)
            else:
                tsum[:, columns(first + c, width)] = part
        if aligned and h < n_tp - 1:
            exchange(h + 1)
    if not aligned:
        for p in range(n_tp):
            rs_send[p] = tsum[:, p * d_loc : (p + 1) * d_loc].astype(BF16)
        for step in range(1, n_tp):
            exchange(step)
    rs_recv[tp] = rs_send[tp]
    local[5].wait()
    for step in range(1, n_tp):
        arrival(rs_recv.at[tp_id(step)], rs_rsem.at[tp_id(step)]).wait()
    moe = rs_recv[0].astype(F32)
    for p in range(1, n_tp):
        moe = moe + rs_recv[p].astype(F32)
    next_hidden = (hid_all[tp].astype(F32) + moe).astype(BF16)
    next_out[...] = next_hidden
    next_wide = next_hidden.astype(F32)
    square = jnp.sum(next_wide * next_wide, -1, keepdims=True)
    scaled = (next_wide * attn_gain[...].reshape(1, d_loc)).astype(BF16)
    kvp = up(kvc + 3, 128)
    tail = kvp - kvc
    part = lax.dot_general(
        scaled, wk[...], (((1,), (1,)), ((), ())), preferred_element_type=F32
    )
    key_send[:, :kvc] = part.astype(BF16)
    key_send[:, kvc:kvp] = split3(square, tail)
    for step in range(1, n_tp):
        copy = tp_copy(key_send, key_recv.at[tp], key_ssem.at[step], key_rsem.at[tp], step)
        copy.start()
        sends.append(copy)
    key_recv[tp] = key_send[...]
    attend(stops[3], tokens)
    half = (kvc - lat) // 2
    lane = lax.broadcasted_iota(jnp.int32, (tokens, 2 * half), 1)
    pair = jnp.where(lane < half, lane, lane - half).astype(F32)
    freq = jnp.exp(pair * (-9.210340371976184 / half))
    row_id = lax.broadcasted_iota(jnp.int32, (tokens, 2 * half), 0)
    place = jnp.zeros((tokens, 2 * half), F32)
    for t in range(tokens):
        place = jnp.where(row_id == t, lengths[t].astype(F32), place)
    angle = place * freq
    cos_table = jnp.cos(angle)
    sin_table = jnp.where(lane < half, -1.0, 1.0) * jnp.sin(angle)
    for step in range(1, n_tp):
        arrival(key_recv.at[tp_id(step)], key_rsem.at[tp_id(step)]).wait()
    total = key_recv[0].astype(F32)
    for p in range(1, n_tp):
        total = total + key_recv[p].astype(F32)
    square = jnp.sum(total[:, kvc:], -1, keepdims=True)
    down = total * lax.rsqrt(square / d_all + epsilon)
    latent = down[:, :lat]
    latent = (
        latent
        * lax.rsqrt(jnp.mean(latent * latent, -1, keepdims=True) + epsilon)
        * kv_gain[...]
    )
    rope = down[:, lat:kvc]
    swapped = jnp.concatenate([rope[:, half:], rope[:, :half]], 1)
    rope = rope * cos_table + swapped * sin_table
    keys[:, :lat] = latent.astype(BF16)
    keys[:, lat:kvc] = rope.astype(BF16)
    pairs = tokens * heads
    own = lax.dot_general(
        q_buf[...].reshape(pairs, kvc),
        keys[...],
        (((1,), (1,)), ((), ())),
        preferred_element_type=F32,
    )
    owner = lax.broadcasted_iota(jnp.int32, (pairs, tokens), 0) // heads
    mine = owner == lax.broadcasted_iota(jnp.int32, (pairs, tokens), 1)
    own = jnp.sum(jnp.where(mine, own, 0.0), -1, keepdims=True) * score_scale
    own = jnp.broadcast_to(own, (pairs, 128))
    peak = peaks[...].reshape(pairs, 128)
    top = jnp.maximum(peak, own)
    factor = jnp.exp(peak - top)
    own_prob = jnp.exp(own - top)
    inverse = 1.0 / (masses[...].reshape(pairs, 128) * factor + own_prob)
    old_part[...] = (factor * inverse).reshape(tokens, heads, 128)
    own_part[...] = (own_prob.astype(BF16).astype(F32) * inverse).reshape(tokens, heads, 128)
    for t in range(tokens):
        for c in range(0, lat, 128):
            value = acc[t, :, c : c + 128] * old_part[t]
            key = keys[t : t + 1, c : c + 128].astype(F32)
            latent_out[t, :, c : c + 128] = (value + own_part[t] * key).astype(BF16)
    for copy in sends:
        copy.wait_send()

    def drain(t, carry):
        for step in range(1, n_tp):
            cache_copy(t, step).wait_send()
        return carry

    lax.fori_loop(0, tokens, drain, 0)


def solution(mesh):
    n_tp, n_ep, n_mb = mesh.shape["tp"], mesh.shape["ep"], mesh.shape["mb"]
    experts = n_ep * n_mb

    def local(
        hidden,
        moe_gain,
        expert_ids,
        slots,
        affinity,
        w_gate,
        w_up,
        w_down,
        attn_gain,
        w_dkv,
        kv_gain,
        queries,
        cache,
        lengths,
    ):
        tokens, d_loc = hidden.shape
        d_all = d_loc * n_tp
        heads, kvc = queries.shape[1:]
        span = cache.shape[1]
        lat = kv_gain.shape[0]
        hid_dim = w_gate.shape[2]
        wide = up(kvc + 3, 128)
        any_space = pl.BlockSpec(memory_space=pl.ANY)
        vmem = pl.BlockSpec(memory_space=pltpu.VMEM)
        smem = pl.BlockSpec(memory_space=pltpu.SMEM)
        dma = pltpu.SemaphoreType.DMA
        return pl.pallas_call(
            functools.partial(kernel, n_tp, n_ep, n_mb),
            out_shape=(
                pltpu.VMEM((tokens, d_loc), BF16),
                pltpu.VMEM((tokens, heads, lat), BF16),
            ),
            in_specs=[
                any_space,
                vmem,
                vmem,
                vmem,
                vmem,
                any_space,
                any_space,
                any_space,
                vmem,
                any_space,
                vmem,
                any_space,
                any_space,
                smem,
            ],
            out_specs=(vmem, vmem),
            scratch_shapes=[
                pltpu.VMEM((n_tp, tokens, d_loc), BF16),
                pltpu.VMEM((n_tp, 1, d_loc), F32),
                pltpu.VMEM((experts, n_tp, CAP, d_loc), BF16),
                pltpu.VMEM((experts, n_tp, CAP, d_loc), BF16),
                pltpu.VMEM((d_all, hid_dim), BF16),
                pltpu.VMEM((d_all, hid_dim), BF16),
                pltpu.VMEM((hid_dim, d_all), BF16),
                pltpu.VMEM((kvc, d_loc), BF16),
                pltpu.VMEM((experts, CAP, d_all), BF16),
                pltpu.VMEM((experts, CAP, d_all), BF16),
                pltpu.VMEM((tokens, d_all), F32),
                pltpu.VMEM((n_tp, tokens, d_loc), BF16),
                pltpu.VMEM((n_tp, tokens, d_loc), BF16),
                pltpu.VMEM((tokens, wide), BF16),
                pltpu.VMEM((n_tp, tokens, wide), BF16),
                pltpu.VMEM((tokens, heads, kvc), BF16),
                pltpu.VMEM((tokens, n_tp, span, kvc), BF16),
                pltpu.VMEM((tokens, heads, lat), F32),
                pltpu.VMEM((tokens, heads, 128), F32),
                pltpu.VMEM((tokens, heads, 128), F32),
                pltpu.VMEM((tokens, kvc), BF16),
                pltpu.VMEM((tokens, heads, 128), F32),
                pltpu.VMEM((tokens, heads, 128), F32),
                dma((6,)),
                dma,
                dma((n_tp,)),
                dma((n_tp,)),
                dma((n_tp,)),
                dma((n_tp,)),
                dma((n_tp, tokens)),
                dma((n_tp, tokens)),
                dma((experts, n_tp)),
                dma((experts, n_tp)),
                dma((experts, max(2, n_tp))),
                dma((experts, max(2, n_tp))),
                dma((n_tp,)),
                dma((n_tp,)),
                dma((n_tp,)),
                dma((n_tp,)),
            ],
            compiler_params=pltpu.CompilerParams(
                collective_id=0, has_side_effects=True, vmem_limit_bytes=60 * 1024 * 1024
            ),
        )(
            hidden,
            moe_gain,
            expert_ids.T,
            slots.T,
            affinity.T,
            w_gate,
            w_up,
            w_down,
            attn_gain,
            w_dkv.T,
            kv_gain[None],
            queries,
            cache,
            lengths,
        )

    return jax.shard_map(
        local,
        mesh=mesh,
        in_specs=(
            P(("grp", "ep", "mb"), "tp"),
            P("tp"),
            P(("grp", "ep", "mb"), None),
            P(("grp", "ep", "mb"), None),
            P(("grp", "ep", "mb"), None),
            P(("ep", "mb"), None, "tp"),
            P(("ep", "mb"), None, "tp"),
            P(("ep", "mb"), "tp", None),
            P("tp"),
            P("tp", None),
            P(),
            P(("grp", "ep", "mb"), "tp", None),
            P(("grp", "ep", "mb"), "tp", None),
            P(("grp", "ep", "mb")),
        ),
        out_specs=(P(("grp", "ep", "mb"), "tp"), P(("grp", "ep", "mb"), "tp", None)),
        check_vma=False,
    )
```

```python
import functools

import jax
import jax.numpy as jnp
from jax import lax
from jax.experimental import pallas as pl
from jax.experimental.pallas import tpu as pltpu
from jax.sharding import PartitionSpec as P

CAP = 8
AHEAD = 3
epsilon = 1e-06
route_scale = 2.5
score_scale = 192.0 ** (-0.5)
STOPS = (2, 5, 10, 13)
MESH = pl.DeviceIdType.MESH
F32 = jnp.float32
BF16 = jnp.bfloat16


def up(value, step):
    return -(-value // step) * step


def split3(value, width):
    high = value.astype(BF16)
    rest = value - high.astype(F32)
    mid = rest.astype(BF16)
    low = (rest - mid.astype(F32)).astype(BF16)
    lane = lax.broadcasted_iota(jnp.int32, (value.shape[0], width), 1)
    parts = jnp.where(lane == 1, mid.astype(F32), jnp.where(lane == 2, low.astype(F32), 0.0))
    return jnp.where(lane == 0, high.astype(F32), parts).astype(BF16)


def kernel(
    n_tp,
    n_ep,
    n_mb,
    hidden,
    moe_gain_in,
    ids_in,
    slots_in,
    affinity_in,
    w_gate,
    w_up,
    w_down,
    attn_gain_in,
    w_dkv,
    kv_gain_in,
    queries,
    cache,
    lengths_in,
    next_out,
    latent_out,
    hid_all,
    gain_all,
    send,
    arrived,
    wg,
    wu,
    wd,
    wk,
    ret_send,
    ret,
    tsum,
    rs_send,
    rs_recv,
    key_send,
    key_recv,
    q_buf,
    kv_buf,
    acc,
    peaks,
    masses,
    keys,
    old_part,
    own_part,
    moe_gain,
    ids,
    slots,
    affinity,
    attn_gain,
    kv_gain,
    lengths,
    small_sem,
    near_sem,
    load_sem,
    kv_load_sem,
    hid_ssem,
    hid_rsem,
    gain_ssem,
    gain_rsem,
    kv_ssem,
    kv_rsem,
    row_ssem,
    row_rsem,
    ret_ssem,
    ret_rsem,
    rs_ssem,
    rs_rsem,
    key_ssem,
    key_rsem,
):
    experts = n_ep * n_mb
    tokens, d_loc = hidden.shape
    d_all = d_loc * n_tp
    lat = kv_gain.shape[1]
    kvc = cache.shape[2]
    tp = lax.axis_index("tp")
    chained = 1 < n_ep <= 4
    me = lax.axis_index("ep") * n_mb + lax.axis_index("mb")

    def tp_id(step):
        return lax.rem(tp + step, n_tp)

    def ex_id(step):
        return lax.rem(me + step, experts)

    def ex_dev(index):
        return {"ep": index // n_mb, "mb": lax.rem(index, n_mb)}
    local = [
        pltpu.make_async_copy(hidden, hid_all.at[tp], load_sem.at[0]),
        pltpu.make_async_copy(queries, q_buf, load_sem.at[1]),
        pltpu.make_async_copy(w_gate.at[0], wg, load_sem.at[2]),
        pltpu.make_async_copy(w_up.at[0], wu, load_sem.at[3]),
        pltpu.make_async_copy(w_down.at[0], wd, load_sem.at[4]),
        pltpu.make_async_copy(w_dkv, wk, load_sem.at[5]),
    ]
    kv_load = pltpu.make_async_copy(cache, kv_buf.at[:, tp], kv_load_sem)
    small = [
        pltpu.make_async_copy(src, dst, small_sem.at[i])
        for i, (src, dst) in enumerate(
            (
                (slots_in, slots),
                (ids_in, ids),
                (affinity_in, affinity),
                (moe_gain_in, moe_gain),
                (attn_gain_in, attn_gain),
                (kv_gain_in, kv_gain),
                (lengths_in, lengths),
            )
        )
    ]
    for copy in small[:4]:
        copy.start()
    local[0].start()
    kv_load.start()
    for copy in small[4:]:
        copy.start()

    ep, mb = lax.axis_index("ep"), lax.axis_index("mb")
    barrier = pltpu.get_barrier_semaphore()

    def hello(sem, ids):
        pl.semaphore_signal(sem, inc=1, device_id=ids, device_id_type=MESH)

    for step in range(1, n_tp):
        hello(barrier, {"tp": tp_id(step)})
    if chained:
        for step in range(1, n_mb):
            hello(barrier, {"mb": lax.rem(mb + step, n_mb)})
        greeted = n_tp - 1 + n_mb - 1 + n_mb * jnp.minimum(ep, 1)
    else:
        for step in range(1, experts):
            hello(barrier, ex_dev(ex_id(step)))
        greeted = n_tp - 1 + experts - 1
    for copy in small[:4]:
        copy.wait()
    gain_all[tp] = moe_gain[...].reshape(1, d_loc)
    kept = slots[...] < CAP
    aff = affinity[...]
    weight = route_scale * aff / jnp.sum(aff, 0, keepdims=True) * kept.astype(F32)
    target = jnp.where(kept, ids[...] * CAP + slots[...], -1)
    rows = experts * CAP
    iota = lax.broadcasted_iota(jnp.int32, (rows, tokens), 0)
    dispatch = jnp.zeros((rows, tokens), F32)
    combine = jnp.zeros((rows, tokens), F32)
    for k in range(ids.shape[0]):
        match = target[k : k + 1] == iota
        dispatch = jnp.where(match, 1.0, dispatch)
        combine = jnp.where(match, weight[k : k + 1], combine)
    dispatch = dispatch.astype(BF16)
    combine = combine.T
    high = combine.astype(BF16)
    rest = combine - high.astype(F32)
    mid = rest.astype(BF16)
    low = (rest - mid.astype(F32)).astype(BF16)
    combine3 = jnp.concatenate([high, mid, low], 0)

    def pick(block):
        picked = jnp.dot(dispatch, hid_all[block], preferred_element_type=F32)
        send[:, block] = picked.reshape(experts, CAP, d_loc).astype(BF16)

    def row_copy(peer, block):
        return pltpu.make_async_remote_copy(
            src_ref=send.at[peer, block],
            dst_ref=arrived.at[me, block],
            send_sem=row_ssem.at[peer, block],
            recv_sem=row_rsem.at[me, block],
            device_id=ex_dev(peer),
            device_id_type=MESH,
        )

    def ship_to(ep_index, block):
        for m in range(n_mb):
            row_copy(ep_index * n_mb + m, block).start()

    def ship_near(block):
        arrived[me, block] = send[me, block]
        for step in range(1, n_mb):
            row_copy(ep * n_mb + lax.rem(mb + step, n_mb), block).start()

    def ship(block):
        ship_near(block)
        for far in range(1, n_ep):
            pl.when(ep >= far)(functools.partial(ship_to, ep - far, block))
            pl.when(ep + far < n_ep)(functools.partial(ship_to, ep + far, block))
    local[0].wait()
    pick(tp)
    kv_load.wait()
    for copy in local[1:]:
        copy.start()
    pl.semaphore_wait(barrier, greeted)
    if chained:

        @pl.when(ep + 1 < n_ep)
        def _():
            for m in range(n_mb):
                hello(barrier, {"ep": ep + 1, "mb": m})

        for far in range(1, n_ep):

            @pl.when(ep >= far)
            def _():
                for m in range(n_mb):
                    hello(near_sem.at[far], {"ep": ep - far, "mb": m})


    def tp_copy(src, dst, ssem, rsem, step):
        return pltpu.make_async_remote_copy(
            src_ref=src,
            dst_ref=dst,
            send_sem=ssem,
            recv_sem=rsem,
            device_id={"tp": tp_id(step)},
            device_id_type=MESH,
        )

    def arrival(dst, rsem):
        return pltpu.make_async_copy(dst, dst, rsem)
    sends = []
    for step in range(1, n_tp):
        for src, dst, ssem, rsem in (
            (hid_all.at[tp], hid_all, hid_ssem, hid_rsem),
            (gain_all.at[tp], gain_all, gain_ssem, gain_rsem),
        ):
            copy = tp_copy(src, dst.at[tp], ssem.at[step], rsem.at[tp], step)
            copy.start()
            sends.append(copy)

    def cache_copy(t, step):
        return tp_copy(
            kv_buf.at[t, tp], kv_buf.at[t, tp], kv_ssem.at[step, t], kv_rsem.at[tp, t], step
        )

    def feed(t):
        for step in range(1, n_tp):
            cache_copy(t, step).start()

    for t in range(AHEAD):
        feed(t)
    if chained:
        ship_near(tp)
        for far in range(1, n_ep):
            pl.when(ep >= far)(functools.partial(ship_to, ep - far, tp))
        for far in range(1, n_ep):

            @pl.when(ep + far < n_ep)
            def _():
                pl.semaphore_wait(near_sem.at[far], n_mb)
                ship_to(ep + far, tp)
    else:
        ship(tp)
    for step in range(1, n_tp):
        arrival(hid_all.at[tp_id(step)], hid_rsem.at[tp_id(step)]).wait()
        arrival(gain_all.at[tp_id(step)], gain_rsem.at[tp_id(step)]).wait()
    for turn in range(1, n_tp):
        pick(tp_id(turn))
        ship(tp_id(turn))

    local[1].wait()
    heads = queries.shape[1]
    span_len = cache.shape[1]
    total_len = n_tp * span_len

    def attend(first, last):
        def body(t, carry):
            for step in range(1, n_tp):
                arrival(kv_buf.at[t, tp_id(step)], kv_rsem.at[tp_id(step), t]).wait()

            @pl.when(t + AHEAD < tokens)
            def _():
                feed(t + AHEAD)

            block = kv_buf[t].reshape(total_len, kvc)
            scores = (
                lax.dot_general(
                    q_buf[t], block, (((1,), (1,)), ((), ())), preferred_element_type=F32
                )
                * score_scale
            )
            live = lax.broadcasted_iota(jnp.int32, (heads, total_len), 1) < lengths[t]
            scores = jnp.where(live, scores, -1e30)
            peak = jnp.max(scores, -1, keepdims=True)
            prob = jnp.where(live, jnp.exp(scores - peak), 0.0)
            mass = jnp.sum(prob, -1, keepdims=True)
            acc[t] = jnp.dot(prob.astype(BF16), block[:, :lat], preferred_element_type=F32)
            peaks[t] = jnp.broadcast_to(peak, (heads, 128))
            masses[t] = jnp.broadcast_to(mass, (heads, 128))
            return carry

        lax.fori_loop(first, last, body, 0)

    for copy in small[4:]:
        copy.wait()
    stops = [tokens * n // 16 for n in STOPS]
    attend(0, stops[0])
    local[2].wait()
    local[3].wait()
    gate = jnp.zeros((rows, wg.shape[1]), F32)
    upper = jnp.zeros((rows, wg.shape[1]), F32)
    square = jnp.zeros((rows, 1), F32)
    for turn in range(n_tp):
        b = tp_id(turn)
        if turn == n_tp - 1:
            attend(stops[0], stops[1])
        for step in range(1, experts):
            peer = ex_id(step)
            arrival(arrived.at[peer, b], row_rsem.at[peer, b]).wait()
        wide = arrived[:, b].astype(F32).reshape(rows, d_loc)
        square = square + jnp.sum(wide * wide, -1, keepdims=True)
        block = (wide * gain_all[b]).astype(BF16)
        deep = pl.ds(pl.multiple_of(b * d_loc, d_loc & -d_loc), d_loc)
        gate = gate + jnp.dot(block, wg[deep], preferred_element_type=F32)
        upper = upper + jnp.dot(block, wu[deep], preferred_element_type=F32)
    scale = lax.rsqrt(square / d_all + epsilon)
    gate = gate * scale
    upper = upper * scale
    units = (gate / (1.0 + jnp.exp(-gate)) * upper).astype(BF16)
    local[4].wait()
    width = 512 if d_all % 512 == 0 else 128
    aligned = d_loc % 128 == 0
    if aligned:
        width = next(w for w in (896, 512, 384, 256, 128) if d_loc % w == 0)
        pieces = [
            (pl.multiple_of(tp_id(turn) * d_loc, 128), d_loc) for turn in (*range(1, n_tp), 0)
        ]
    else:
        middle = d_all // width // 2 * width
        pieces = [(0, middle), (middle, d_all - middle)]

    def columns(start, size):
        return pl.ds(pl.multiple_of(start, 128), size)

    for h, (first, size) in enumerate(pieces):
        for c in range(0, size, width):
            part = jnp.dot(units, wd[:, columns(first + c, width)], preferred_element_type=F32)
            ret_send[:, :, columns(first + c, width)] = part.reshape(
                experts, CAP, width
            ).astype(BF16)
        for step in range(1, experts):
            peer = ex_id(step)
            copy = pltpu.make_async_remote_copy(
                src_ref=ret_send.at[peer, :, columns(first, size)],
                dst_ref=ret.at[me, :, columns(first, size)],
                send_sem=ret_ssem.at[step, h],
                recv_sem=ret_rsem.at[me, h],
                device_id=ex_dev(peer),
                device_id_type=MESH,
            )
            copy.start()
            sends.append(copy)
    ret[me] = ret_send[me]

    def exchange(step):
        copy = tp_copy(
            rs_send.at[tp_id(step)], rs_recv.at[tp], rs_ssem.at[step], rs_rsem.at[tp], step
        )
        copy.start()
        sends.append(copy)

    for h, (first, size) in enumerate(pieces):
        if h < 2:
            attend(stops[h + 1], stops[h + 2])
        for step in range(1, experts):
            peer = ex_id(step)
            arrival(ret.at[peer, :, columns(first, size)], ret_rsem.at[peer, h]).wait()
        for c in range(0, size, width):
            block = ret[:, :, columns(first + c, width)].astype(F32)
            block = block.reshape(rows, width).astype(BF16)
            part = jnp.dot(combine3, block, preferred_element_type=F32)
            part = part[:tokens] + (part[tokens : 2 * tokens] + part[2 * tokens : 3 * tokens])
            if aligned:
                rs_send[tp_id(h + 1), :, c : c + width] = part.astype(BF16)
            else:
                tsum[:, columns(first + c, width)] = part
        if aligned and h < n_tp - 1:
            exchange(h + 1)
    if not aligned:
        for p in range(n_tp):
            rs_send[p] = tsum[:, p * d_loc : (p + 1) * d_loc].astype(BF16)
        for step in range(1, n_tp):
            exchange(step)
    rs_recv[tp] = rs_send[tp]
    local[5].wait()
    for step in range(1, n_tp):
        arrival(rs_recv.at[tp_id(step)], rs_rsem.at[tp_id(step)]).wait()
    moe = rs_recv[0].astype(F32)
    for p in range(1, n_tp):
        moe = moe + rs_recv[p].astype(F32)
    next_hidden = (hid_all[tp].astype(F32) + moe).astype(BF16)
    next_out[...] = next_hidden
    next_wide = next_hidden.astype(F32)
    square = jnp.sum(next_wide * next_wide, -1, keepdims=True)
    scaled = (next_wide * attn_gain[...].reshape(1, d_loc)).astype(BF16)
    kvp = up(kvc + 3, 128)
    tail = kvp - kvc
    part = lax.dot_general(
        scaled, wk[...], (((1,), (1,)), ((), ())), preferred_element_type=F32
    )
    key_send[:, :kvc] = part.astype(BF16)
    key_send[:, kvc:kvp] = split3(square, tail)
    for step in range(1, n_tp):
        copy = tp_copy(key_send, key_recv.at[tp], key_ssem.at[step], key_rsem.at[tp], step)
        copy.start()
        sends.append(copy)
    key_recv[tp] = key_send[...]
    attend(stops[3], tokens)
    half = (kvc - lat) // 2
    lane = lax.broadcasted_iota(jnp.int32, (tokens, 2 * half), 1)
    pair = jnp.where(lane < half, lane, lane - half).astype(F32)
    freq = jnp.exp(pair * (-9.210340371976184 / half))
    row_id = lax.broadcasted_iota(jnp.int32, (tokens, 2 * half), 0)
    place = jnp.zeros((tokens, 2 * half), F32)
    for t in range(tokens):
        place = jnp.where(row_id == t, lengths[t].astype(F32), place)
    angle = place * freq
    cos_table = jnp.cos(angle)
    sin_table = jnp.where(lane < half, -1.0, 1.0) * jnp.sin(angle)
    for step in range(1, n_tp):
        arrival(key_recv.at[tp_id(step)], key_rsem.at[tp_id(step)]).wait()
    total = key_recv[0].astype(F32)
    for p in range(1, n_tp):
        total = total + key_recv[p].astype(F32)
    square = jnp.sum(total[:, kvc:], -1, keepdims=True)
    down = total * lax.rsqrt(square / d_all + epsilon)
    latent = down[:, :lat]
    latent = (
        latent
        * lax.rsqrt(jnp.mean(latent * latent, -1, keepdims=True) + epsilon)
        * kv_gain[...]
    )
    rope = down[:, lat:kvc]
    swapped = jnp.concatenate([rope[:, half:], rope[:, :half]], 1)
    rope = rope * cos_table + swapped * sin_table
    keys[:, :lat] = latent.astype(BF16)
    keys[:, lat:kvc] = rope.astype(BF16)
    pairs = tokens * heads
    own = lax.dot_general(
        q_buf[...].reshape(pairs, kvc),
        keys[...],
        (((1,), (1,)), ((), ())),
        preferred_element_type=F32,
    )
    owner = lax.broadcasted_iota(jnp.int32, (pairs, tokens), 0) // heads
    mine = owner == lax.broadcasted_iota(jnp.int32, (pairs, tokens), 1)
    own = jnp.sum(jnp.where(mine, own, 0.0), -1, keepdims=True) * score_scale
    own = jnp.broadcast_to(own, (pairs, 128))
    peak = peaks[...].reshape(pairs, 128)
    top = jnp.maximum(peak, own)
    factor = jnp.exp(peak - top)
    own_prob = jnp.exp(own - top)
    inverse = 1.0 / (masses[...].reshape(pairs, 128) * factor + own_prob)
    old_part[...] = (factor * inverse).reshape(tokens, heads, 128)
    own_part[...] = (own_prob.astype(BF16).astype(F32) * inverse).reshape(tokens, heads, 128)
    for t in range(tokens):
        for c in range(0, lat, 128):
            value = acc[t, :, c : c + 128] * old_part[t]
            key = keys[t : t + 1, c : c + 128].astype(F32)
            latent_out[t, :, c : c + 128] = (value + own_part[t] * key).astype(BF16)
    for copy in sends:
        copy.wait_send()

    for step in range(1, experts):
        for block in range(n_tp):
            row_copy(ex_id(step), block).wait_send()

    def drain(t, carry):
        for step in range(1, n_tp):
            cache_copy(t, step).wait_send()
        return carry

    lax.fori_loop(0, tokens, drain, 0)


def solution(mesh):
    n_tp, n_ep, n_mb = mesh.shape["tp"], mesh.shape["ep"], mesh.shape["mb"]
    experts = n_ep * n_mb

    def local(
        hidden,
        moe_gain,
        expert_ids,
        slots,
        affinity,
        w_gate,
        w_up,
        w_down,
        attn_gain,
        w_dkv,
        kv_gain,
        queries,
        cache,
        lengths,
    ):
        tokens, d_loc = hidden.shape
        d_all = d_loc * n_tp
        heads, kvc = queries.shape[1:]
        span = cache.shape[1]
        lat = kv_gain.shape[0]
        hid_dim = w_gate.shape[2]
        top = expert_ids.shape[1]
        wide = up(kvc + 3, 128)
        any_space = pl.BlockSpec(memory_space=pl.ANY)
        vmem = pl.BlockSpec(memory_space=pltpu.VMEM)
        dma = pltpu.SemaphoreType.DMA
        return pl.pallas_call(
            functools.partial(kernel, n_tp, n_ep, n_mb),
            out_shape=(
                pltpu.VMEM((tokens, d_loc), BF16),
                pltpu.VMEM((tokens, heads, lat), BF16),
            ),
            in_specs=[any_space] * 14,
            out_specs=(vmem, vmem),
            scratch_shapes=[
                pltpu.VMEM((n_tp, tokens, d_loc), BF16),
                pltpu.VMEM((n_tp, 1, d_loc), F32),
                pltpu.VMEM((experts, n_tp, CAP, d_loc), BF16),
                pltpu.VMEM((experts, n_tp, CAP, d_loc), BF16),
                pltpu.VMEM((d_all, hid_dim), BF16),
                pltpu.VMEM((d_all, hid_dim), BF16),
                pltpu.VMEM((hid_dim, d_all), BF16),
                pltpu.VMEM((kvc, d_loc), BF16),
                pltpu.VMEM((experts, CAP, d_all), BF16),
                pltpu.VMEM((experts, CAP, d_all), BF16),
                pltpu.VMEM((tokens, d_all), F32),
                pltpu.VMEM((n_tp, tokens, d_loc), BF16),
                pltpu.VMEM((n_tp, tokens, d_loc), BF16),
                pltpu.VMEM((tokens, wide), BF16),
                pltpu.VMEM((n_tp, tokens, wide), BF16),
                pltpu.VMEM((tokens, heads, kvc), BF16),
                pltpu.VMEM((tokens, n_tp, span, kvc), BF16),
                pltpu.VMEM((tokens, heads, lat), F32),
                pltpu.VMEM((tokens, heads, 128), F32),
                pltpu.VMEM((tokens, heads, 128), F32),
                pltpu.VMEM((tokens, kvc), BF16),
                pltpu.VMEM((tokens, heads, 128), F32),
                pltpu.VMEM((tokens, heads, 128), F32),
                pltpu.VMEM((d_loc,), F32),
                pltpu.VMEM((top, tokens), jnp.int32),
                pltpu.VMEM((top, tokens), jnp.int32),
                pltpu.VMEM((top, tokens), F32),
                pltpu.VMEM((d_loc,), F32),
                pltpu.VMEM((1, lat), F32),
                pltpu.SMEM((tokens,), jnp.int32),
                dma((7,)),
                pltpu.SemaphoreType.REGULAR((n_ep,)),
                dma((6,)),
                dma,
                dma((n_tp,)),
                dma((n_tp,)),
                dma((n_tp,)),
                dma((n_tp,)),
                dma((n_tp, tokens)),
                dma((n_tp, tokens)),
                dma((experts, n_tp)),
                dma((experts, n_tp)),
                dma((experts, max(2, n_tp))),
                dma((experts, max(2, n_tp))),
                dma((n_tp,)),
                dma((n_tp,)),
                dma((n_tp,)),
                dma((n_tp,)),
            ],
            compiler_params=pltpu.CompilerParams(
                collective_id=0, has_side_effects=True, vmem_limit_bytes=60 * 1024 * 1024
            ),
        )(
            hidden,
            moe_gain,
            expert_ids.T,
            slots.T,
            affinity.T,
            w_gate,
            w_up,
            w_down,
            attn_gain,
            w_dkv.T,
            kv_gain[None],
            queries,
            cache,
            lengths,
        )

    return jax.shard_map(
        local,
        mesh=mesh,
        in_specs=(
            P(("grp", "ep", "mb"), "tp"),
            P("tp"),
            P(("grp", "ep", "mb"), None),
            P(("grp", "ep", "mb"), None),
            P(("grp", "ep", "mb"), None),
            P(("ep", "mb"), None, "tp"),
            P(("ep", "mb"), None, "tp"),
            P(("ep", "mb"), "tp", None),
            P("tp"),
            P("tp", None),
            P(),
            P(("grp", "ep", "mb"), "tp", None),
            P(("grp", "ep", "mb"), "tp", None),
            P(("grp", "ep", "mb")),
        ),
        out_specs=(P(("grp", "ep", "mb"), "tp"), P(("grp", "ep", "mb"), "tp", None)),
        check_vma=False,
    )
```

```python
import functools

import jax
import jax.numpy as jnp
from jax import lax
from jax.experimental import pallas as pl
from jax.experimental.pallas import tpu as pltpu
from jax.sharding import PartitionSpec as P

CAP = 8
AHEAD = 3
epsilon = 1e-06
route_scale = 2.5
score_scale = 192.0 ** (-0.5)
STOPS = (1, 2, 4, 6)
MESH = pl.DeviceIdType.MESH
F32 = jnp.float32
BF16 = jnp.bfloat16


def up(value, step):
    return -(-value // step) * step


def split3(value, width):
    high = value.astype(BF16)
    rest = value - high.astype(F32)
    mid = rest.astype(BF16)
    low = (rest - mid.astype(F32)).astype(BF16)
    lane = lax.broadcasted_iota(jnp.int32, (value.shape[0], width), 1)
    parts = jnp.where(lane == 1, mid.astype(F32), jnp.where(lane == 2, low.astype(F32), 0.0))
    return jnp.where(lane == 0, high.astype(F32), parts).astype(BF16)


def kernel(
    n_tp,
    n_ep,
    n_mb,
    hidden,
    moe_gain_in,
    ids_in,
    slots_in,
    affinity_in,
    w_gate,
    w_up,
    w_down,
    attn_gain_in,
    w_dkv,
    kv_gain_in,
    queries,
    cache,
    lengths_in,
    next_out,
    latent_out,
    hid_all,
    gain_all,
    send,
    arrived,
    wg,
    wu,
    wd,
    wk,
    ret_send,
    ret,
    tsum,
    rs_send,
    rs_recv,
    key_send,
    key_recv,
    q_buf,
    kv_buf,
    rope_in,
    acc,
    peaks,
    masses,
    keys,
    old_part,
    own_part,
    moe_gain,
    ids,
    slots,
    affinity,
    attn_gain,
    kv_gain,
    lengths,
    small_sem,
    near_sem,
    load_sem,
    kv_load_sem,
    hid_ssem,
    hid_rsem,
    gain_ssem,
    gain_rsem,
    kv_ssem,
    kv_rsem,
    row_ssem,
    row_rsem,
    ret_ssem,
    ret_rsem,
    rs_ssem,
    rs_rsem,
    key_ssem,
    key_rsem,
):
    experts = n_ep * n_mb
    tokens, d_loc = hidden.shape
    d_all = d_loc * n_tp
    lat = kv_gain.shape[1]
    pairs, span_len, kvc = cache.shape[0], cache.shape[2], cache.shape[3]
    tp = lax.axis_index("tp")
    staged = 1 < n_ep <= 4
    me = lax.axis_index("ep") * n_mb + lax.axis_index("mb")

    def tp_id(step):
        return lax.rem(tp + step, n_tp)

    def ex_id(step):
        return lax.rem(me + step, experts)

    def ex_dev(index):
        return {"ep": index // n_mb, "mb": lax.rem(index, n_mb)}
    local = [
        pltpu.make_async_copy(hidden, hid_all.at[tp], load_sem.at[0]),
        pltpu.make_async_copy(queries, q_buf, load_sem.at[1]),
        pltpu.make_async_copy(w_gate.at[0], wg, load_sem.at[2]),
        pltpu.make_async_copy(w_up.at[0], wu, load_sem.at[3]),
        pltpu.make_async_copy(w_down.at[0], wd, load_sem.at[4]),
        pltpu.make_async_copy(w_dkv, wk, load_sem.at[5]),
    ]
    rope = kvc - lat
    lanes = kv_buf.shape[3]
    kv_loads = [
        pltpu.make_async_copy(
            cache.at[:, i, :, :lat], kv_buf.at[:, tp, :, i * lat : (i + 1) * lat], kv_load_sem.at[i]
        )
        for i in range(2)
    ]
    kv_loads.append(pltpu.make_async_copy(cache.at[:, :, :, lat:], rope_in, kv_load_sem.at[2]))
    small = [
        pltpu.make_async_copy(src, dst, small_sem.at[i])
        for i, (src, dst) in enumerate(
            (
                (slots_in, slots),
                (ids_in, ids),
                (affinity_in, affinity),
                (moe_gain_in, moe_gain),
                (attn_gain_in, attn_gain),
                (kv_gain_in, kv_gain),
                (lengths_in, lengths),
            )
        )
    ]
    for copy in small[:4]:
        copy.start()
    local[0].start()
    for copy in kv_loads:
        copy.start()
    for copy in small[4:]:
        copy.start()

    ep, mb = lax.axis_index("ep"), lax.axis_index("mb")
    barrier = pltpu.get_barrier_semaphore()

    def hello(sem, ids):
        pl.semaphore_signal(sem, inc=1, device_id=ids, device_id_type=MESH)

    for step in range(1, n_tp):
        hello(barrier, {"tp": tp_id(step)})
    if staged:
        for step in range(1, n_mb):
            hello(barrier, {"mb": lax.rem(mb + step, n_mb)})
        for far in range(1, n_ep):

            @pl.when(ep + far < n_ep)
            def _():
                for m in range(n_mb):
                    hello(barrier, {"ep": ep + far, "mb": m})

        greeted = n_tp - 1 + n_mb - 1 + n_mb * ep
    else:
        for step in range(1, experts):
            hello(barrier, ex_dev(ex_id(step)))
        greeted = n_tp - 1 + experts - 1

    def tp_copy(src, dst, ssem, rsem, step):
        return pltpu.make_async_remote_copy(
            src_ref=src,
            dst_ref=dst,
            send_sem=ssem,
            recv_sem=rsem,
            device_id={"tp": tp_id(step)},
            device_id_type=MESH,
        )

    def arrival(dst, rsem):
        return pltpu.make_async_copy(dst, dst, rsem)

    def cache_copy(t, step):
        return tp_copy(
            kv_buf.at[t, tp], kv_buf.at[t, tp], kv_ssem.at[step, t], kv_rsem.at[tp, t], step
        )

    def feed(t):
        for step in range(1, n_tp):
            cache_copy(t, step).start()

    def row_copy(peer, block):
        return pltpu.make_async_remote_copy(
            src_ref=send.at[peer, block],
            dst_ref=arrived.at[me, block],
            send_sem=row_ssem.at[peer, block],
            recv_sem=row_rsem.at[me, block],
            device_id=ex_dev(peer),
            device_id_type=MESH,
        )

    def ship_to(ep_index, block):
        for m in range(n_mb):
            row_copy(ep_index * n_mb + m, block).start()

    def ship_near(block):
        arrived[me, block] = send[me, block]
        for step in range(1, n_mb):
            row_copy(ep * n_mb + lax.rem(mb + step, n_mb), block).start()

    def ship(block):
        ship_near(block)
        for far in range(1, n_ep):
            pl.when(ep >= far)(functools.partial(ship_to, ep - far, block))
            pl.when(ep + far < n_ep)(functools.partial(ship_to, ep + far, block))
    small[3].wait()
    gain_all[tp] = moe_gain[...].reshape(1, d_loc)
    local[0].wait()
    pl.semaphore_wait(barrier, greeted)
    sends = []
    for step in range(1, n_tp):
        for src, dst, ssem, rsem in (
            (hid_all.at[tp], hid_all, hid_ssem, hid_rsem),
            (gain_all.at[tp], gain_all, gain_ssem, gain_rsem),
        ):
            copy = tp_copy(src, dst.at[tp], ssem.at[step], rsem.at[tp], step)
            copy.start()
            sends.append(copy)
    if staged:
        for far in range(1, n_ep):

            @pl.when(ep >= far)
            def _():
                for m in range(n_mb):
                    hello(near_sem.at[far], {"ep": ep - far, "mb": m})

    for copy in small[:3]:
        copy.wait()
    kept = slots[...] < CAP
    target = jnp.where(kept, ids[...] * CAP + slots[...], -1)
    rows = experts * CAP
    iota = lax.broadcasted_iota(jnp.int32, (rows, tokens), 0)
    dispatch = jnp.zeros((rows, tokens), F32)
    for k in range(ids.shape[0]):
        dispatch = jnp.where(target[k : k + 1] == iota, 1.0, dispatch)
    dispatch = dispatch.astype(BF16)

    def pick(block):
        picked = jnp.dot(dispatch, hid_all[block], preferred_element_type=F32)
        send[:, block] = picked.reshape(experts, CAP, d_loc).astype(BF16)

    pick(tp)
    if staged:
        ship_near(tp)
        for far in range(1, n_ep):
            pl.when(ep >= far)(functools.partial(ship_to, ep - far, tp))
    else:
        ship(tp)
    for copy in kv_loads:
        copy.wait()
    kv_buf[:, tp, :, 2 * lat : 2 * lat + 2 * rope] = jnp.concatenate(
        [rope_in[:, 0], rope_in[:, 1]], -1
    )
    for t in range(AHEAD):
        feed(t)
    for copy in local[1:]:
        copy.start()
    aff = affinity[...]
    weight = route_scale * aff / jnp.sum(aff, 0, keepdims=True) * kept.astype(F32)
    combine = jnp.zeros((rows, tokens), F32)
    for k in range(ids.shape[0]):
        combine = jnp.where(target[k : k + 1] == iota, weight[k : k + 1], combine)
    combine = combine.T
    high = combine.astype(BF16)
    rest = combine - high.astype(F32)
    mid = rest.astype(BF16)
    low = (rest - mid.astype(F32)).astype(BF16)
    combine3 = jnp.concatenate([high, mid, low], 0)
    if staged:
        for far in range(1, n_ep):

            @pl.when(ep + far < n_ep)
            def _():
                pl.semaphore_wait(near_sem.at[far], n_mb)
                ship_to(ep + far, tp)
    for step in range(1, n_tp):
        arrival(hid_all.at[tp_id(step)], hid_rsem.at[tp_id(step)]).wait()
        arrival(gain_all.at[tp_id(step)], gain_rsem.at[tp_id(step)]).wait()
    for turn in range(1, n_tp):
        pick(tp_id(turn))
        ship(tp_id(turn))

    local[1].wait()
    heads = queries.shape[1]
    total_len = n_tp * span_len

    def attend(first, last):
        def body(p, carry):
            for step in range(1, n_tp):
                arrival(kv_buf.at[p, tp_id(step)], kv_rsem.at[tp_id(step), p]).wait()

            @pl.when(p + AHEAD < pairs)
            def _():
                feed(p + AHEAD)

            ropes = kv_buf[p, :, :, 2 * lat :].reshape(total_len, lanes - 2 * lat)
            gap = jnp.zeros((heads, rope), BF16)
            turned = [q_buf[2 * p][:, lat:], gap, gap, q_buf[2 * p + 1][:, lat:]]
            turned = jnp.concatenate(
                [jnp.concatenate(turned[:2], 1), jnp.concatenate(turned[2:], 1)], 0
            )
            turned = lax.dot_general(
                turned, ropes, (((1,), (1,)), ((), ())), preferred_element_type=F32
            )
            for i in range(2):
                t = 2 * p + i
                block = kv_buf[p, :, :, i * lat : (i + 1) * lat].reshape(total_len, lat)
                scores = lax.dot_general(
                    q_buf[t][:, :lat], block, (((1,), (1,)), ((), ())), preferred_element_type=F32
                )
                scores = (scores + turned[i * heads : (i + 1) * heads]) * score_scale
                live = lax.broadcasted_iota(jnp.int32, (heads, total_len), 1) < lengths[t]
                scores = jnp.where(live, scores, -1e30)
                peak = jnp.max(scores, -1, keepdims=True)
                prob = jnp.where(live, jnp.exp(scores - peak), 0.0)
                mass = jnp.sum(prob, -1, keepdims=True)
                acc[t] = jnp.dot(prob.astype(BF16), block, preferred_element_type=F32)
                peaks[t] = jnp.broadcast_to(peak, (heads, 128))
                masses[t] = jnp.broadcast_to(mass, (heads, 128))
            return carry

        lax.fori_loop(first, last, body, 0)

    for copy in small[4:]:
        copy.wait()
    stops = [pairs * n // 8 for n in STOPS]
    attend(0, stops[0])
    local[2].wait()
    local[3].wait()
    gate = jnp.zeros((rows, wg.shape[1]), F32)
    upper = jnp.zeros((rows, wg.shape[1]), F32)
    square = jnp.zeros((rows, 1), F32)
    for turn in range(n_tp):
        b = tp_id(turn)
        if turn == n_tp - 1:
            attend(stops[0], stops[1])
        for step in range(1, experts):
            peer = ex_id(step)
            arrival(arrived.at[peer, b], row_rsem.at[peer, b]).wait()
        wide = arrived[:, b].astype(F32).reshape(rows, d_loc)
        square = square + jnp.sum(wide * wide, -1, keepdims=True)
        block = (wide * gain_all[b]).astype(BF16)
        deep = pl.ds(pl.multiple_of(b * d_loc, d_loc & -d_loc), d_loc)
        gate = gate + jnp.dot(block, wg[deep], preferred_element_type=F32)
        upper = upper + jnp.dot(block, wu[deep], preferred_element_type=F32)
    scale = lax.rsqrt(square / d_all + epsilon)
    gate = gate * scale
    upper = upper * scale
    units = (gate / (1.0 + jnp.exp(-gate)) * upper).astype(BF16)
    local[4].wait()
    width = 512 if d_all % 512 == 0 else 128
    aligned = d_loc % 128 == 0
    if aligned:
        width = next(w for w in (896, 512, 384, 256, 128) if d_loc % w == 0)
        pieces = [
            (pl.multiple_of(tp_id(turn) * d_loc, 128), d_loc) for turn in (*range(1, n_tp), 0)
        ]
    else:
        middle = d_all // width // 2 * width
        pieces = [(0, middle), (middle, d_all - middle)]

    def columns(start, size):
        return pl.ds(pl.multiple_of(start, 128), size)

    for h, (first, size) in enumerate(pieces):
        for c in range(0, size, width):
            part = jnp.dot(units, wd[:, columns(first + c, width)], preferred_element_type=F32)
            ret_send[:, :, columns(first + c, width)] = part.reshape(
                experts, CAP, width
            ).astype(BF16)
        for step in range(1, experts):
            peer = ex_id(step)
            copy = pltpu.make_async_remote_copy(
                src_ref=ret_send.at[peer, :, columns(first, size)],
                dst_ref=ret.at[me, :, columns(first, size)],
                send_sem=ret_ssem.at[step, h],
                recv_sem=ret_rsem.at[me, h],
                device_id=ex_dev(peer),
                device_id_type=MESH,
            )
            copy.start()
            sends.append(copy)
    ret[me] = ret_send[me]

    def exchange(step):
        copy = tp_copy(
            rs_send.at[tp_id(step)], rs_recv.at[tp], rs_ssem.at[step], rs_rsem.at[tp], step
        )
        copy.start()
        sends.append(copy)

    for h, (first, size) in enumerate(pieces):
        if h < 2:
            attend(stops[h + 1], stops[h + 2])
        for step in range(1, experts):
            peer = ex_id(step)
            arrival(ret.at[peer, :, columns(first, size)], ret_rsem.at[peer, h]).wait()
        for c in range(0, size, width):
            block = ret[:, :, columns(first + c, width)].astype(F32)
            block = block.reshape(rows, width).astype(BF16)
            part = jnp.dot(combine3, block, preferred_element_type=F32)
            part = part[:tokens] + (part[tokens : 2 * tokens] + part[2 * tokens : 3 * tokens])
            if aligned:
                rs_send[tp_id(h + 1), :, c : c + width] = part.astype(BF16)
            else:
                tsum[:, columns(first + c, width)] = part
        if aligned and h < n_tp - 1:
            exchange(h + 1)
    if not aligned:
        for p in range(n_tp):
            rs_send[p] = tsum[:, p * d_loc : (p + 1) * d_loc].astype(BF16)
        for step in range(1, n_tp):
            exchange(step)
    rs_recv[tp] = rs_send[tp]
    local[5].wait()
    for step in range(1, n_tp):
        arrival(rs_recv.at[tp_id(step)], rs_rsem.at[tp_id(step)]).wait()
    moe = rs_recv[0].astype(F32)
    for p in range(1, n_tp):
        moe = moe + rs_recv[p].astype(F32)
    next_hidden = (hid_all[tp].astype(F32) + moe).astype(BF16)
    next_out[...] = next_hidden
    next_wide = next_hidden.astype(F32)
    square = jnp.sum(next_wide * next_wide, -1, keepdims=True)
    scaled = (next_wide * attn_gain[...].reshape(1, d_loc)).astype(BF16)
    kvp = up(kvc + 3, 128)
    tail = kvp - kvc
    part = lax.dot_general(
        scaled, wk[...], (((1,), (1,)), ((), ())), preferred_element_type=F32
    )
    key_send[:, :kvc] = part.astype(BF16)
    key_send[:, kvc:kvp] = split3(square, tail)
    for step in range(1, n_tp):
        copy = tp_copy(key_send, key_recv.at[tp], key_ssem.at[step], key_rsem.at[tp], step)
        copy.start()
        sends.append(copy)
    key_recv[tp] = key_send[...]
    attend(stops[3], pairs)
    half = (kvc - lat) // 2
    lane = lax.broadcasted_iota(jnp.int32, (tokens, 2 * half), 1)
    pair = jnp.where(lane < half, lane, lane - half).astype(F32)
    freq = jnp.exp(pair * (-9.210340371976184 / half))
    row_id = lax.broadcasted_iota(jnp.int32, (tokens, 2 * half), 0)
    place = jnp.zeros((tokens, 2 * half), F32)
    for t in range(tokens):
        place = jnp.where(row_id == t, lengths[t].astype(F32), place)
    angle = place * freq
    cos_table = jnp.cos(angle)
    sin_table = jnp.where(lane < half, -1.0, 1.0) * jnp.sin(angle)
    for step in range(1, n_tp):
        arrival(key_recv.at[tp_id(step)], key_rsem.at[tp_id(step)]).wait()
    total = key_recv[0].astype(F32)
    for p in range(1, n_tp):
        total = total + key_recv[p].astype(F32)
    square = jnp.sum(total[:, kvc:], -1, keepdims=True)
    down = total * lax.rsqrt(square / d_all + epsilon)
    latent = down[:, :lat]
    latent = (
        latent
        * lax.rsqrt(jnp.mean(latent * latent, -1, keepdims=True) + epsilon)
        * kv_gain[...]
    )
    turn = down[:, lat:kvc]
    swapped = jnp.concatenate([turn[:, half:], turn[:, :half]], 1)
    turn = turn * cos_table + swapped * sin_table
    keys[:, :lat] = latent.astype(BF16)
    keys[:, lat:kvc] = turn.astype(BF16)
    rows_all = tokens * heads
    own = lax.dot_general(
        q_buf[...].reshape(rows_all, kvc),
        keys[...],
        (((1,), (1,)), ((), ())),
        preferred_element_type=F32,
    )
    owner = lax.broadcasted_iota(jnp.int32, (rows_all, tokens), 0) // heads
    mine = owner == lax.broadcasted_iota(jnp.int32, (rows_all, tokens), 1)
    own = jnp.sum(jnp.where(mine, own, 0.0), -1, keepdims=True) * score_scale
    own = jnp.broadcast_to(own, (rows_all, 128))
    peak = peaks[...].reshape(rows_all, 128)
    top = jnp.maximum(peak, own)
    factor = jnp.exp(peak - top)
    own_prob = jnp.exp(own - top)
    inverse = 1.0 / (masses[...].reshape(rows_all, 128) * factor + own_prob)
    old_part[...] = (factor * inverse).reshape(tokens, heads, 128)
    own_part[...] = (own_prob.astype(BF16).astype(F32) * inverse).reshape(tokens, heads, 128)
    for t in range(tokens):
        for c in range(0, lat, 128):
            value = acc[t, :, c : c + 128] * old_part[t]
            key = keys[t : t + 1, c : c + 128].astype(F32)
            latent_out[t, :, c : c + 128] = (value + own_part[t] * key).astype(BF16)
    for copy in sends:
        copy.wait_send()

    for step in range(1, experts):
        for block in range(n_tp):
            row_copy(ex_id(step), block).wait_send()

    def drain(t, carry):
        for step in range(1, n_tp):
            cache_copy(t, step).wait_send()
        return carry

    lax.fori_loop(0, pairs, drain, 0)


def solution(mesh):
    n_tp, n_ep, n_mb = mesh.shape["tp"], mesh.shape["ep"], mesh.shape["mb"]
    experts = n_ep * n_mb

    def local(
        hidden,
        moe_gain,
        expert_ids,
        slots,
        affinity,
        w_gate,
        w_up,
        w_down,
        attn_gain,
        w_dkv,
        kv_gain,
        queries,
        cache,
        lengths,
    ):
        tokens, d_loc = hidden.shape
        d_all = d_loc * n_tp
        heads, kvc = queries.shape[1:]
        span = cache.shape[1]
        lat = kv_gain.shape[0]
        hid_dim = w_gate.shape[2]
        top = expert_ids.shape[1]
        wide = up(kvc + 3, 128)
        any_space = pl.BlockSpec(memory_space=pl.ANY)
        vmem = pl.BlockSpec(memory_space=pltpu.VMEM)
        dma = pltpu.SemaphoreType.DMA
        return pl.pallas_call(
            functools.partial(kernel, n_tp, n_ep, n_mb),
            out_shape=(
                pltpu.VMEM((tokens, d_loc), BF16),
                pltpu.VMEM((tokens, heads, lat), BF16),
            ),
            in_specs=[any_space] * 14,
            out_specs=(vmem, vmem),
            scratch_shapes=[
                pltpu.VMEM((n_tp, tokens, d_loc), BF16),
                pltpu.VMEM((n_tp, 1, d_loc), F32),
                pltpu.VMEM((experts, n_tp, CAP, d_loc), BF16),
                pltpu.VMEM((experts, n_tp, CAP, d_loc), BF16),
                pltpu.VMEM((d_all, hid_dim), BF16),
                pltpu.VMEM((d_all, hid_dim), BF16),
                pltpu.VMEM((hid_dim, d_all), BF16),
                pltpu.VMEM((kvc, d_loc), BF16),
                pltpu.VMEM((experts, CAP, d_all), BF16),
                pltpu.VMEM((experts, CAP, d_all), BF16),
                pltpu.VMEM((tokens, d_all), F32),
                pltpu.VMEM((n_tp, tokens, d_loc), BF16),
                pltpu.VMEM((n_tp, tokens, d_loc), BF16),
                pltpu.VMEM((tokens, wide), BF16),
                pltpu.VMEM((n_tp, tokens, wide), BF16),
                pltpu.VMEM((tokens, heads, kvc), BF16),
                pltpu.VMEM((tokens // 2, n_tp, span, up(2 * kvc, 128)), BF16),
                pltpu.VMEM((tokens // 2, 2, span, kvc - lat), BF16),
                pltpu.VMEM((tokens, heads, lat), F32),
                pltpu.VMEM((tokens, heads, 128), F32),
                pltpu.VMEM((tokens, heads, 128), F32),
                pltpu.VMEM((tokens, kvc), BF16),
                pltpu.VMEM((tokens, heads, 128), F32),
                pltpu.VMEM((tokens, heads, 128), F32),
                pltpu.VMEM((d_loc,), F32),
                pltpu.VMEM((top, tokens), jnp.int32),
                pltpu.VMEM((top, tokens), jnp.int32),
                pltpu.VMEM((top, tokens), F32),
                pltpu.VMEM((d_loc,), F32),
                pltpu.VMEM((1, lat), F32),
                pltpu.SMEM((tokens,), jnp.int32),
                dma((7,)),
                pltpu.SemaphoreType.REGULAR((n_ep,)),
                dma((6,)),
                dma((3,)),
                dma((n_tp,)),
                dma((n_tp,)),
                dma((n_tp,)),
                dma((n_tp,)),
                dma((n_tp, tokens // 2)),
                dma((n_tp, tokens // 2)),
                dma((experts, n_tp)),
                dma((experts, n_tp)),
                dma((experts, max(2, n_tp))),
                dma((experts, max(2, n_tp))),
                dma((n_tp,)),
                dma((n_tp,)),
                dma((n_tp,)),
                dma((n_tp,)),
            ],
            compiler_params=pltpu.CompilerParams(
                collective_id=0, has_side_effects=True, vmem_limit_bytes=60 * 1024 * 1024
            ),
        )(
            hidden,
            moe_gain,
            expert_ids.T,
            slots.T,
            affinity.T,
            w_gate,
            w_up,
            w_down,
            attn_gain,
            w_dkv.T,
            kv_gain[None],
            queries,
            cache.reshape(tokens // 2, 2, span, kvc),
            lengths,
        )

    return jax.shard_map(
        local,
        mesh=mesh,
        in_specs=(
            P(("grp", "ep", "mb"), "tp"),
            P("tp"),
            P(("grp", "ep", "mb"), None),
            P(("grp", "ep", "mb"), None),
            P(("grp", "ep", "mb"), None),
            P(("ep", "mb"), None, "tp"),
            P(("ep", "mb"), None, "tp"),
            P(("ep", "mb"), "tp", None),
            P("tp"),
            P("tp", None),
            P(),
            P(("grp", "ep", "mb"), "tp", None),
            P(("grp", "ep", "mb"), "tp", None),
            P(("grp", "ep", "mb")),
        ),
        out_specs=(P(("grp", "ep", "mb"), "tp"), P(("grp", "ep", "mb"), "tp", None)),
        check_vma=False,
    )
```

```python
import functools

import jax
import jax.numpy as jnp
from jax import lax
from jax.experimental import pallas as pl
from jax.experimental.pallas import tpu as pltpu
from jax.sharding import PartitionSpec as P

CAP = 8
AHEAD = 3
epsilon = 1e-06
route_scale = 2.5
score_scale = 192.0 ** (-0.5)
STOPS = (1, 2, 4, 6)
MESH = pl.DeviceIdType.MESH
F32 = jnp.float32
BF16 = jnp.bfloat16


def up(value, step):
    return -(-value // step) * step


def split3(value, width):
    high = value.astype(BF16)
    rest = value - high.astype(F32)
    mid = rest.astype(BF16)
    low = (rest - mid.astype(F32)).astype(BF16)
    lane = lax.broadcasted_iota(jnp.int32, (value.shape[0], width), 1)
    parts = jnp.where(lane == 1, mid.astype(F32), jnp.where(lane == 2, low.astype(F32), 0.0))
    return jnp.where(lane == 0, high.astype(F32), parts).astype(BF16)


def kernel(
    n_tp,
    n_ep,
    n_mb,
    hidden,
    moe_gain_in,
    ids_in,
    slots_in,
    affinity_in,
    w_gate,
    w_up,
    w_down,
    attn_gain_in,
    w_dkv,
    kv_gain_in,
    queries,
    cache,
    lengths_in,
    next_out,
    latent_out,
    hid_all,
    gain_all,
    send,
    arrived,
    wg,
    wu,
    wd,
    wk,
    ret_send,
    ret,
    tsum,
    rs_send,
    rs_recv,
    key_send,
    key_recv,
    q_buf,
    kv_buf,
    rope_in,
    acc,
    peaks,
    masses,
    keys,
    old_part,
    own_part,
    moe_gain,
    ids,
    slots,
    affinity,
    attn_gain,
    kv_gain,
    lengths,
    small_sem,
    near_sem,
    load_sem,
    kv_load_sem,
    hid_ssem,
    hid_rsem,
    gain_ssem,
    gain_rsem,
    kv_ssem,
    kv_rsem,
    row_ssem,
    row_rsem,
    ret_ssem,
    ret_rsem,
    rs_ssem,
    rs_rsem,
    key_ssem,
    key_rsem,
):
    experts = n_ep * n_mb
    tokens, d_loc = hidden.shape
    d_all = d_loc * n_tp
    lat = kv_gain.shape[1]
    pairs, span_len, kvc = cache.shape[0], cache.shape[2], cache.shape[3]
    tp = lax.axis_index("tp")
    staged = 1 < n_ep <= 4
    me = lax.axis_index("ep") * n_mb + lax.axis_index("mb")

    def tp_id(step):
        return lax.rem(tp + step, n_tp)

    def ex_id(step):
        return lax.rem(me + step, experts)

    def ex_dev(index):
        return {"ep": index // n_mb, "mb": lax.rem(index, n_mb)}
    local = [
        pltpu.make_async_copy(hidden, hid_all.at[tp], load_sem.at[0]),
        pltpu.make_async_copy(queries, q_buf, load_sem.at[1]),
        pltpu.make_async_copy(w_gate.at[0], wg, load_sem.at[2]),
        pltpu.make_async_copy(w_up.at[0], wu, load_sem.at[3]),
        pltpu.make_async_copy(w_down.at[0], wd, load_sem.at[4]),
        pltpu.make_async_copy(w_dkv, wk, load_sem.at[5]),
    ]
    rope = kvc - lat
    lanes = kv_buf.shape[3]
    kv_loads = [
        pltpu.make_async_copy(
            cache.at[:, i, :, :lat], kv_buf.at[:, tp, :, i * lat : (i + 1) * lat], kv_load_sem.at[i]
        )
        for i in range(2)
    ]
    kv_loads.append(pltpu.make_async_copy(cache.at[:, :, :, lat:], rope_in, kv_load_sem.at[2]))
    small = [
        pltpu.make_async_copy(src, dst, small_sem.at[i])
        for i, (src, dst) in enumerate(
            (
                (slots_in, slots),
                (ids_in, ids),
                (affinity_in, affinity),
                (moe_gain_in, moe_gain),
                (attn_gain_in, attn_gain),
                (kv_gain_in, kv_gain),
                (lengths_in, lengths),
            )
        )
    ]
    for copy in small[:4]:
        copy.start()
    local[0].start()
    for copy in kv_loads:
        copy.start()
    for copy in small[4:]:
        copy.start()

    ep, mb = lax.axis_index("ep"), lax.axis_index("mb")
    barrier = pltpu.get_barrier_semaphore()

    def hello(sem, ids):
        pl.semaphore_signal(sem, inc=1, device_id=ids, device_id_type=MESH)

    for step in range(1, n_tp):
        hello(barrier, {"tp": tp_id(step)})
    if staged:
        for step in range(1, n_mb):
            hello(barrier, {"mb": lax.rem(mb + step, n_mb)})
        for far in range(1, n_ep):

            @pl.when(ep + far < n_ep)
            def _():
                for m in range(n_mb):
                    hello(barrier, {"ep": ep + far, "mb": m})

        greeted = n_tp - 1 + n_mb - 1 + n_mb * ep
    else:
        for step in range(1, experts):
            hello(barrier, ex_dev(ex_id(step)))
        greeted = n_tp - 1 + experts - 1

    def tp_copy(src, dst, ssem, rsem, step):
        return pltpu.make_async_remote_copy(
            src_ref=src,
            dst_ref=dst,
            send_sem=ssem,
            recv_sem=rsem,
            device_id={"tp": tp_id(step)},
            device_id_type=MESH,
        )

    def arrival(dst, rsem):
        return pltpu.make_async_copy(dst, dst, rsem)

    def cache_copy(t, step):
        return tp_copy(
            kv_buf.at[t, tp], kv_buf.at[t, tp], kv_ssem.at[0], kv_rsem.at[t], step
        )

    def feed(t):
        for step in range(1, n_tp):
            cache_copy(t, step).start()

    def row_copy(peer, block):
        return pltpu.make_async_remote_copy(
            src_ref=send.at[peer, block],
            dst_ref=arrived.at[me, block],
            send_sem=row_ssem.at[0],
            recv_sem=row_rsem.at[block],
            device_id=ex_dev(peer),
            device_id_type=MESH,
        )

    def ship_to(ep_index, block):
        for m in range(n_mb):
            row_copy(ep_index * n_mb + m, block).start()

    def ship_near(block):
        arrived[me, block] = send[me, block]
        for step in range(1, n_mb):
            row_copy(ep * n_mb + lax.rem(mb + step, n_mb), block).start()

    def ship(block):
        ship_near(block)
        for far in range(1, n_ep):
            pl.when(ep >= far)(functools.partial(ship_to, ep - far, block))
            pl.when(ep + far < n_ep)(functools.partial(ship_to, ep + far, block))
    small[3].wait()
    gain_all[tp] = moe_gain[...].reshape(1, d_loc)
    local[0].wait()
    pl.semaphore_wait(barrier, greeted)
    for step in range(1, n_tp):
        for src, dst, ssem, rsem in (
            (hid_all.at[tp], hid_all, hid_ssem, hid_rsem),
            (gain_all.at[tp], gain_all, gain_ssem, gain_rsem),
        ):
            tp_copy(src, dst.at[tp], ssem.at[0], rsem.at[0], step).start()
    if staged:
        for far in range(1, n_ep):

            @pl.when(ep >= far)
            def _():
                for m in range(n_mb):
                    hello(near_sem.at[far], {"ep": ep - far, "mb": m})

    for copy in small[:3]:
        copy.wait()
    kept = slots[...] < CAP
    target = jnp.where(kept, ids[...] * CAP + slots[...], -1)
    rows = experts * CAP
    iota = lax.broadcasted_iota(jnp.int32, (rows, tokens), 0)
    dispatch = jnp.zeros((rows, tokens), F32)
    for k in range(ids.shape[0]):
        dispatch = jnp.where(target[k : k + 1] == iota, 1.0, dispatch)
    dispatch = dispatch.astype(BF16)

    def pick(block):
        picked = jnp.dot(dispatch, hid_all[block], preferred_element_type=F32)
        send[:, block] = picked.reshape(experts, CAP, d_loc).astype(BF16)

    pick(tp)
    if staged:
        ship_near(tp)
        for far in range(1, n_ep):
            pl.when(ep >= far)(functools.partial(ship_to, ep - far, tp))
    else:
        ship(tp)
    for copy in kv_loads:
        copy.wait()
    kv_buf[:, tp, :, 2 * lat : 2 * lat + 2 * rope] = jnp.concatenate(
        [rope_in[:, 0], rope_in[:, 1]], -1
    )
    for t in range(AHEAD):
        feed(t)
    for copy in local[1:]:
        copy.start()
    aff = affinity[...]
    weight = route_scale * aff / jnp.sum(aff, 0, keepdims=True) * kept.astype(F32)
    combine = jnp.zeros((rows, tokens), F32)
    for k in range(ids.shape[0]):
        combine = jnp.where(target[k : k + 1] == iota, weight[k : k + 1], combine)
    combine = combine.T
    high = combine.astype(BF16)
    rest = combine - high.astype(F32)
    mid = rest.astype(BF16)
    low = (rest - mid.astype(F32)).astype(BF16)
    combine3 = jnp.concatenate([high, mid, low], 0)
    if staged:
        for far in range(1, n_ep):

            @pl.when(ep + far < n_ep)
            def _():
                pl.semaphore_wait(near_sem.at[far], n_mb)
                ship_to(ep + far, tp)
    arrival(hid_all.at[pl.ds(0, n_tp - 1)], hid_rsem.at[0]).wait()
    arrival(gain_all.at[pl.ds(0, n_tp - 1)], gain_rsem.at[0]).wait()
    for turn in range(1, n_tp):
        pick(tp_id(turn))
        ship(tp_id(turn))

    local[1].wait()
    heads = queries.shape[1]
    total_len = n_tp * span_len

    def attend(first, last):
        def body(p, carry):
            arrival(kv_buf.at[p, pl.ds(0, n_tp - 1)], kv_rsem.at[p]).wait()

            @pl.when(p + AHEAD < pairs)
            def _():
                feed(p + AHEAD)

            ropes = kv_buf[p, :, :, 2 * lat :].reshape(total_len, lanes - 2 * lat)
            gap = jnp.zeros((heads, rope), BF16)
            turned = [q_buf[2 * p][:, lat:], gap, gap, q_buf[2 * p + 1][:, lat:]]
            turned = jnp.concatenate(
                [jnp.concatenate(turned[:2], 1), jnp.concatenate(turned[2:], 1)], 0
            )
            turned = lax.dot_general(
                turned, ropes, (((1,), (1,)), ((), ())), preferred_element_type=F32
            )
            for i in range(2):
                t = 2 * p + i
                block = kv_buf[p, :, :, i * lat : (i + 1) * lat].reshape(total_len, lat)
                scores = lax.dot_general(
                    q_buf[t][:, :lat], block, (((1,), (1,)), ((), ())), preferred_element_type=F32
                )
                scores = (scores + turned[i * heads : (i + 1) * heads]) * score_scale
                live = lax.broadcasted_iota(jnp.int32, (heads, total_len), 1) < lengths[t]
                scores = jnp.where(live, scores, -1e30)
                peak = jnp.max(scores, -1, keepdims=True)
                prob = jnp.where(live, jnp.exp(scores - peak), 0.0)
                mass = jnp.sum(prob, -1, keepdims=True)
                acc[t] = jnp.dot(prob.astype(BF16), block, preferred_element_type=F32)
                peaks[t] = jnp.broadcast_to(peak, (heads, 128))
                masses[t] = jnp.broadcast_to(mass, (heads, 128))
            return carry

        lax.fori_loop(first, last, body, 0)

    for copy in small[4:]:
        copy.wait()
    stops = [pairs * n // 8 for n in STOPS]
    attend(0, stops[0])
    local[2].wait()
    local[3].wait()
    gate = jnp.zeros((rows, wg.shape[1]), F32)
    upper = jnp.zeros((rows, wg.shape[1]), F32)
    square = jnp.zeros((rows, 1), F32)
    for turn in range(n_tp):
        b = tp_id(turn)
        if turn == n_tp - 1:
            attend(stops[0], stops[1])
        arrival(arrived.at[pl.ds(0, experts - 1), b], row_rsem.at[b]).wait()
        wide = arrived[:, b].astype(F32).reshape(rows, d_loc)
        square = square + jnp.sum(wide * wide, -1, keepdims=True)
        block = (wide * gain_all[b]).astype(BF16)
        deep = pl.ds(pl.multiple_of(b * d_loc, d_loc & -d_loc), d_loc)
        gate = gate + jnp.dot(block, wg[deep], preferred_element_type=F32)
        upper = upper + jnp.dot(block, wu[deep], preferred_element_type=F32)
    scale = lax.rsqrt(square / d_all + epsilon)
    gate = gate * scale
    upper = upper * scale
    units = (gate / (1.0 + jnp.exp(-gate)) * upper).astype(BF16)
    local[4].wait()
    width = 512 if d_all % 512 == 0 else 128
    aligned = d_loc % 128 == 0
    if aligned:
        width = next(w for w in (896, 512, 384, 256, 128) if d_loc % w == 0)
        pieces = [
            (pl.multiple_of(tp_id(turn) * d_loc, 128), d_loc) for turn in (*range(1, n_tp), 0)
        ]
    else:
        middle = d_all // width // 2 * width
        pieces = [(0, middle), (middle, d_all - middle)]

    def columns(start, size):
        return pl.ds(pl.multiple_of(start, 128), size)

    for h, (first, size) in enumerate(pieces):
        for c in range(0, size, width):
            part = jnp.dot(units, wd[:, columns(first + c, width)], preferred_element_type=F32)
            ret_send[:, :, columns(first + c, width)] = part.reshape(
                experts, CAP, width
            ).astype(BF16)
        for step in range(1, experts):
            peer = ex_id(step)
            copy = pltpu.make_async_remote_copy(
                src_ref=ret_send.at[peer, :, columns(first, size)],
                dst_ref=ret.at[me, :, columns(first, size)],
                send_sem=ret_ssem.at[0],
                recv_sem=ret_rsem.at[h],
                device_id=ex_dev(peer),
                device_id_type=MESH,
            )
            copy.start()
    ret[me] = ret_send[me]

    def exchange(step):
        tp_copy(
            rs_send.at[tp_id(step)], rs_recv.at[tp], rs_ssem.at[0], rs_rsem.at[0], step
        ).start()

    for h, (first, size) in enumerate(pieces):
        if h < 2:
            attend(stops[h + 1], stops[h + 2])
        arrival(
            ret.at[pl.ds(0, experts - 1), :, columns(first, size)], ret_rsem.at[h]
        ).wait()
        for c in range(0, size, width):
            block = ret[:, :, columns(first + c, width)].astype(F32)
            block = block.reshape(rows, width).astype(BF16)
            part = jnp.dot(combine3, block, preferred_element_type=F32)
            part = part[:tokens] + (part[tokens : 2 * tokens] + part[2 * tokens : 3 * tokens])
            if aligned:
                rs_send[tp_id(h + 1), :, c : c + width] = part.astype(BF16)
            else:
                tsum[:, columns(first + c, width)] = part
        if aligned and h < n_tp - 1:
            exchange(h + 1)
    if not aligned:
        for p in range(n_tp):
            rs_send[p] = tsum[:, p * d_loc : (p + 1) * d_loc].astype(BF16)
        for step in range(1, n_tp):
            exchange(step)
    rs_recv[tp] = rs_send[tp]
    local[5].wait()
    arrival(rs_recv.at[pl.ds(0, n_tp - 1)], rs_rsem.at[0]).wait()
    moe = rs_recv[0].astype(F32)
    for p in range(1, n_tp):
        moe = moe + rs_recv[p].astype(F32)
    next_hidden = (hid_all[tp].astype(F32) + moe).astype(BF16)
    next_out[...] = next_hidden
    next_wide = next_hidden.astype(F32)
    square = jnp.sum(next_wide * next_wide, -1, keepdims=True)
    scaled = (next_wide * attn_gain[...].reshape(1, d_loc)).astype(BF16)
    kvp = up(kvc + 3, 128)
    tail = kvp - kvc
    part = lax.dot_general(
        scaled, wk[...], (((1,), (1,)), ((), ())), preferred_element_type=F32
    )
    key_send[:, :kvc] = part.astype(BF16)
    key_send[:, kvc:kvp] = split3(square, tail)
    for step in range(1, n_tp):
        tp_copy(key_send, key_recv.at[tp], key_ssem.at[0], key_rsem.at[0], step).start()
    key_recv[tp] = key_send[...]
    attend(stops[3], pairs)
    half = (kvc - lat) // 2
    lane = lax.broadcasted_iota(jnp.int32, (tokens, 2 * half), 1)
    pair = jnp.where(lane < half, lane, lane - half).astype(F32)
    freq = jnp.exp(pair * (-9.210340371976184 / half))
    row_id = lax.broadcasted_iota(jnp.int32, (tokens, 2 * half), 0)
    place = jnp.zeros((tokens, 2 * half), F32)
    for t in range(tokens):
        place = jnp.where(row_id == t, lengths[t].astype(F32), place)
    angle = place * freq
    cos_table = jnp.cos(angle)
    sin_table = jnp.where(lane < half, -1.0, 1.0) * jnp.sin(angle)
    arrival(key_recv.at[pl.ds(0, n_tp - 1)], key_rsem.at[0]).wait()
    total = key_recv[0].astype(F32)
    for p in range(1, n_tp):
        total = total + key_recv[p].astype(F32)
    square = jnp.sum(total[:, kvc:], -1, keepdims=True)
    down = total * lax.rsqrt(square / d_all + epsilon)
    latent = down[:, :lat]
    latent = (
        latent
        * lax.rsqrt(jnp.mean(latent * latent, -1, keepdims=True) + epsilon)
        * kv_gain[...]
    )
    turn = down[:, lat:kvc]
    swapped = jnp.concatenate([turn[:, half:], turn[:, :half]], 1)
    turn = turn * cos_table + swapped * sin_table
    keys[:, :lat] = latent.astype(BF16)
    keys[:, lat:kvc] = turn.astype(BF16)
    rows_all = tokens * heads
    own = lax.dot_general(
        q_buf[...].reshape(rows_all, kvc),
        keys[...],
        (((1,), (1,)), ((), ())),
        preferred_element_type=F32,
    )
    owner = lax.broadcasted_iota(jnp.int32, (rows_all, tokens), 0) // heads
    mine = owner == lax.broadcasted_iota(jnp.int32, (rows_all, tokens), 1)
    own = jnp.sum(jnp.where(mine, own, 0.0), -1, keepdims=True) * score_scale
    own = jnp.broadcast_to(own, (rows_all, 128))
    peak = peaks[...].reshape(rows_all, 128)
    top = jnp.maximum(peak, own)
    factor = jnp.exp(peak - top)
    own_prob = jnp.exp(own - top)
    inverse = 1.0 / (masses[...].reshape(rows_all, 128) * factor + own_prob)
    old_part[...] = (factor * inverse).reshape(tokens, heads, 128)
    own_part[...] = (own_prob.astype(BF16).astype(F32) * inverse).reshape(tokens, heads, 128)
    for t in range(tokens):
        for c in range(0, lat, 128):
            value = acc[t, :, c : c + 128] * old_part[t]
            key = keys[t : t + 1, c : c + 128].astype(F32)
            latent_out[t, :, c : c + 128] = (value + own_part[t] * key).astype(BF16)
    for sent, sem in (
        (send.at[pl.ds(0, experts - 1)], row_ssem),
        (ret_send.at[pl.ds(0, experts - 1)], ret_ssem),
        (hid_all.at[pl.ds(0, n_tp - 1)], hid_ssem),
        (gain_all.at[pl.ds(0, n_tp - 1)], gain_ssem),
        (rs_send.at[pl.ds(0, n_tp - 1)], rs_ssem),
        (key_recv.at[pl.ds(0, n_tp - 1)], key_ssem),
        (kv_buf.at[:, pl.ds(0, n_tp - 1)], kv_ssem),
    ):
        arrival(sent, sem.at[0]).wait()


def put_out(hidden_in, latent_in, hidden_out, latent_out, sem):
    copies = [
        pltpu.make_async_copy(latent_in, latent_out, sem.at[0]),
        pltpu.make_async_copy(hidden_in, hidden_out, sem.at[1]),
    ]
    for copy in copies:
        copy.start()
    for copy in copies:
        copy.wait()


def solution(mesh):
    n_tp, n_ep, n_mb = mesh.shape["tp"], mesh.shape["ep"], mesh.shape["mb"]
    experts = n_ep * n_mb

    def local(
        hidden,
        moe_gain,
        expert_ids,
        slots,
        affinity,
        w_gate,
        w_up,
        w_down,
        attn_gain,
        w_dkv,
        kv_gain,
        queries,
        cache,
        lengths,
    ):
        tokens, d_loc = hidden.shape
        d_all = d_loc * n_tp
        heads, kvc = queries.shape[1:]
        span = cache.shape[1]
        lat = kv_gain.shape[0]
        hid_dim = w_gate.shape[2]
        top = expert_ids.shape[1]
        wide = up(kvc + 3, 128)
        any_space = pl.BlockSpec(memory_space=pl.ANY)
        vmem = pl.BlockSpec(memory_space=pltpu.VMEM)
        dma = pltpu.SemaphoreType.DMA
        results = pl.pallas_call(
            functools.partial(kernel, n_tp, n_ep, n_mb),
            out_shape=(
                pltpu.VMEM((tokens, d_loc), BF16),
                pltpu.VMEM((tokens, heads, lat), BF16),
            ),
            in_specs=[any_space] * 14,
            out_specs=(vmem, vmem),
            scratch_shapes=[
                pltpu.VMEM((n_tp, tokens, d_loc), BF16),
                pltpu.VMEM((n_tp, 1, d_loc), F32),
                pltpu.VMEM((experts, n_tp, CAP, d_loc), BF16),
                pltpu.VMEM((experts, n_tp, CAP, d_loc), BF16),
                pltpu.VMEM((d_all, hid_dim), BF16),
                pltpu.VMEM((d_all, hid_dim), BF16),
                pltpu.VMEM((hid_dim, d_all), BF16),
                pltpu.VMEM((kvc, d_loc), BF16),
                pltpu.VMEM((experts, CAP, d_all), BF16),
                pltpu.VMEM((experts, CAP, d_all), BF16),
                pltpu.VMEM((tokens, d_all), F32),
                pltpu.VMEM((n_tp, tokens, d_loc), BF16),
                pltpu.VMEM((n_tp, tokens, d_loc), BF16),
                pltpu.VMEM((tokens, wide), BF16),
                pltpu.VMEM((n_tp, tokens, wide), BF16),
                pltpu.VMEM((tokens, heads, kvc), BF16),
                pltpu.VMEM((tokens // 2, n_tp, span, up(2 * kvc, 128)), BF16),
                pltpu.VMEM((tokens // 2, 2, span, kvc - lat), BF16),
                pltpu.VMEM((tokens, heads, lat), F32),
                pltpu.VMEM((tokens, heads, 128), F32),
                pltpu.VMEM((tokens, heads, 128), F32),
                pltpu.VMEM((tokens, kvc), BF16),
                pltpu.VMEM((tokens, heads, 128), F32),
                pltpu.VMEM((tokens, heads, 128), F32),
                pltpu.VMEM((d_loc,), F32),
                pltpu.VMEM((top, tokens), jnp.int32),
                pltpu.VMEM((top, tokens), jnp.int32),
                pltpu.VMEM((top, tokens), F32),
                pltpu.VMEM((d_loc,), F32),
                pltpu.VMEM((1, lat), F32),
                pltpu.SMEM((tokens,), jnp.int32),
                dma((7,)),
                pltpu.SemaphoreType.REGULAR((n_ep,)),
                dma((6,)),
                dma((3,)),
                dma((1,)),
                dma((1,)),
                dma((1,)),
                dma((1,)),
                dma((1,)),
                dma((tokens // 2,)),
                dma((1,)),
                dma((n_tp,)),
                dma((1,)),
                dma((max(2, n_tp),)),
                dma((1,)),
                dma((1,)),
                dma((1,)),
                dma((1,)),
            ],
            compiler_params=pltpu.CompilerParams(
                collective_id=0, has_side_effects=True, vmem_limit_bytes=60 * 1024 * 1024
            ),
        )(
            hidden,
            moe_gain,
            expert_ids.T,
            slots.T,
            affinity.T,
            w_gate,
            w_up,
            w_down,
            attn_gain,
            w_dkv.T,
            kv_gain[None],
            queries,
            cache.reshape(tokens // 2, 2, span, kvc),
            lengths,
        )
        return pl.pallas_call(
            put_out,
            out_shape=(
                jax.ShapeDtypeStruct((tokens, d_loc), BF16),
                jax.ShapeDtypeStruct((tokens, heads, lat), BF16),
            ),
            in_specs=[vmem, vmem],
            out_specs=(any_space, any_space),
            scratch_shapes=[dma((2,))],
        )(*[pltpu.with_memory_space_constraint(r, pltpu.VMEM) for r in results])

    return jax.shard_map(
        local,
        mesh=mesh,
        in_specs=(
            P(("grp", "ep", "mb"), "tp"),
            P("tp"),
            P(("grp", "ep", "mb"), None),
            P(("grp", "ep", "mb"), None),
            P(("grp", "ep", "mb"), None),
            P(("ep", "mb"), None, "tp"),
            P(("ep", "mb"), None, "tp"),
            P(("ep", "mb"), "tp", None),
            P("tp"),
            P("tp", None),
            P(),
            P(("grp", "ep", "mb"), "tp", None),
            P(("grp", "ep", "mb"), "tp", None),
            P(("grp", "ep", "mb")),
        ),
        out_specs=(P(("grp", "ep", "mb"), "tp"), P(("grp", "ep", "mb"), "tp", None)),
        check_vma=False,
    )
```

```python
import functools

import jax
import jax.numpy as jnp
from jax import lax
from jax.experimental import pallas as pl
from jax.experimental.pallas import tpu as pltpu
from jax.sharding import PartitionSpec as P

CAP = 8
AHEAD = 4
epsilon = 1e-06
route_scale = 2.5
score_scale = 192.0 ** (-0.5)
STOPS = (1, 4, 6, 8)
MESH = pl.DeviceIdType.MESH
F32 = jnp.float32
BF16 = jnp.bfloat16


def up(value, step):
    return -(-value // step) * step


def split3(value, width):
    high = value.astype(BF16)
    rest = value - high.astype(F32)
    mid = rest.astype(BF16)
    low = (rest - mid.astype(F32)).astype(BF16)
    lane = lax.broadcasted_iota(jnp.int32, (value.shape[0], width), 1)
    parts = jnp.where(lane == 1, mid.astype(F32), jnp.where(lane == 2, low.astype(F32), 0.0))
    return jnp.where(lane == 0, high.astype(F32), parts).astype(BF16)


def kernel(
    n_tp,
    n_ep,
    n_mb,
    hidden,
    moe_gain_in,
    ids_in,
    slots_in,
    affinity_in,
    w_gate,
    w_up,
    w_down,
    attn_gain_in,
    w_dkv,
    kv_gain_in,
    queries,
    cache,
    lengths_in,
    next_out,
    latent_out,
    hid_all,
    gain_all,
    send,
    arrived,
    wg,
    wu,
    wd,
    wk,
    ret_send,
    ret,
    tsum,
    rs_send,
    rs_recv,
    key_send,
    key_recv,
    q_all,
    q_rope,
    k_lat,
    k_rope,
    k_pad,
    o_send,
    o_recv,
    stat_send,
    stat_recv,
    mid_units,
    mid_key,
    gain_row,
    acc,
    peaks,
    masses,
    keys,
    old_part,
    own_part,
    moe_gain,
    ids,
    slots,
    affinity,
    attn_gain,
    kv_gain,
    lengths,
    small_sem,
    near_sem,
    load_sem,
    q_sem,
    kv_load_sem,
    hid_ssem,
    hid_rsem,
    gain_ssem,
    gain_rsem,
    q_ssem,
    q_rsem,
    o_ssem,
    o_rsem,
    stat_ssem,
    stat_rsem,
    row_ssem,
    row_rsem,
    ret_ssem,
    ret_rsem,
    rs_ssem,
    rs_rsem,
    key_ssem,
    key_rsem,
):
    experts = n_ep * n_mb
    tokens, d_loc = hidden.shape
    d_all = d_loc * n_tp
    lat = kv_gain.shape[1]
    pairs, span_len, kvc = cache.shape[0], cache.shape[2], cache.shape[3]
    tp = lax.axis_index("tp")
    staged = 1 < n_ep <= 4
    me = lax.axis_index("ep") * n_mb + lax.axis_index("mb")

    def tp_id(step):
        return lax.rem(tp + step, n_tp)

    def ex_id(step):
        return lax.rem(me + step, experts)

    def ex_dev(index):
        return {"ep": index // n_mb, "mb": lax.rem(index, n_mb)}
    local = [
        pltpu.make_async_copy(hidden, hid_all.at[tp], load_sem.at[0]),
        pltpu.make_async_copy(w_gate.at[0], wg, load_sem.at[2]),
        pltpu.make_async_copy(w_up.at[0], wu, load_sem.at[3]),
        pltpu.make_async_copy(w_down.at[0], wd, load_sem.at[4]),
        pltpu.make_async_copy(w_dkv, wk, load_sem.at[5]),
    ]
    rope = kvc - lat
    q_loads = [
        pltpu.make_async_copy(
            queries.at[:, i, :, :lat], q_all.at[:, 0, :, i * lat : (i + 1) * lat], q_sem.at[i]
        )
        for i in range(2)
    ]
    q_loads.append(pltpu.make_async_copy(queries.at[:, :, :, lat:], q_rope, q_sem.at[2]))
    kv_loads = [
        pltpu.make_async_copy(cache.at[:, :, :, :lat], k_lat, kv_load_sem.at[0]),
        pltpu.make_async_copy(cache.at[:, :, :, lat:], k_rope, kv_load_sem.at[1]),
    ]
    small = [
        pltpu.make_async_copy(src, dst, small_sem.at[i])
        for i, (src, dst) in enumerate(
            (
                (slots_in, slots),
                (ids_in, ids),
                (affinity_in, affinity),
                (moe_gain_in, moe_gain),
                (attn_gain_in, attn_gain),
                (kv_gain_in, kv_gain),
                (lengths_in, lengths),
            )
        )
    ]
    for copy in small[:4]:
        copy.start()
    local[0].start()
    for copy in q_loads + kv_loads:
        copy.start()
    for copy in small[4:]:
        copy.start()

    ep, mb = lax.axis_index("ep"), lax.axis_index("mb")
    barrier = pltpu.get_barrier_semaphore()

    def hello(sem, ids):
        pl.semaphore_signal(sem, inc=1, device_id=ids, device_id_type=MESH)

    for step in range(1, n_tp):
        hello(barrier, {"tp": tp_id(step)})
    if staged:
        for step in range(1, n_mb):
            hello(barrier, {"mb": lax.rem(mb + step, n_mb)})
        for far in range(1, n_ep):

            @pl.when(ep + far < n_ep)
            def _():
                for m in range(n_mb):
                    hello(barrier, {"ep": ep + far, "mb": m})

        greeted = n_tp - 1 + n_mb - 1 + n_mb * ep
    else:
        for step in range(1, experts):
            hello(barrier, ex_dev(ex_id(step)))
        greeted = n_tp - 1 + experts - 1

    def tp_copy(src, dst, ssem, rsem, step):
        return pltpu.make_async_remote_copy(
            src_ref=src,
            dst_ref=dst,
            send_sem=ssem,
            recv_sem=rsem,
            device_id={"tp": tp_id(step)},
            device_id_type=MESH,
        )

    def arrival(dst, rsem):
        return pltpu.make_async_copy(dst, dst, rsem)

    def feed(p):
        for step in range(1, n_tp):
            tp_copy(
                q_all.at[p, 0], q_all.at[p, n_tp - step], q_ssem.at[0], q_rsem.at[p], step
            ).start()

    def row_copy(peer, block):
        return pltpu.make_async_remote_copy(
            src_ref=send.at[peer, block],
            dst_ref=arrived.at[me, block],
            send_sem=row_ssem.at[0],
            recv_sem=row_rsem.at[block],
            device_id=ex_dev(peer),
            device_id_type=MESH,
        )

    def ship_to(ep_index, block):
        for m in range(n_mb):
            row_copy(ep_index * n_mb + m, block).start()

    def ship_near(block):
        arrived[me, block] = send[me, block]
        for step in range(1, n_mb):
            row_copy(ep * n_mb + lax.rem(mb + step, n_mb), block).start()

    def ship(block):
        ship_near(block)
        for far in range(1, n_ep):
            pl.when(ep >= far)(functools.partial(ship_to, ep - far, block))
            pl.when(ep + far < n_ep)(functools.partial(ship_to, ep + far, block))
    small[3].wait()
    gain_all[tp] = moe_gain[...].reshape(1, d_loc)
    local[0].wait()
    pl.semaphore_wait(barrier, greeted)
    for step in range(1, n_tp):
        for src, dst, ssem, rsem in (
            (hid_all.at[tp], hid_all, hid_ssem, hid_rsem),
            (gain_all.at[tp], gain_all, gain_ssem, gain_rsem),
        ):
            tp_copy(src, dst.at[tp], ssem.at[0], rsem.at[0], step).start()
    if staged:
        for far in range(1, n_ep):

            @pl.when(ep >= far)
            def _():
                for m in range(n_mb):
                    hello(near_sem.at[far], {"ep": ep - far, "mb": m})

    for copy in small[:3]:
        copy.wait()
    kept = slots[...] < CAP
    target = jnp.where(kept, ids[...] * CAP + slots[...], -1)
    rows = experts * CAP
    iota = lax.broadcasted_iota(jnp.int32, (rows, tokens), 0)
    dispatch = jnp.zeros((rows, tokens), F32)
    for k in range(ids.shape[0]):
        dispatch = jnp.where(target[k : k + 1] == iota, 1.0, dispatch)
    dispatch = dispatch.astype(BF16)

    def pick(block):
        picked = jnp.dot(dispatch, hid_all[block], preferred_element_type=F32)
        send[:, block] = picked.reshape(experts, CAP, d_loc).astype(BF16)

    pick(tp)
    if staged:
        ship_near(tp)
        for far in range(1, n_ep):
            pl.when(ep >= far)(functools.partial(ship_to, ep - far, tp))
    else:
        ship(tp)
    for copy in q_loads:
        copy.wait()
    q_all[:, 0, :, 2 * lat : 2 * kvc] = jnp.concatenate([q_rope[:, 0], q_rope[:, 1]], -1)
    for t in range(AHEAD):
        feed(t)
    for copy in local[1:]:
        copy.start()
    for copy in kv_loads:
        copy.wait()
    blank = jnp.zeros((pairs, span_len, rope), BF16)
    k_pad[:, :span_len] = jnp.concatenate([k_rope[:, 0], blank], -1)
    k_pad[:, span_len:] = jnp.concatenate([blank, k_rope[:, 1]], -1)
    stat_send[...] = jnp.zeros(stat_send.shape, F32)
    aff = affinity[...]
    weight = route_scale * aff / jnp.sum(aff, 0, keepdims=True) * kept.astype(F32)
    combine = jnp.zeros((rows, tokens), F32)
    for k in range(ids.shape[0]):
        combine = jnp.where(target[k : k + 1] == iota, weight[k : k + 1], combine)
    combine = combine.T
    high = combine.astype(BF16)
    rest = combine - high.astype(F32)
    mid = rest.astype(BF16)
    low = (rest - mid.astype(F32)).astype(BF16)
    combine3 = jnp.concatenate([high, mid, low], 0)
    if staged:
        for far in range(1, n_ep):

            @pl.when(ep + far < n_ep)
            def _():
                pl.semaphore_wait(near_sem.at[far], n_mb)
                ship_to(ep + far, tp)
    arrival(hid_all.at[pl.ds(0, n_tp - 1)], hid_rsem.at[0]).wait()
    arrival(gain_all.at[pl.ds(0, n_tp - 1)], gain_rsem.at[0]).wait()
    for turn in range(1, n_tp):
        pick(tp_id(turn))
        ship(tp_id(turn))

    heads = queries.shape[2]
    both = n_tp * heads
    keys_two = 2 * span_len
    lane = lax.broadcasted_iota(jnp.int32, (both, keys_two), 1)
    first_token = lane < span_len
    stat_lane = lax.broadcasted_iota(jnp.int32, stat_send.shape[1:], 1)

    def attend(first, last):
        def body(p, carry):
            arrival(q_all.at[p, pl.ds(1, n_tp - 1)], q_rsem.at[p]).wait()

            @pl.when(p + AHEAD < pairs)
            def _():
                feed(p + AHEAD)

            q = q_all[p].reshape(both, q_all.shape[3])
            block = k_lat[p].reshape(keys_two, lat)
            crossed = lax.dot_general(
                jnp.concatenate([q[:, :lat], q[:, lat : 2 * lat]], 0),
                block,
                (((1,), (1,)), ((), ())),
                preferred_element_type=F32,
            )
            turned = lax.dot_general(
                q[:, 2 * lat :], k_pad[p], (((1,), (1,)), ((), ())), preferred_element_type=F32
            )
            scores = (jnp.where(first_token, crossed[:both], crossed[both:]) + turned) * score_scale
            done = tp * span_len
            stop = jnp.where(first_token, lengths[2 * p] - done, lengths[2 * p + 1] - done + span_len)
            live = lane < stop
            scores = jnp.where(live, scores, -1e30)
            mine = [first_token, jnp.logical_not(first_token)]
            tops = [
                jnp.max(jnp.where(m, scores, -1e30), -1, keepdims=True).astype(BF16).astype(F32)
                for m in mine
            ]
            prob = jnp.where(live, jnp.exp(scores - jnp.where(first_token, tops[0], tops[1])), 0.0)
            parts = [jnp.where(m, prob, 0.0) for m in mine]
            sums = [jnp.sum(part, -1, keepdims=True) for part in parts]
            out = jnp.dot(
                jnp.concatenate(parts, 0).astype(BF16), block, preferred_element_type=F32
            )
            for i in range(2):
                acc[2 * p + i] = out[i * both : i * both + heads]
                peaks[2 * p + i] = jnp.broadcast_to(tops[i][:heads], (heads, 128))
                masses[2 * p + i] = jnp.broadcast_to(sums[i][:heads], (heads, 128))
            for step in range(1, n_tp):
                stat = stat_send[step]
                for i in range(2):
                    start = step * heads
                    o_send[step, p, i] = out[i * both + start : i * both + start + heads].astype(BF16)
                    base = 2 * (2 * p + i)
                    stat = jnp.where(stat_lane == base, tops[i][start : start + heads], stat)
                    stat = jnp.where(stat_lane == base + 1, sums[i][start : start + heads], stat)
                stat_send[step] = stat
                tp_copy(
                    o_send.at[step, p], o_recv.at[n_tp - step, p], o_ssem.at[0], o_rsem.at[0], step
                ).start()
            return carry

        lax.fori_loop(first, last, body, 0)

    for copy in small[4:]:
        copy.wait()
    gain_row[...] = attn_gain[...].reshape(1, d_loc)
    stops = [pairs * n // 8 for n in STOPS]
    attend(0, stops[0])
    local[1].wait()
    local[2].wait()
    square = jnp.zeros((rows, 1), F32)
    for turn in range(n_tp):
        b = tp_id(turn)
        if turn == n_tp - 1:
            attend(stops[0], stops[1])
        arrival(arrived.at[pl.ds(0, experts - 1), b], row_rsem.at[b]).wait()
        wide = arrived[:, b].astype(F32).reshape(rows, d_loc)
        square = square + jnp.sum(wide * wide, -1, keepdims=True)
        block = (wide * gain_all[b]).astype(BF16)
        deep = pl.ds(pl.multiple_of(b * d_loc, d_loc & -d_loc), d_loc)
        gate = jnp.dot(block, wg[deep], preferred_element_type=F32)
        upper = jnp.dot(block, wu[deep], preferred_element_type=F32)
        if turn > 0:
            gate = gate + mid_units[0]
            upper = upper + mid_units[1]
        if turn < n_tp - 1:
            mid_units[0] = gate
            mid_units[1] = upper
    scale = lax.rsqrt(square / d_all + epsilon)
    gate = gate * scale
    upper = upper * scale
    units = (gate / (1.0 + jnp.exp(-gate)) * upper).astype(BF16)
    local[3].wait()
    width = 512 if d_all % 512 == 0 else 128
    aligned = d_loc % 128 == 0
    if aligned:
        width = next(w for w in (896, 512, 384, 256, 128) if d_loc % w == 0)
        pieces = [(tp_id(turn) * d_loc, d_loc) for turn in range(1, n_tp)]
        pieces += [(tp * d_loc + c, width) for c in range(0, d_loc, width)]
    else:
        middle = d_all // width // 2 * width
        pieces = [(0, middle), (middle, d_all - middle)]

    def columns(start, size):
        return pl.ds(pl.multiple_of(start, 128), size)

    for h, (first, size) in enumerate(pieces):
        for c in range(0, size, width):
            part = jnp.dot(units, wd[:, columns(first + c, width)], preferred_element_type=F32)
            ret_send[:, :, columns(first + c, width)] = part.reshape(
                experts, CAP, width
            ).astype(BF16)
            for step in range(1, experts):
                peer = ex_id(step)
                pltpu.make_async_remote_copy(
                    src_ref=ret_send.at[peer, :, columns(first + c, width)],
                    dst_ref=ret.at[me, :, columns(first + c, width)],
                    send_sem=ret_ssem.at[0],
                    recv_sem=ret_rsem.at[h],
                    device_id=ex_dev(peer),
                    device_id_type=MESH,
                ).start()
    ret[me] = ret_send[me]

    def exchange(step):
        tp_copy(
            rs_send.at[step], rs_recv.at[n_tp - step], rs_ssem.at[0], rs_rsem.at[0], step
        ).start()

    def gather(h):
        first, size = pieces[h]
        arrival(
            ret.at[pl.ds(0, experts - 1), :, columns(first, size)], ret_rsem.at[h]
        ).wait()

    def mixed(start):
        block = ret[:, :, columns(start, width)].astype(F32)
        block = block.reshape(rows, width).astype(BF16)
        part = jnp.dot(combine3, block, preferred_element_type=F32)
        return part[:tokens] + (part[tokens : 2 * tokens] + part[2 * tokens : 3 * tokens])

    def send_stats():
        for step in range(1, n_tp):
            tp_copy(
                stat_send.at[step],
                stat_recv.at[n_tp - step],
                stat_ssem.at[0],
                stat_rsem.at[0],
                step,
            ).start()

    def renew(start, size, moe):
        span = pl.ds(start, size)
        fresh = (hid_all[tp, :, span].astype(F32) + moe).astype(BF16)
        next_out[:, span] = fresh
        fresh = fresh.astype(F32)
        scaled = (fresh * gain_row[...][:, start : start + size]).astype(BF16)
        part = lax.dot_general(
            scaled, wk[:, span], (((1,), (1,)), ((), ())), preferred_element_type=F32
        )
        return jnp.sum(fresh * fresh, -1, keepdims=True), part

    def others(start, size):
        total = rs_recv[1, :, pl.ds(start, size)].astype(F32)
        for step in range(2, n_tp):
            total = total + rs_recv[step, :, pl.ds(start, size)].astype(F32)
        return total
    attend(stops[1], stops[2])
    if aligned:
        for turn in range(1, n_tp):
            gather(turn - 1)
            for c in range(0, d_loc, width):
                rs_send[turn, :, c : c + width] = mixed(pieces[turn - 1][0] + c).astype(BF16)
            exchange(turn)
        attend(stops[2], stops[3])
        if stops[3] == pairs:
            send_stats()
        local[4].wait()
        square = jnp.zeros((tokens, 1), F32)
        for i, c in enumerate(range(0, d_loc, width)):
            gather(n_tp - 1 + i)
            part = mixed(tp * d_loc + c)
            if i == 0:
                arrival(rs_recv.at[pl.ds(1, n_tp - 1)], rs_rsem.at[0]).wait()
            more, part = renew(c, width, part + others(c, width))
            square = square + more
            if i > 0:
                part = part + mid_key[...]
            if c + width < d_loc:
                mid_key[...] = part
    else:
        for h in range(2):
            gather(h)
            first, size = pieces[h]
            for c in range(0, size, width):
                tsum[:, columns(first + c, width)] = mixed(first + c)
            if h == 0:
                attend(stops[2], stops[3])
        for p in range(n_tp):
            rs_send[lax.rem(p - tp + n_tp, n_tp)] = tsum[:, p * d_loc : (p + 1) * d_loc].astype(BF16)
        for step in range(1, n_tp):
            exchange(step)
        if stops[3] == pairs:
            send_stats()
        local[4].wait()
        arrival(rs_recv.at[pl.ds(1, n_tp - 1)], rs_rsem.at[0]).wait()
        square, part = renew(0, d_loc, rs_send[0].astype(F32) + others(0, d_loc))
    kvp = up(kvc + 3, 128)
    tail = kvp - kvc
    key_send[:, :kvc] = part.astype(BF16)
    key_send[:, kvc:kvp] = split3(square, tail)
    for step in range(1, n_tp):
        tp_copy(key_send, key_recv.at[tp], key_ssem.at[0], key_rsem.at[0], step).start()
    key_recv[tp] = key_send[...]
    if stops[3] < pairs:
        attend(stops[3], pairs)
        send_stats()
    half = (kvc - lat) // 2
    column = lax.broadcasted_iota(jnp.int32, (tokens, 2 * half), 1)
    pair = jnp.where(column < half, column, column - half).astype(F32)
    freq = jnp.exp(pair * (-9.210340371976184 / half))
    row_id = lax.broadcasted_iota(jnp.int32, (tokens, 2 * half), 0)
    place = jnp.zeros((tokens, 2 * half), F32)
    for t in range(tokens):
        place = jnp.where(row_id == t, lengths[t].astype(F32), place)
    angle = place * freq
    cos_table = jnp.cos(angle)
    sin_table = jnp.where(column < half, -1.0, 1.0) * jnp.sin(angle)
    arrival(o_recv.at[pl.ds(1, n_tp - 1)], o_rsem.at[0]).wait()
    arrival(stat_recv.at[pl.ds(1, n_tp - 1)], stat_rsem.at[0]).wait()
    for t in range(tokens):
        for step in range(1, n_tp):
            stat = stat_recv[step]
            far_top = jnp.sum(jnp.where(stat_lane == 2 * t, stat, 0.0), -1, keepdims=True)
            far_mass = jnp.sum(jnp.where(stat_lane == 2 * t + 1, stat, 0.0), -1, keepdims=True)
            near_top = peaks[t]
            top = jnp.maximum(near_top, far_top)
            near_factor = jnp.exp(near_top - top)
            far_factor = jnp.exp(far_top - top)
            peaks[t] = top
            masses[t] = masses[t] * near_factor + far_mass * far_factor
            for c in range(0, lat, 128):
                far = o_recv[step, t // 2, t % 2, :, c : c + 128].astype(F32) * far_factor
                acc[t, :, c : c + 128] = acc[t, :, c : c + 128] * near_factor + far
    arrival(key_recv.at[pl.ds(0, n_tp - 1)], key_rsem.at[0]).wait()
    total = key_recv[0].astype(F32)
    for p in range(1, n_tp):
        total = total + key_recv[p].astype(F32)
    square = jnp.sum(total[:, kvc:], -1, keepdims=True)
    down = total * lax.rsqrt(square / d_all + epsilon)
    latent = down[:, :lat]
    latent = (
        latent
        * lax.rsqrt(jnp.mean(latent * latent, -1, keepdims=True) + epsilon)
        * kv_gain[...]
    )
    turn = down[:, lat:kvc]
    swapped = jnp.concatenate([turn[:, half:], turn[:, :half]], 1)
    turn = turn * cos_table + swapped * sin_table
    keys[:, :lat] = latent.astype(BF16)
    turn = turn.astype(BF16)
    blank = jnp.zeros((tokens, rope), BF16)
    keys[:, lat:] = jnp.concatenate([turn, blank, blank, turn], 1)
    rows_all = tokens * heads
    own = jnp.concatenate(
        [
            jnp.concatenate(
                [
                    lax.dot_general(
                        q_all[p, 0, :, i * lat : (i + 1) * lat],
                        keys[:, :lat],
                        (((1,), (1,)), ((), ())),
                        preferred_element_type=F32,
                    )
                    + lax.dot_general(
                        q_all[p, 0, :, 2 * lat :],
                        keys[:, lat + 2 * rope * i : lat + 2 * rope * (i + 1)],
                        (((1,), (1,)), ((), ())),
                        preferred_element_type=F32,
                    )
                    for i in range(2)
                ],
                0,
            )
            for p in range(pairs)
        ],
        0,
    )
    owner = lax.broadcasted_iota(jnp.int32, (rows_all, tokens), 0) // heads
    mine = owner == lax.broadcasted_iota(jnp.int32, (rows_all, tokens), 1)
    own = jnp.sum(jnp.where(mine, own, 0.0), -1, keepdims=True) * score_scale
    own = jnp.broadcast_to(own, (rows_all, 128))
    peak = peaks[...].reshape(rows_all, 128)
    top = jnp.maximum(peak, own)
    factor = jnp.exp(peak - top)
    own_prob = jnp.exp(own - top)
    inverse = 1.0 / (masses[...].reshape(rows_all, 128) * factor + own_prob)
    old_part[...] = (factor * inverse).reshape(tokens, heads, 128)
    own_part[...] = (own_prob.astype(BF16).astype(F32) * inverse).reshape(tokens, heads, 128)
    for t in range(tokens):
        for c in range(0, lat, 128):
            value = acc[t, :, c : c + 128] * old_part[t]
            key = keys[t : t + 1, c : c + 128].astype(F32)
            latent_out[t, :, c : c + 128] = (value + own_part[t] * key).astype(BF16)
    for sent, sem in (
        (send.at[pl.ds(0, experts - 1)], row_ssem),
        (ret_send.at[pl.ds(0, experts - 1)], ret_ssem),
        (hid_all.at[pl.ds(0, n_tp - 1)], hid_ssem),
        (gain_all.at[pl.ds(0, n_tp - 1)], gain_ssem),
        (rs_send.at[pl.ds(1, n_tp - 1)], rs_ssem),
        (key_recv.at[pl.ds(0, n_tp - 1)], key_ssem),
        (q_all.at[:, pl.ds(0, n_tp - 1)], q_ssem),
        (o_send.at[pl.ds(1, n_tp - 1)], o_ssem),
        (stat_send.at[pl.ds(1, n_tp - 1)], stat_ssem),
    ):
        arrival(sent, sem.at[0]).wait()


def put_out(hidden_in, latent_in, hidden_out, latent_out, sem):
    copies = [
        pltpu.make_async_copy(latent_in, latent_out, sem.at[0]),
        pltpu.make_async_copy(hidden_in, hidden_out, sem.at[1]),
    ]
    for copy in copies:
        copy.start()
    for copy in copies:
        copy.wait()


def solution(mesh):
    n_tp, n_ep, n_mb = mesh.shape["tp"], mesh.shape["ep"], mesh.shape["mb"]
    experts = n_ep * n_mb

    def local(
        hidden,
        moe_gain,
        expert_ids,
        slots,
        affinity,
        w_gate,
        w_up,
        w_down,
        attn_gain,
        w_dkv,
        kv_gain,
        queries,
        cache,
        lengths,
    ):
        tokens, d_loc = hidden.shape
        d_all = d_loc * n_tp
        heads, kvc = queries.shape[1:]
        span = cache.shape[1]
        lat = kv_gain.shape[0]
        pairs = tokens // 2
        hid_dim = w_gate.shape[2]
        top = expert_ids.shape[1]
        wide = up(kvc + 3, 128)
        any_space = pl.BlockSpec(memory_space=pl.ANY)
        vmem = pl.BlockSpec(memory_space=pltpu.VMEM)
        dma = pltpu.SemaphoreType.DMA
        results = pl.pallas_call(
            functools.partial(kernel, n_tp, n_ep, n_mb),
            out_shape=(
                pltpu.VMEM((tokens, d_loc), BF16),
                pltpu.VMEM((tokens, heads, lat), BF16),
            ),
            in_specs=[any_space] * 14,
            out_specs=(vmem, vmem),
            scratch_shapes=[
                pltpu.VMEM((n_tp, tokens, d_loc), BF16),
                pltpu.VMEM((n_tp, 1, d_loc), F32),
                pltpu.VMEM((experts, n_tp, CAP, d_loc), BF16),
                pltpu.VMEM((experts, n_tp, CAP, d_loc), BF16),
                pltpu.VMEM((d_all, hid_dim), BF16),
                pltpu.VMEM((d_all, hid_dim), BF16),
                pltpu.VMEM((hid_dim, d_all), BF16),
                pltpu.VMEM((kvc, d_loc), BF16),
                pltpu.VMEM((experts, CAP, d_all), BF16),
                pltpu.VMEM((experts, CAP, d_all), BF16),
                pltpu.VMEM((tokens, d_all), F32),
                pltpu.VMEM((n_tp, tokens, d_loc), BF16),
                pltpu.VMEM((n_tp, tokens, d_loc), BF16),
                pltpu.VMEM((tokens, wide), BF16),
                pltpu.VMEM((n_tp, tokens, wide), BF16),
                pltpu.VMEM((pairs, n_tp, heads, 2 * kvc), BF16),
                pltpu.VMEM((pairs, 2, heads, kvc - lat), BF16),
                pltpu.VMEM((pairs, 2, span, lat), BF16),
                pltpu.VMEM((pairs, 2, span, kvc - lat), BF16),
                pltpu.VMEM((pairs, 2 * span, 2 * (kvc - lat)), BF16),
                pltpu.VMEM((n_tp, pairs, 2, heads, lat), BF16),
                pltpu.VMEM((n_tp, pairs, 2, heads, lat), BF16),
                pltpu.VMEM((n_tp, heads, up(2 * tokens, 128)), F32),
                pltpu.VMEM((n_tp, heads, up(2 * tokens, 128)), F32),
                pltpu.VMEM((2, experts * CAP, hid_dim), F32),
                pltpu.VMEM((tokens, kvc), F32),
                pltpu.VMEM((1, d_loc), F32),
                pltpu.VMEM((tokens, heads, lat), F32),
                pltpu.VMEM((tokens, heads, 128), F32),
                pltpu.VMEM((tokens, heads, 128), F32),
                pltpu.VMEM((tokens, lat + 4 * (kvc - lat)), BF16),
                pltpu.VMEM((tokens, heads, 128), F32),
                pltpu.VMEM((tokens, heads, 128), F32),
                pltpu.VMEM((d_loc,), F32),
                pltpu.VMEM((top, tokens), jnp.int32),
                pltpu.VMEM((top, tokens), jnp.int32),
                pltpu.VMEM((top, tokens), F32),
                pltpu.VMEM((d_loc,), F32),
                pltpu.VMEM((1, lat), F32),
                pltpu.SMEM((tokens,), jnp.int32),
                dma((7,)),
                pltpu.SemaphoreType.REGULAR((n_ep,)),
                dma((6,)),
                dma((3,)),
                dma((2,)),
                dma((1,)),
                dma((1,)),
                dma((1,)),
                dma((1,)),
                dma((1,)),
                dma((pairs,)),
                dma((1,)),
                dma((1,)),
                dma((1,)),
                dma((1,)),
                dma((1,)),
                dma((n_tp,)),
                dma((1,)),
                dma((max(2, n_tp - 1 + up(d_loc, 128) // 128),)),
                dma((1,)),
                dma((1,)),
                dma((1,)),
                dma((1,)),
            ],
            compiler_params=pltpu.CompilerParams(
                collective_id=0, has_side_effects=True, vmem_limit_bytes=60 * 1024 * 1024
            ),
        )(
            hidden,
            moe_gain,
            expert_ids.T,
            slots.T,
            affinity.T,
            w_gate,
            w_up,
            w_down,
            attn_gain,
            w_dkv.T,
            kv_gain[None],
            queries.reshape(pairs, 2, heads, kvc),
            cache.reshape(pairs, 2, span, kvc),
            lengths,
        )
        return pl.pallas_call(
            put_out,
            out_shape=(
                jax.ShapeDtypeStruct((tokens, d_loc), BF16),
                jax.ShapeDtypeStruct((tokens, heads, lat), BF16),
            ),
            in_specs=[vmem, vmem],
            out_specs=(any_space, any_space),
            scratch_shapes=[dma((2,))],
        )(*[pltpu.with_memory_space_constraint(r, pltpu.VMEM) for r in results])

    return jax.shard_map(
        local,
        mesh=mesh,
        in_specs=(
            P(("grp", "ep", "mb"), "tp"),
            P("tp"),
            P(("grp", "ep", "mb"), None),
            P(("grp", "ep", "mb"), None),
            P(("grp", "ep", "mb"), None),
            P(("ep", "mb"), None, "tp"),
            P(("ep", "mb"), None, "tp"),
            P(("ep", "mb"), "tp", None),
            P("tp"),
            P("tp", None),
            P(),
            P(("grp", "ep", "mb"), "tp", None),
            P(("grp", "ep", "mb"), "tp", None),
            P(("grp", "ep", "mb")),
        ),
        out_specs=(P(("grp", "ep", "mb"), "tp"), P(("grp", "ep", "mb"), "tp", None)),
        check_vma=False,
    )
```

```python
import functools

import jax
import jax.numpy as jnp
from jax import lax
from jax.experimental import pallas as pl
from jax.experimental.pallas import tpu as pltpu
from jax.sharding import PartitionSpec as P

CAP = 8
AHEAD = 4
epsilon = 1e-06
route_scale = 2.5
score_scale = 192.0 ** (-0.5)
STOPS = (1, 4, 6, 8)
MESH = pl.DeviceIdType.MESH
F32 = jnp.float32
BF16 = jnp.bfloat16


def up(value, step):
    return -(-value // step) * step


def piece_width(d_loc, d_all):
    if d_loc % 128 == 0:
        return next(w for w in (896, 512, 384, 256, 128) if d_loc % w == 0)
    return 512 if d_all % 512 == 0 else 128


def split3(value, width):
    high = value.astype(BF16)
    rest = value - high.astype(F32)
    mid = rest.astype(BF16)
    low = (rest - mid.astype(F32)).astype(BF16)
    lane = lax.broadcasted_iota(jnp.int32, (value.shape[0], width), 1)
    parts = jnp.where(lane == 1, mid.astype(F32), jnp.where(lane == 2, low.astype(F32), 0.0))
    return jnp.where(lane == 0, high.astype(F32), parts).astype(BF16)


def kernel(
    n_tp,
    n_ep,
    n_mb,
    hidden,
    moe_gain_in,
    ids_in,
    slots_in,
    affinity_in,
    w_gate,
    w_up,
    w_down,
    attn_gain_in,
    w_dkv,
    kv_gain_in,
    queries,
    cache,
    lengths_in,
    next_out,
    latent_out,
    hid_all,
    gain_all,
    send,
    arrived,
    wg,
    wu,
    wd,
    wk,
    ret_send,
    ret,
    tsum,
    rs_send,
    rs_recv,
    key_send,
    key_recv,
    q_all,
    q_rope,
    k_lat,
    k_rope,
    k_pad,
    o_send,
    o_recv,
    stat_all,
    stat_send,
    stat_recv,
    mid_units,
    mid_key,
    gain_row,
    acc,
    peaks,
    masses,
    keys,
    old_part,
    own_part,
    moe_gain,
    ids,
    slots,
    affinity,
    attn_gain,
    kv_gain,
    lengths,
    small_sem,
    near_sem,
    load_sem,
    q_sem,
    kv_load_sem,
    hid_ssem,
    hid_rsem,
    gain_ssem,
    gain_rsem,
    q_ssem,
    q_rsem,
    o_ssem,
    o_rsem,
    stat_ssem,
    stat_rsem,
    row_ssem,
    row_rsem,
    ret_ssem,
    ret_rsem,
    rs_ssem,
    rs_rsem,
    key_ssem,
    key_rsem,
):
    experts = n_ep * n_mb
    tokens, d_loc = hidden.shape
    d_all = d_loc * n_tp
    lat = kv_gain.shape[1]
    pairs, span_len, kvc = cache.shape[0], cache.shape[2], cache.shape[3]
    tp = lax.axis_index("tp")
    staged = 1 < n_ep <= 4
    me = lax.axis_index("ep") * n_mb + lax.axis_index("mb")

    def tp_id(step):
        return lax.rem(tp + step, n_tp)

    def ex_id(step):
        return lax.rem(me + step, experts)

    def ex_dev(index):
        return {"ep": index // n_mb, "mb": lax.rem(index, n_mb)}

    ep, mb = lax.axis_index("ep"), lax.axis_index("mb")
    barrier = pltpu.get_barrier_semaphore()

    def hello(sem, ids):
        pl.semaphore_signal(sem, inc=1, device_id=ids, device_id_type=MESH)

    for step in range(1, n_tp):
        hello(barrier, {"tp": tp_id(step)})
    local = [
        pltpu.make_async_copy(hidden, hid_all.at[tp], load_sem.at[0]),
        pltpu.make_async_copy(w_gate.at[0], wg, load_sem.at[1]),
        pltpu.make_async_copy(w_up.at[0], wu, load_sem.at[2]),
        pltpu.make_async_copy(w_down.at[0], wd, load_sem.at[3]),
        pltpu.make_async_copy(w_dkv, wk, load_sem.at[4]),
    ]
    rope = kvc - lat
    q_loads = [
        pltpu.make_async_copy(
            queries.at[:, i, :, :lat], q_all.at[:, 0, :, i * lat : (i + 1) * lat], q_sem.at[i]
        )
        for i in range(2)
    ]
    q_loads.append(pltpu.make_async_copy(queries.at[:, :, :, lat:], q_rope, q_sem.at[2]))
    kv_loads = [
        pltpu.make_async_copy(cache.at[:, :, :, :lat], k_lat, kv_load_sem.at[0]),
        pltpu.make_async_copy(cache.at[:, :, :, lat:], k_rope, kv_load_sem.at[1]),
    ]
    small = [
        pltpu.make_async_copy(src, dst, small_sem.at[i])
        for i, (src, dst) in enumerate(
            (
                (slots_in, slots),
                (ids_in, ids),
                (affinity_in, affinity),
                (moe_gain_in, moe_gain),
                (attn_gain_in, attn_gain),
                (kv_gain_in, kv_gain),
                (lengths_in, lengths),
            )
        )
    ]
    local[0].start()
    for copy in small[3::-1]:
        copy.start()
    for copy in q_loads + kv_loads:
        copy.start()
    for copy in small[4:]:
        copy.start()

    if staged:
        for step in range(1, n_mb):
            hello(barrier, {"mb": lax.rem(mb + step, n_mb)})
        for far in range(1, n_ep):

            @pl.when(ep + far < n_ep)
            def _():
                for m in range(n_mb):
                    hello(barrier, {"ep": ep + far, "mb": m})

        greeted = n_tp - 1 + n_mb - 1 + n_mb * ep
    else:
        for step in range(1, experts):
            hello(barrier, ex_dev(ex_id(step)))
        greeted = n_tp - 1 + experts - 1

    def tp_copy(src, dst, ssem, rsem, step):
        return pltpu.make_async_remote_copy(
            src_ref=src,
            dst_ref=dst,
            send_sem=ssem,
            recv_sem=rsem,
            device_id={"tp": tp_id(step)},
            device_id_type=MESH,
        )

    def arrival(dst, rsem):
        return pltpu.make_async_copy(dst, dst, rsem)

    def feed(p):
        for step in range(1, n_tp):
            tp_copy(
                q_all.at[p, 0], q_all.at[p, n_tp - step], q_ssem.at[0], q_rsem.at[p], step
            ).start()

    def row_copy(peer, block):
        return pltpu.make_async_remote_copy(
            src_ref=send.at[peer, block],
            dst_ref=arrived.at[me, block],
            send_sem=row_ssem.at[0],
            recv_sem=row_rsem.at[block],
            device_id=ex_dev(peer),
            device_id_type=MESH,
        )

    def ship_to(ep_index, block):
        for m in range(n_mb):
            row_copy(ep_index * n_mb + m, block).start()

    def ship_near(block):
        arrived[me, block] = send[me, block]
        for step in range(1, n_mb):
            row_copy(ep * n_mb + lax.rem(mb + step, n_mb), block).start()

    def ship(block):
        ship_near(block)
        for far in range(1, n_ep):
            pl.when(ep >= far)(functools.partial(ship_to, ep - far, block))
            pl.when(ep + far < n_ep)(functools.partial(ship_to, ep + far, block))
    small[3].wait()
    gain_all[tp] = moe_gain[...].reshape(1, d_loc)
    local[0].wait()
    pl.semaphore_wait(barrier, greeted)
    for step in range(1, n_tp):
        for src, dst, ssem, rsem in (
            (hid_all.at[tp], hid_all, hid_ssem, hid_rsem),
            (gain_all.at[tp], gain_all, gain_ssem, gain_rsem),
        ):
            tp_copy(src, dst.at[tp], ssem.at[0], rsem.at[0], step).start()
    if staged:
        for far in range(1, n_ep):

            @pl.when(ep >= far)
            def _():
                for m in range(n_mb):
                    hello(near_sem.at[far], {"ep": ep - far, "mb": m})

    for copy in small[:3]:
        copy.wait()
    kept = slots[...] < CAP
    target = jnp.where(kept, ids[...] * CAP + slots[...], -1)
    rows = experts * CAP
    iota = lax.broadcasted_iota(jnp.int32, (rows, tokens), 0)
    dispatch = jnp.zeros((rows, tokens), F32)
    for k in range(ids.shape[0]):
        dispatch = jnp.where(target[k : k + 1] == iota, 1.0, dispatch)
    dispatch = dispatch.astype(BF16)

    def pick(block):
        picked = jnp.dot(dispatch, hid_all[block], preferred_element_type=F32)
        send[:, block] = picked.reshape(experts, CAP, d_loc).astype(BF16)

    pick(tp)
    if staged:
        ship_near(tp)
        for far in range(1, n_ep):
            pl.when(ep >= far)(functools.partial(ship_to, ep - far, tp))
    else:
        ship(tp)
    for copy in q_loads:
        copy.wait()
    q_all[:, 0, :, 2 * lat : 2 * kvc] = jnp.concatenate([q_rope[:, 0], q_rope[:, 1]], -1)
    for t in range(AHEAD):
        feed(t)
    for copy in local[1:]:
        copy.start()
    for copy in kv_loads:
        copy.wait()
    blank = jnp.zeros((pairs, span_len, rope), BF16)
    k_pad[:, :span_len] = jnp.concatenate([k_rope[:, 0], blank], -1)
    k_pad[:, span_len:] = jnp.concatenate([blank, k_rope[:, 1]], -1)
    stat_all[...] = jnp.zeros(stat_all.shape, F32)
    aff = affinity[...]
    weight = route_scale * aff / jnp.sum(aff, 0, keepdims=True) * kept.astype(F32)
    combine = jnp.zeros((rows, tokens), F32)
    for k in range(ids.shape[0]):
        combine = jnp.where(target[k : k + 1] == iota, weight[k : k + 1], combine)
    combine = combine.T
    high = combine.astype(BF16)
    rest = combine - high.astype(F32)
    mid = rest.astype(BF16)
    low = (rest - mid.astype(F32)).astype(BF16)
    combine3 = jnp.concatenate([high, mid, low], 0)
    if staged:
        for far in range(1, n_ep):

            @pl.when(ep + far < n_ep)
            def _():
                pl.semaphore_wait(near_sem.at[far], n_mb)
                ship_to(ep + far, tp)
    arrival(hid_all.at[pl.ds(0, n_tp - 1)], hid_rsem.at[0]).wait()
    arrival(gain_all.at[pl.ds(0, n_tp - 1)], gain_rsem.at[0]).wait()
    for turn in range(1, n_tp):
        pick(tp_id(turn))
        ship(tp_id(turn))

    heads = queries.shape[2]
    both = n_tp * heads
    keys_two = 2 * span_len
    lane = lax.broadcasted_iota(jnp.int32, (both, keys_two), 1)
    first_token = lane < span_len
    stat_lane = lax.broadcasted_iota(jnp.int32, stat_send.shape[1:], 1)

    def attend(first, last):
        def body(p, carry):
            arrival(q_all.at[p, pl.ds(1, n_tp - 1)], q_rsem.at[p]).wait()

            @pl.when(p + AHEAD < pairs)
            def _():
                feed(p + AHEAD)

            q = q_all[p].reshape(both, q_all.shape[3])
            block = k_lat[p].reshape(keys_two, lat)
            crossed = lax.dot_general(
                jnp.concatenate([q[:, :lat], q[:, lat : 2 * lat]], 0),
                block,
                (((1,), (1,)), ((), ())),
                preferred_element_type=F32,
            )
            turned = lax.dot_general(
                q[:, 2 * lat :], k_pad[p], (((1,), (1,)), ((), ())), preferred_element_type=F32
            )
            scores = (jnp.where(first_token, crossed[:both], crossed[both:]) + turned) * score_scale
            done = tp * span_len
            stop = jnp.where(first_token, lengths[2 * p] - done, lengths[2 * p + 1] - done + span_len)
            live = lane < stop
            scores = jnp.where(live, scores, -1e30)
            mine = [first_token, jnp.logical_not(first_token)]
            tops = [
                jnp.max(jnp.where(m, scores, -1e30), -1, keepdims=True).astype(BF16).astype(F32)
                for m in mine
            ]
            prob = jnp.where(live, jnp.exp(scores - jnp.where(first_token, tops[0], tops[1])), 0.0)
            parts = [jnp.where(m, prob, 0.0) for m in mine]
            sums = [jnp.sum(part, -1, keepdims=True) for part in parts]
            out = jnp.dot(
                jnp.concatenate(parts, 0).astype(BF16), block, preferred_element_type=F32
            )
            for i in range(2):
                acc[2 * p + i] = out[i * both : i * both + heads]
                peaks[2 * p + i] = jnp.broadcast_to(tops[i][:heads], (heads, 128))
                masses[2 * p + i] = jnp.broadcast_to(sums[i][:heads], (heads, 128))
            for step in range(1, n_tp):
                stat = stat_all[step]
                for i in range(2):
                    start = step * heads
                    o_send[step, p, i] = out[i * both + start : i * both + start + heads].astype(BF16)
                    base = 3 * (2 * p + i)
                    mass = sums[i][start : start + heads]
                    high = mass.astype(BF16).astype(F32)
                    stat = jnp.where(stat_lane == base, tops[i][start : start + heads], stat)
                    stat = jnp.where(stat_lane == base + 1, high, stat)
                    stat = jnp.where(stat_lane == base + 2, mass - high, stat)
                stat_all[step] = stat
                tp_copy(
                    o_send.at[step, p], o_recv.at[n_tp - step, p], o_ssem.at[0], o_rsem.at[0], step
                ).start()
            return carry

        lax.fori_loop(first, last, body, 0)

    for copy in small[4:]:
        copy.wait()
    gain_row[...] = attn_gain[...].reshape(1, d_loc)
    stops = [pairs * n // 8 for n in STOPS]
    attend(0, stops[0])
    local[1].wait()
    local[2].wait()
    square = jnp.zeros((rows, 1), F32)
    for turn in range(n_tp):
        b = tp_id(turn)
        if turn == n_tp - 1:
            attend(stops[0], stops[1])
        arrival(arrived.at[pl.ds(0, experts - 1), b], row_rsem.at[b]).wait()
        wide = arrived[:, b].astype(F32).reshape(rows, d_loc)
        square = square + jnp.sum(wide * wide, -1, keepdims=True)
        block = (wide * gain_all[b]).astype(BF16)
        deep = pl.ds(pl.multiple_of(b * d_loc, d_loc & -d_loc), d_loc)
        gate = jnp.dot(block, wg[deep], preferred_element_type=F32)
        upper = jnp.dot(block, wu[deep], preferred_element_type=F32)
        if turn > 0:
            gate = gate + mid_units[0]
            upper = upper + mid_units[1]
        if turn < n_tp - 1:
            mid_units[0] = gate
            mid_units[1] = upper
    scale = lax.rsqrt(square / d_all + epsilon)
    gate = gate * scale
    upper = upper * scale
    units = (gate / (1.0 + jnp.exp(-gate)) * upper).astype(BF16)
    local[3].wait()
    aligned = d_loc % 128 == 0
    width = piece_width(d_loc, d_all)
    if aligned:
        pieces = [(tp_id(turn) * d_loc, d_loc) for turn in range(1, n_tp)]
        pieces += [(tp * d_loc + c, width) for c in range(0, d_loc, width)]
    else:
        middle = d_all // width // 2 * width
        pieces = [(0, middle), (middle, d_all - middle)]

    def columns(start, size):
        return pl.ds(pl.multiple_of(start, 128), size)

    for h, (first, size) in enumerate(pieces):
        for c in range(0, size, width):
            part = jnp.dot(units, wd[:, columns(first + c, width)], preferred_element_type=F32)
            ret_send[:, :, columns(first + c, width)] = part.reshape(
                experts, CAP, width
            ).astype(BF16)
            for step in range(1, experts):
                peer = ex_id(step)
                pltpu.make_async_remote_copy(
                    src_ref=ret_send.at[peer, :, columns(first + c, width)],
                    dst_ref=ret.at[me, :, columns(first + c, width)],
                    send_sem=ret_ssem.at[0],
                    recv_sem=ret_rsem.at[h],
                    device_id=ex_dev(peer),
                    device_id_type=MESH,
                ).start()
    ret[me] = ret_send[me]

    def exchange(step):
        tp_copy(
            rs_send.at[step], rs_recv.at[n_tp - step], rs_ssem.at[0], rs_rsem.at[0], step
        ).start()

    def gather(h):
        first, size = pieces[h]
        arrival(
            ret.at[pl.ds(0, experts - 1), :, columns(first, size)], ret_rsem.at[h]
        ).wait()

    def mixed(start):
        block = ret[:, :, columns(start, width)].astype(F32)
        block = block.reshape(rows, width).astype(BF16)
        part = jnp.dot(combine3, block, preferred_element_type=F32)
        return part[:tokens] + (part[tokens : 2 * tokens] + part[2 * tokens : 3 * tokens])

    def send_stats():
        stat_send[...] = stat_all[...].astype(BF16)
        for step in range(1, n_tp):
            tp_copy(
                stat_send.at[step],
                stat_recv.at[n_tp - step],
                stat_ssem.at[0],
                stat_rsem.at[0],
                step,
            ).start()

    def renew(start, size, moe):
        span = pl.ds(start, size)
        fresh = (hid_all[tp, :, span].astype(F32) + moe).astype(BF16)
        next_out[:, span] = fresh
        fresh = fresh.astype(F32)
        scaled = (fresh * gain_row[...][:, start : start + size]).astype(BF16)
        part = lax.dot_general(
            scaled, wk[:, span], (((1,), (1,)), ((), ())), preferred_element_type=F32
        )
        return jnp.sum(fresh * fresh, -1, keepdims=True), part

    def others(start, size):
        total = rs_recv[1, :, pl.ds(start, size)].astype(F32)
        for step in range(2, n_tp):
            total = total + rs_recv[step, :, pl.ds(start, size)].astype(F32)
        return total
    attend(stops[1], stops[2])
    if aligned:
        for turn in range(1, n_tp):
            gather(turn - 1)
            for c in range(0, d_loc, width):
                rs_send[turn, :, c : c + width] = mixed(pieces[turn - 1][0] + c).astype(BF16)
            exchange(turn)
        attend(stops[2], stops[3])
        if stops[3] == pairs:
            send_stats()
        local[4].wait()
        square = jnp.zeros((tokens, 1), F32)
        for i, c in enumerate(range(0, d_loc, width)):
            gather(n_tp - 1 + i)
            part = mixed(tp * d_loc + c)
            if i == 0:
                arrival(rs_recv.at[pl.ds(1, n_tp - 1)], rs_rsem.at[0]).wait()
            more, part = renew(c, width, part + others(c, width))
            square = square + more
            if i > 0:
                part = part + mid_key[...]
            if c + width < d_loc:
                mid_key[...] = part
    else:
        for h in range(2):
            gather(h)
            first, size = pieces[h]
            for c in range(0, size, width):
                tsum[:, columns(first + c, width)] = mixed(first + c)
            if h == 0:
                attend(stops[2], stops[3])
        for p in range(n_tp):
            rs_send[lax.rem(p - tp + n_tp, n_tp)] = tsum[:, p * d_loc : (p + 1) * d_loc].astype(BF16)
        for step in range(1, n_tp):
            exchange(step)
        if stops[3] == pairs:
            send_stats()
        local[4].wait()
        arrival(rs_recv.at[pl.ds(1, n_tp - 1)], rs_rsem.at[0]).wait()
        square, part = renew(0, d_loc, rs_send[0].astype(F32) + others(0, d_loc))
    kvp = up(kvc + 3, 128)
    tail = kvp - kvc
    key_send[:, :kvc] = part.astype(BF16)
    key_send[:, kvc:kvp] = split3(square, tail)
    for step in range(1, n_tp):
        tp_copy(key_send, key_recv.at[tp], key_ssem.at[0], key_rsem.at[0], step).start()
    key_recv[tp] = key_send[...]
    if stops[3] < pairs:
        attend(stops[3], pairs)
        send_stats()
    half = (kvc - lat) // 2
    column = lax.broadcasted_iota(jnp.int32, (tokens, 2 * half), 1)
    pair = jnp.where(column < half, column, column - half).astype(F32)
    freq = jnp.exp(pair * (-9.210340371976184 / half))
    row_id = lax.broadcasted_iota(jnp.int32, (tokens, 2 * half), 0)
    place = jnp.zeros((tokens, 2 * half), F32)
    for t in range(tokens):
        place = jnp.where(row_id == t, lengths[t].astype(F32), place)
    angle = place * freq
    cos_table = jnp.cos(angle)
    sin_table = jnp.where(column < half, -1.0, 1.0) * jnp.sin(angle)
    arrival(o_recv.at[pl.ds(1, n_tp - 1)], o_rsem.at[0]).wait()
    arrival(stat_recv.at[pl.ds(1, n_tp - 1)], stat_rsem.at[0]).wait()
    for t in range(tokens):
        for step in range(1, n_tp):
            stat = stat_recv[step].astype(F32)
            far_top = jnp.sum(jnp.where(stat_lane == 3 * t, stat, 0.0), -1, keepdims=True)
            far_mass = jnp.where(stat_lane == 3 * t + 1, stat, 0.0)
            far_mass = far_mass + jnp.where(stat_lane == 3 * t + 2, stat, 0.0)
            far_mass = jnp.sum(far_mass, -1, keepdims=True)
            near_top = peaks[t]
            top = jnp.maximum(near_top, far_top)
            near_factor = jnp.exp(near_top - top)
            far_factor = jnp.exp(far_top - top)
            peaks[t] = top
            masses[t] = masses[t] * near_factor + far_mass * far_factor
            for c in range(0, lat, 128):
                far = o_recv[step, t // 2, t % 2, :, c : c + 128].astype(F32) * far_factor
                acc[t, :, c : c + 128] = acc[t, :, c : c + 128] * near_factor + far
    arrival(key_recv.at[pl.ds(0, n_tp - 1)], key_rsem.at[0]).wait()
    total = key_recv[0].astype(F32)
    for p in range(1, n_tp):
        total = total + key_recv[p].astype(F32)
    square = jnp.sum(total[:, kvc:], -1, keepdims=True)
    down = total * lax.rsqrt(square / d_all + epsilon)
    latent = down[:, :lat]
    latent = (
        latent
        * lax.rsqrt(jnp.mean(latent * latent, -1, keepdims=True) + epsilon)
        * kv_gain[...]
    )
    turn = down[:, lat:kvc]
    swapped = jnp.concatenate([turn[:, half:], turn[:, :half]], 1)
    turn = turn * cos_table + swapped * sin_table
    keys[:, :lat] = latent.astype(BF16)
    turn = turn.astype(BF16)
    blank = jnp.zeros((tokens, rope), BF16)
    keys[:, lat:] = jnp.concatenate([turn, blank, blank, turn], 1)
    rows_all = tokens * heads
    own = jnp.concatenate(
        [
            jnp.concatenate(
                [
                    lax.dot_general(
                        q_all[p, 0, :, i * lat : (i + 1) * lat],
                        keys[:, :lat],
                        (((1,), (1,)), ((), ())),
                        preferred_element_type=F32,
                    )
                    + lax.dot_general(
                        q_all[p, 0, :, 2 * lat :],
                        keys[:, lat + 2 * rope * i : lat + 2 * rope * (i + 1)],
                        (((1,), (1,)), ((), ())),
                        preferred_element_type=F32,
                    )
                    for i in range(2)
                ],
                0,
            )
            for p in range(pairs)
        ],
        0,
    )
    owner = lax.broadcasted_iota(jnp.int32, (rows_all, tokens), 0) // heads
    mine = owner == lax.broadcasted_iota(jnp.int32, (rows_all, tokens), 1)
    own = jnp.sum(jnp.where(mine, own, 0.0), -1, keepdims=True) * score_scale
    own = jnp.broadcast_to(own, (rows_all, 128))
    peak = peaks[...].reshape(rows_all, 128)
    top = jnp.maximum(peak, own)
    factor = jnp.exp(peak - top)
    own_prob = jnp.exp(own - top)
    inverse = 1.0 / (masses[...].reshape(rows_all, 128) * factor + own_prob)
    old_part[...] = (factor * inverse).reshape(tokens, heads, 128)
    own_part[...] = (own_prob.astype(BF16).astype(F32) * inverse).reshape(tokens, heads, 128)
    for t in range(tokens):
        for c in range(0, lat, 128):
            value = acc[t, :, c : c + 128] * old_part[t]
            key = keys[t : t + 1, c : c + 128].astype(F32)
            latent_out[t, :, c : c + 128] = (value + own_part[t] * key).astype(BF16)
    for sent, sem in (
        (send.at[pl.ds(0, experts - 1)], row_ssem),
        (ret_send.at[pl.ds(0, experts - 1)], ret_ssem),
        (hid_all.at[pl.ds(0, n_tp - 1)], hid_ssem),
        (gain_all.at[pl.ds(0, n_tp - 1)], gain_ssem),
        (rs_send.at[pl.ds(1, n_tp - 1)], rs_ssem),
        (key_recv.at[pl.ds(0, n_tp - 1)], key_ssem),
        (q_all.at[:, pl.ds(0, n_tp - 1)], q_ssem),
        (o_send.at[pl.ds(1, n_tp - 1)], o_ssem),
        (stat_send.at[pl.ds(1, n_tp - 1)], stat_ssem),
    ):
        arrival(sent, sem.at[0]).wait()


def put_out(hidden_in, latent_in, hidden_out, latent_out, sem):
    step = latent_in.shape[0] // 4
    copies = [pltpu.make_async_copy(hidden_in, hidden_out, sem.at[4])]
    for i in range(4):
        part = pl.ds(i * step, step)
        copies.append(
            pltpu.make_async_copy(latent_in.at[part], latent_out.at[part], sem.at[i])
        )
    for copy in copies:
        copy.start()
    for copy in copies:
        copy.wait()


def solution(mesh):
    n_tp, n_ep, n_mb = mesh.shape["tp"], mesh.shape["ep"], mesh.shape["mb"]
    experts = n_ep * n_mb

    def local(
        hidden,
        moe_gain,
        expert_ids,
        slots,
        affinity,
        w_gate,
        w_up,
        w_down,
        attn_gain,
        w_dkv,
        kv_gain,
        queries,
        cache,
        lengths,
    ):
        tokens, d_loc = hidden.shape
        d_all = d_loc * n_tp
        heads, kvc = queries.shape[1:]
        span = cache.shape[1]
        lat = kv_gain.shape[0]
        pairs = tokens // 2
        hid_dim = w_gate.shape[2]
        top = expert_ids.shape[1]
        wide = up(kvc + 3, 128)
        returns = n_tp - 1 + d_loc // piece_width(d_loc, d_all) if d_loc % 128 == 0 else 2
        any_space = pl.BlockSpec(memory_space=pl.ANY)
        vmem = pl.BlockSpec(memory_space=pltpu.VMEM)
        dma = pltpu.SemaphoreType.DMA
        results = pl.pallas_call(
            functools.partial(kernel, n_tp, n_ep, n_mb),
            out_shape=(
                pltpu.VMEM((tokens, d_loc), BF16),
                pltpu.VMEM((tokens, heads, lat), BF16),
            ),
            in_specs=[any_space] * 14,
            out_specs=(vmem, vmem),
            scratch_shapes=[
                pltpu.VMEM((n_tp, tokens, d_loc), BF16),
                pltpu.VMEM((n_tp, 1, d_loc), F32),
                pltpu.VMEM((experts, n_tp, CAP, d_loc), BF16),
                pltpu.VMEM((experts, n_tp, CAP, d_loc), BF16),
                pltpu.VMEM((d_all, hid_dim), BF16),
                pltpu.VMEM((d_all, hid_dim), BF16),
                pltpu.VMEM((hid_dim, d_all), BF16),
                pltpu.VMEM((kvc, d_loc), BF16),
                pltpu.VMEM((experts, CAP, d_all), BF16),
                pltpu.VMEM((experts, CAP, d_all), BF16),
                pltpu.VMEM((tokens, d_all), F32),
                pltpu.VMEM((n_tp, tokens, d_loc), BF16),
                pltpu.VMEM((n_tp, tokens, d_loc), BF16),
                pltpu.VMEM((tokens, wide), BF16),
                pltpu.VMEM((n_tp, tokens, wide), BF16),
                pltpu.VMEM((pairs, n_tp, heads, 2 * kvc), BF16),
                pltpu.VMEM((pairs, 2, heads, kvc - lat), BF16),
                pltpu.VMEM((pairs, 2, span, lat), BF16),
                pltpu.VMEM((pairs, 2, span, kvc - lat), BF16),
                pltpu.VMEM((pairs, 2 * span, 2 * (kvc - lat)), BF16),
                pltpu.VMEM((n_tp, pairs, 2, heads, lat), BF16),
                pltpu.VMEM((n_tp, pairs, 2, heads, lat), BF16),
                pltpu.VMEM((n_tp, heads, up(3 * tokens, 128)), F32),
                pltpu.VMEM((n_tp, heads, up(3 * tokens, 128)), BF16),
                pltpu.VMEM((n_tp, heads, up(3 * tokens, 128)), BF16),
                pltpu.VMEM((2, experts * CAP, hid_dim), F32),
                pltpu.VMEM((tokens, kvc), F32),
                pltpu.VMEM((1, d_loc), F32),
                pltpu.VMEM((tokens, heads, lat), F32),
                pltpu.VMEM((tokens, heads, 128), F32),
                pltpu.VMEM((tokens, heads, 128), F32),
                pltpu.VMEM((tokens, lat + 4 * (kvc - lat)), BF16),
                pltpu.VMEM((tokens, heads, 128), F32),
                pltpu.VMEM((tokens, heads, 128), F32),
                pltpu.VMEM((d_loc,), F32),
                pltpu.VMEM((top, tokens), jnp.int32),
                pltpu.VMEM((top, tokens), jnp.int32),
                pltpu.VMEM((top, tokens), F32),
                pltpu.VMEM((d_loc,), F32),
                pltpu.VMEM((1, lat), F32),
                pltpu.SMEM((tokens,), jnp.int32),
                dma((7,)),
                pltpu.SemaphoreType.REGULAR((n_ep,)),
                dma((5,)),
                dma((3,)),
                dma((2,)),
                dma((1,)),
                dma((1,)),
                dma((1,)),
                dma((1,)),
                dma((1,)),
                dma((pairs,)),
                dma((1,)),
                dma((1,)),
                dma((1,)),
                dma((1,)),
                dma((1,)),
                dma((n_tp,)),
                dma((1,)),
                dma((returns,)),
                dma((1,)),
                dma((1,)),
                dma((1,)),
                dma((1,)),
            ],
            compiler_params=pltpu.CompilerParams(
                collective_id=0, has_side_effects=True, vmem_limit_bytes=60 * 1024 * 1024
            ),
        )(
            hidden,
            moe_gain,
            expert_ids.T,
            slots.T,
            affinity.T,
            w_gate,
            w_up,
            w_down,
            attn_gain,
            w_dkv.T,
            kv_gain[None],
            queries.reshape(pairs, 2, heads, kvc),
            cache.reshape(pairs, 2, span, kvc),
            lengths,
        )
        return pl.pallas_call(
            put_out,
            out_shape=(
                jax.ShapeDtypeStruct((tokens, d_loc), BF16),
                jax.ShapeDtypeStruct((tokens, heads, lat), BF16),
            ),
            in_specs=[vmem, vmem],
            out_specs=(any_space, any_space),
            scratch_shapes=[dma((5,))],
        )(*[pltpu.with_memory_space_constraint(r, pltpu.VMEM) for r in results])

    return jax.shard_map(
        local,
        mesh=mesh,
        in_specs=(
            P(("grp", "ep", "mb"), "tp"),
            P("tp"),
            P(("grp", "ep", "mb"), None),
            P(("grp", "ep", "mb"), None),
            P(("grp", "ep", "mb"), None),
            P(("ep", "mb"), None, "tp"),
            P(("ep", "mb"), None, "tp"),
            P(("ep", "mb"), "tp", None),
            P("tp"),
            P("tp", None),
            P(),
            P(("grp", "ep", "mb"), "tp", None),
            P(("grp", "ep", "mb"), "tp", None),
            P(("grp", "ep", "mb")),
        ),
        out_specs=(P(("grp", "ep", "mb"), "tp"), P(("grp", "ep", "mb"), "tp", None)),
        check_vma=False,
    )
```

```python
import functools

import jax
import jax.numpy as jnp
from jax import lax
from jax.experimental import pallas as pl
from jax.experimental.pallas import tpu as pltpu
from jax.sharding import PartitionSpec as P

CAP = 8
AHEAD = 4
epsilon = 1e-06
route_scale = 2.5
score_scale = 192.0 ** (-0.5)
STOPS = (1, 4, 6, 8)
MESH = pl.DeviceIdType.MESH
F32 = jnp.float32
BF16 = jnp.bfloat16


def up(value, step):
    return -(-value // step) * step


def piece_width(d_loc, d_all):
    if d_loc % 128 == 0:
        return next(w for w in (896, 512, 384, 256, 128) if d_loc % w == 0)
    return 512 if d_all % 512 == 0 else 128


def split3(value, width):
    high = value.astype(BF16)
    rest = value - high.astype(F32)
    mid = rest.astype(BF16)
    low = (rest - mid.astype(F32)).astype(BF16)
    lane = lax.broadcasted_iota(jnp.int32, (value.shape[0], width), 1)
    parts = jnp.where(lane == 1, mid.astype(F32), jnp.where(lane == 2, low.astype(F32), 0.0))
    return jnp.where(lane == 0, high.astype(F32), parts).astype(BF16)


def kernel(
    n_tp,
    n_ep,
    n_mb,
    hidden,
    moe_gain_in,
    ids_in,
    slots_in,
    affinity_in,
    w_gate,
    w_up,
    w_down,
    attn_gain_in,
    w_dkv,
    kv_gain_in,
    queries,
    cache,
    lengths_in,
    next_out,
    latent_out,
    hid_all,
    gain_all,
    send,
    arrived,
    wg,
    wu,
    wd,
    wk,
    ret_send,
    ret,
    tsum,
    rs_send,
    rs_recv,
    key_send,
    key_recv,
    q_all,
    q_rope,
    k_lat,
    k_rope,
    k_pad,
    o_send,
    o_recv,
    stat_all,
    stat_send,
    stat_recv,
    mid_units,
    mid_key,
    gain_row,
    acc,
    peaks,
    masses,
    keys,
    old_part,
    own_part,
    moe_gain,
    ids,
    slots,
    affinity,
    attn_gain,
    kv_gain,
    lengths,
    small_sem,
    near_sem,
    load_sem,
    q_sem,
    kv_load_sem,
    hid_ssem,
    hid_rsem,
    gain_ssem,
    gain_rsem,
    q_ssem,
    q_rsem,
    o_ssem,
    o_rsem,
    stat_ssem,
    stat_rsem,
    row_ssem,
    row_rsem,
    ret_ssem,
    ret_rsem,
    rs_ssem,
    rs_rsem,
    key_ssem,
    key_rsem,
):
    experts = n_ep * n_mb
    tokens, d_loc = hidden.shape
    d_all = d_loc * n_tp
    lat = kv_gain.shape[1]
    pairs, span_len, kvc = cache.shape[0], cache.shape[2], cache.shape[3]
    tp = lax.axis_index("tp")
    staged = 1 < n_ep <= 4
    me = lax.axis_index("ep") * n_mb + lax.axis_index("mb")

    def tp_id(step):
        return lax.rem(tp + step, n_tp)

    def ex_id(step):
        return lax.rem(me + step, experts)

    def ex_dev(index):
        return {"ep": index // n_mb, "mb": lax.rem(index, n_mb)}

    ep, mb = lax.axis_index("ep"), lax.axis_index("mb")
    barrier = pltpu.get_barrier_semaphore()

    def hello(sem, ids):
        pl.semaphore_signal(sem, inc=1, device_id=ids, device_id_type=MESH)

    for step in range(1, n_tp):
        hello(barrier, {"tp": tp_id(step)})
    local = [
        pltpu.make_async_copy(hidden, hid_all.at[tp], load_sem.at[0]),
        pltpu.make_async_copy(w_gate.at[0], wg, load_sem.at[1]),
        pltpu.make_async_copy(w_up.at[0], wu, load_sem.at[2]),
        pltpu.make_async_copy(w_down.at[0], wd, load_sem.at[3]),
        pltpu.make_async_copy(w_dkv, wk, load_sem.at[4]),
    ]
    rope = kvc - lat
    q_loads = [
        pltpu.make_async_copy(
            queries.at[:, i, :, :lat], q_all.at[:, 0, :, i * lat : (i + 1) * lat], q_sem.at[i]
        )
        for i in range(2)
    ]
    q_loads.append(pltpu.make_async_copy(queries.at[:, :, :, lat:], q_rope, q_sem.at[2]))
    kv_loads = [
        pltpu.make_async_copy(cache.at[:, :, :, :lat], k_lat, kv_load_sem.at[0]),
        pltpu.make_async_copy(cache.at[:, :, :, lat:], k_rope, kv_load_sem.at[1]),
    ]
    small = [
        pltpu.make_async_copy(src, dst, small_sem.at[i])
        for i, (src, dst) in enumerate(
            (
                (slots_in, slots),
                (ids_in, ids),
                (affinity_in, affinity),
                (moe_gain_in, moe_gain),
                (attn_gain_in, attn_gain),
                (kv_gain_in, kv_gain),
                (lengths_in, lengths),
            )
        )
    ]
    local[0].start()
    for copy in small[3::-1]:
        copy.start()
    for copy in q_loads + kv_loads:
        copy.start()
    for copy in small[4:]:
        copy.start()

    if staged:
        for step in range(1, n_mb):
            hello(barrier, {"mb": lax.rem(mb + step, n_mb)})
        for far in range(1, n_ep):

            @pl.when(ep + far < n_ep)
            def _():
                for m in range(n_mb):
                    hello(barrier, {"ep": ep + far, "mb": m})

        greeted = n_tp - 1 + n_mb - 1 + n_mb * ep
    else:
        for step in range(1, experts):
            hello(barrier, ex_dev(ex_id(step)))
        greeted = n_tp - 1 + experts - 1

    def tp_copy(src, dst, ssem, rsem, step):
        return pltpu.make_async_remote_copy(
            src_ref=src,
            dst_ref=dst,
            send_sem=ssem,
            recv_sem=rsem,
            device_id={"tp": tp_id(step)},
            device_id_type=MESH,
        )

    def arrival(dst, rsem):
        return pltpu.make_async_copy(dst, dst, rsem)

    def feed(p):
        for step in range(1, n_tp):
            tp_copy(
                q_all.at[p, 0], q_all.at[p, n_tp - step], q_ssem.at[0], q_rsem.at[p], step
            ).start()

    def row_copy(peer, block):
        return pltpu.make_async_remote_copy(
            src_ref=send.at[peer, block],
            dst_ref=arrived.at[me, block],
            send_sem=row_ssem.at[0],
            recv_sem=row_rsem.at[block],
            device_id=ex_dev(peer),
            device_id_type=MESH,
        )

    def ship_to(ep_index, block):
        for m in range(n_mb):
            row_copy(ep_index * n_mb + m, block).start()

    def ship_near(block):
        arrived[me, block] = send[me, block]
        for step in range(1, n_mb):
            row_copy(ep * n_mb + lax.rem(mb + step, n_mb), block).start()

    def ship(block):
        ship_near(block)
        for far in range(1, n_ep):
            pl.when(ep >= far)(functools.partial(ship_to, ep - far, block))
            pl.when(ep + far < n_ep)(functools.partial(ship_to, ep + far, block))
    small[3].wait()
    gain_all[tp] = moe_gain[...].reshape(1, d_loc)
    local[0].wait()
    pl.semaphore_wait(barrier, greeted)
    for step in range(1, n_tp):
        for src, dst, ssem, rsem in (
            (hid_all.at[tp], hid_all, hid_ssem, hid_rsem),
            (gain_all.at[tp], gain_all, gain_ssem, gain_rsem),
        ):
            tp_copy(src, dst.at[tp], ssem.at[0], rsem.at[0], step).start()
    if staged:
        for far in range(1, n_ep):

            @pl.when(ep >= far)
            def _():
                for m in range(n_mb):
                    hello(near_sem.at[far], {"ep": ep - far, "mb": m})

    for copy in small[:3]:
        copy.wait()
    kept = slots[...] < CAP
    target = jnp.where(kept, ids[...] * CAP + slots[...], -1)
    rows = experts * CAP
    iota = lax.broadcasted_iota(jnp.int32, (rows, tokens), 0)
    dispatch = jnp.zeros((rows, tokens), F32)
    for k in range(ids.shape[0]):
        dispatch = jnp.where(target[k : k + 1] == iota, 1.0, dispatch)
    dispatch = dispatch.astype(BF16)

    def pick(block):
        picked = jnp.dot(dispatch, hid_all[block], preferred_element_type=F32)
        send[:, block] = picked.reshape(experts, CAP, d_loc).astype(BF16)

    pick(tp)
    if staged:
        ship_near(tp)
        for far in range(1, n_ep):
            pl.when(ep >= far)(functools.partial(ship_to, ep - far, tp))
    else:
        ship(tp)
    for copy in q_loads:
        copy.wait()
    q_all[:, 0, :, 2 * lat : 2 * kvc] = jnp.concatenate([q_rope[:, 0], q_rope[:, 1]], -1)
    for t in range(AHEAD):
        feed(t)
    for copy in local[1:]:
        copy.start()
    for copy in kv_loads:
        copy.wait()
    blank = jnp.zeros((pairs, span_len, rope), BF16)
    k_pad[:, :span_len] = jnp.concatenate([k_rope[:, 0], blank], -1)
    k_pad[:, span_len:] = jnp.concatenate([blank, k_rope[:, 1]], -1)
    stat_all[...] = jnp.zeros(stat_all.shape, F32)
    aff = affinity[...]
    weight = route_scale * aff / jnp.sum(aff, 0, keepdims=True) * kept.astype(F32)
    combine = jnp.zeros((rows, tokens), F32)
    for k in range(ids.shape[0]):
        combine = jnp.where(target[k : k + 1] == iota, weight[k : k + 1], combine)
    combine = combine.T
    high = combine.astype(BF16)
    rest = combine - high.astype(F32)
    mid = rest.astype(BF16)
    low = (rest - mid.astype(F32)).astype(BF16)
    combine3 = jnp.concatenate([high, mid, low], 0)
    if staged:
        for far in range(1, n_ep):

            @pl.when(ep + far < n_ep)
            def _():
                pl.semaphore_wait(near_sem.at[far], n_mb)
                ship_to(ep + far, tp)
    arrival(hid_all.at[pl.ds(0, n_tp - 1)], hid_rsem.at[0]).wait()
    arrival(gain_all.at[pl.ds(0, n_tp - 1)], gain_rsem.at[0]).wait()
    for turn in range(1, n_tp):
        pick(tp_id(turn))
        ship(tp_id(turn))

    heads = queries.shape[2]
    both = n_tp * heads
    keys_two = 2 * span_len
    lane = lax.broadcasted_iota(jnp.int32, (both, keys_two), 1)
    first_token = lane < span_len
    stat_lane = lax.broadcasted_iota(jnp.int32, stat_send.shape[1:], 1)

    def attend(first, last):
        def body(p, carry):
            arrival(q_all.at[p, pl.ds(1, n_tp - 1)], q_rsem.at[p]).wait()

            @pl.when(p + AHEAD < pairs)
            def _():
                feed(p + AHEAD)

            q = q_all[p].reshape(both, q_all.shape[3])
            block = k_lat[p].reshape(keys_two, lat)
            crossed = lax.dot_general(
                jnp.concatenate([q[:, :lat], q[:, lat : 2 * lat]], 0),
                block,
                (((1,), (1,)), ((), ())),
                preferred_element_type=F32,
            )
            turned = lax.dot_general(
                q[:, 2 * lat :], k_pad[p], (((1,), (1,)), ((), ())), preferred_element_type=F32
            )
            scores = (jnp.where(first_token, crossed[:both], crossed[both:]) + turned) * score_scale
            done = tp * span_len
            stop = jnp.where(first_token, lengths[2 * p] - done, lengths[2 * p + 1] - done + span_len)
            live = lane < stop
            scores = jnp.where(live, scores, -1e30)
            mine = [first_token, jnp.logical_not(first_token)]
            tops = [
                jnp.max(jnp.where(m, scores, -1e30), -1, keepdims=True).astype(BF16).astype(F32)
                for m in mine
            ]
            prob = jnp.where(live, jnp.exp(scores - jnp.where(first_token, tops[0], tops[1])), 0.0)
            parts = [jnp.where(m, prob, 0.0) for m in mine]
            sums = [jnp.sum(part, -1, keepdims=True) for part in parts]
            out = jnp.dot(
                jnp.concatenate(parts, 0).astype(BF16), block, preferred_element_type=F32
            )
            for i in range(2):
                acc[2 * p + i] = out[i * both : i * both + heads]
                peaks[2 * p + i] = jnp.broadcast_to(tops[i][:heads], (heads, 128))
                masses[2 * p + i] = jnp.broadcast_to(sums[i][:heads], (heads, 128))
            for step in range(1, n_tp):
                stat = stat_all[step]
                for i in range(2):
                    start = step * heads
                    o_send[step, p, i] = out[i * both + start : i * both + start + heads].astype(BF16)
                    base = 3 * (2 * p + i)
                    mass = sums[i][start : start + heads]
                    high = mass.astype(BF16).astype(F32)
                    stat = jnp.where(stat_lane == base, tops[i][start : start + heads], stat)
                    stat = jnp.where(stat_lane == base + 1, high, stat)
                    stat = jnp.where(stat_lane == base + 2, mass - high, stat)
                stat_all[step] = stat
                tp_copy(
                    o_send.at[step, p], o_recv.at[n_tp - step, p], o_ssem.at[0], o_rsem.at[0], step
                ).start()
            return carry

        lax.fori_loop(first, last, body, 0)

    for copy in small[4:]:
        copy.wait()
    gain_row[...] = attn_gain[...].reshape(1, d_loc)
    stops = [pairs * n // 8 for n in STOPS]
    attend(0, stops[0])
    local[1].wait()
    local[2].wait()
    square = jnp.zeros((rows, 1), F32)
    for turn in range(n_tp):
        b = tp_id(turn)
        if turn == n_tp - 1:
            attend(stops[0], stops[1])
        arrival(arrived.at[pl.ds(0, experts - 1), b], row_rsem.at[b]).wait()
        wide = arrived[:, b].astype(F32).reshape(rows, d_loc)
        square = square + jnp.sum(wide * wide, -1, keepdims=True)
        block = (wide * gain_all[b]).astype(BF16)
        deep = pl.ds(pl.multiple_of(b * d_loc, d_loc & -d_loc), d_loc)
        gate = jnp.dot(block, wg[deep], preferred_element_type=F32)
        upper = jnp.dot(block, wu[deep], preferred_element_type=F32)
        if turn > 0:
            gate = gate + mid_units[0]
            upper = upper + mid_units[1]
        if turn < n_tp - 1:
            mid_units[0] = gate
            mid_units[1] = upper
    scale = lax.rsqrt(square / d_all + epsilon)
    gate = gate * scale
    upper = upper * scale
    units = (gate / (1.0 + jnp.exp(-gate)) * upper).astype(BF16)
    local[3].wait()
    aligned = d_loc % 128 == 0
    width = piece_width(d_loc, d_all)
    if aligned:
        pieces = [(tp_id(turn) * d_loc, d_loc) for turn in range(1, n_tp)]
        pieces += [(tp * d_loc + c, width) for c in range(0, d_loc, width)]
    else:
        middle = d_all // width // 2 * width
        pieces = [(0, middle), (middle, d_all - middle)]

    def columns(start, size):
        return pl.ds(pl.multiple_of(start, 128), size)

    for h, (first, size) in enumerate(pieces):
        for c in range(0, size, width):
            part = jnp.dot(units, wd[:, columns(first + c, width)], preferred_element_type=F32)
            ret_send[:, :, columns(first + c, width)] = part.reshape(
                experts, CAP, width
            ).astype(BF16)
            for step in range(1, experts):
                peer = ex_id(step)
                pltpu.make_async_remote_copy(
                    src_ref=ret_send.at[peer, :, columns(first + c, width)],
                    dst_ref=ret.at[me, :, columns(first + c, width)],
                    send_sem=ret_ssem.at[0],
                    recv_sem=ret_rsem.at[h],
                    device_id=ex_dev(peer),
                    device_id_type=MESH,
                ).start()
    ret[me] = ret_send[me]

    def exchange(step):
        tp_copy(
            rs_send.at[step], rs_recv.at[n_tp - step], rs_ssem.at[0], rs_rsem.at[0], step
        ).start()

    def gather(h):
        first, size = pieces[h]
        arrival(
            ret.at[pl.ds(0, experts - 1), :, columns(first, size)], ret_rsem.at[h]
        ).wait()

    def mixed(start):
        block = ret[:, :, columns(start, width)].astype(F32)
        block = block.reshape(rows, width).astype(BF16)
        part = jnp.dot(combine3, block, preferred_element_type=F32)
        return part[:tokens] + (part[tokens : 2 * tokens] + part[2 * tokens : 3 * tokens])

    def send_stats():
        stat_send[...] = stat_all[...].astype(BF16)
        for step in range(1, n_tp):
            tp_copy(
                stat_send.at[step],
                stat_recv.at[n_tp - step],
                stat_ssem.at[0],
                stat_rsem.at[0],
                step,
            ).start()

    def renew(start, size, moe):
        span = pl.ds(start, size)
        fresh = (hid_all[tp, :, span].astype(F32) + moe).astype(BF16)
        next_out[:, span] = fresh
        fresh = fresh.astype(F32)
        scaled = (fresh * gain_row[...][:, start : start + size]).astype(BF16)
        part = lax.dot_general(
            scaled, wk[:, span], (((1,), (1,)), ((), ())), preferred_element_type=F32
        )
        return jnp.sum(fresh * fresh, -1, keepdims=True), part

    def others(start, size):
        total = rs_recv[1, :, pl.ds(start, size)].astype(F32)
        for step in range(2, n_tp):
            total = total + rs_recv[step, :, pl.ds(start, size)].astype(F32)
        return total
    attend(stops[1], stops[2])
    if aligned:
        for turn in range(1, n_tp):
            gather(turn - 1)
            for c in range(0, d_loc, width):
                rs_send[turn, :, c : c + width] = mixed(pieces[turn - 1][0] + c).astype(BF16)
            exchange(turn)
        attend(stops[2], stops[3])
        if stops[3] == pairs:
            send_stats()
        local[4].wait()
        square = jnp.zeros((tokens, 1), F32)
        for i, c in enumerate(range(0, d_loc, width)):
            gather(n_tp - 1 + i)
            part = mixed(tp * d_loc + c)
            if i == 0:
                arrival(rs_recv.at[pl.ds(1, n_tp - 1)], rs_rsem.at[0]).wait()
            more, part = renew(c, width, part + others(c, width))
            square = square + more
            if i > 0:
                part = part + mid_key[...]
            if c + width < d_loc:
                mid_key[...] = part
    else:
        for h in range(2):
            gather(h)
            first, size = pieces[h]
            for c in range(0, size, width):
                tsum[:, columns(first + c, width)] = mixed(first + c)
            if h == 0:
                attend(stops[2], stops[3])
        for p in range(n_tp):
            rs_send[lax.rem(p - tp + n_tp, n_tp)] = tsum[:, p * d_loc : (p + 1) * d_loc].astype(BF16)
        for step in range(1, n_tp):
            exchange(step)
        if stops[3] == pairs:
            send_stats()
        local[4].wait()
        arrival(rs_recv.at[pl.ds(1, n_tp - 1)], rs_rsem.at[0]).wait()
        square, part = renew(0, d_loc, rs_send[0].astype(F32) + others(0, d_loc))
    kvp = up(kvc + 3, 128)
    tail = kvp - kvc
    key_send[:, :kvc] = part.astype(BF16)
    key_send[:, kvc:kvp] = split3(square, tail)
    for step in range(1, n_tp):
        tp_copy(key_send, key_recv.at[tp], key_ssem.at[0], key_rsem.at[0], step).start()
    key_recv[tp] = key_send[...]
    if stops[3] < pairs:
        attend(stops[3], pairs)
        send_stats()
    half = (kvc - lat) // 2
    column = lax.broadcasted_iota(jnp.int32, (tokens, 2 * half), 1)
    pair = jnp.where(column < half, column, column - half).astype(F32)
    freq = jnp.exp(pair * (-9.210340371976184 / half))
    row_id = lax.broadcasted_iota(jnp.int32, (tokens, 2 * half), 0)
    place = jnp.zeros((tokens, 2 * half), F32)
    for t in range(tokens):
        place = jnp.where(row_id == t, lengths[t].astype(F32), place)
    angle = place * freq
    cos_table = jnp.cos(angle)
    sin_table = jnp.where(column < half, -1.0, 1.0) * jnp.sin(angle)
    arrival(o_recv.at[pl.ds(1, n_tp - 1)], o_rsem.at[0]).wait()
    arrival(stat_recv.at[pl.ds(1, n_tp - 1)], stat_rsem.at[0]).wait()
    for t in range(tokens):
        for step in range(1, n_tp):
            stat = stat_recv[step].astype(F32)
            far_top = jnp.sum(jnp.where(stat_lane == 3 * t, stat, 0.0), -1, keepdims=True)
            far_mass = jnp.where(stat_lane == 3 * t + 1, stat, 0.0)
            far_mass = far_mass + jnp.where(stat_lane == 3 * t + 2, stat, 0.0)
            far_mass = jnp.sum(far_mass, -1, keepdims=True)
            near_top = peaks[t]
            top = jnp.maximum(near_top, far_top)
            near_factor = jnp.exp(near_top - top)
            far_factor = jnp.exp(far_top - top)
            peaks[t] = top
            masses[t] = masses[t] * near_factor + far_mass * far_factor
            for c in range(0, lat, 128):
                far = o_recv[step, t // 2, t % 2, :, c : c + 128].astype(F32) * far_factor
                acc[t, :, c : c + 128] = acc[t, :, c : c + 128] * near_factor + far
    arrival(key_recv.at[pl.ds(0, n_tp - 1)], key_rsem.at[0]).wait()
    total = key_recv[0].astype(F32)
    for p in range(1, n_tp):
        total = total + key_recv[p].astype(F32)
    rows_all = tokens * heads
    turn = total[:, lat:kvc]
    swapped = jnp.concatenate([turn[:, half:], turn[:, :half]], 1)
    turn = turn * cos_table + swapped * sin_table
    gained = total[:, :lat] * kv_gain[...]
    raw = gained.astype(BF16)
    blank = jnp.zeros((tokens, rope), F32)
    turns = [jnp.concatenate(p, 1).astype(BF16) for p in ((turn, blank), (blank, turn))]

    def against(columns, key):
        return lax.dot_general(
            q_all[:, 0, :, columns].reshape(pairs * heads, -1),
            key,
            (((1,), (1,)), ((), ())),
            preferred_element_type=F32,
        )

    flat = [against(slice(i * lat, (i + 1) * lat), raw) for i in range(2)]
    curled = [against(slice(2 * lat, 2 * kvc), turns[i]) for i in range(2)]
    square = jnp.sum(total[:, kvc:], -1, keepdims=True)
    spread = jnp.mean(total[:, :lat] * total[:, :lat], -1, keepdims=True)
    shrink = lax.rsqrt(square / d_all + epsilon)
    level = shrink * lax.rsqrt(spread * shrink * shrink + epsilon)
    keys[...] = (gained * level).astype(BF16)
    eye = lax.broadcasted_iota(jnp.int32, (tokens, tokens), 0) == lax.broadcasted_iota(
        jnp.int32, (tokens, tokens), 1
    )
    level = jnp.sum(jnp.where(eye, level, 0.0), 0, keepdims=True)
    shrink = jnp.sum(jnp.where(eye, shrink, 0.0), 0, keepdims=True)
    halves = [flat[i] * level + curled[i] * shrink for i in range(2)]
    own = jnp.concatenate(
        [halves[i][p * heads : (p + 1) * heads] for p in range(pairs) for i in range(2)], 0
    )
    owner = lax.broadcasted_iota(jnp.int32, (rows_all, tokens), 0) // heads
    mine = owner == lax.broadcasted_iota(jnp.int32, (rows_all, tokens), 1)
    own = jnp.sum(jnp.where(mine, own, 0.0), -1, keepdims=True) * score_scale
    own = jnp.broadcast_to(own, (rows_all, 128))
    peak = peaks[...].reshape(rows_all, 128)
    top = jnp.maximum(peak, own)
    factor = jnp.exp(peak - top)
    own_prob = jnp.exp(own - top)
    inverse = 1.0 / (masses[...].reshape(rows_all, 128) * factor + own_prob)
    old_part[...] = (factor * inverse).reshape(tokens, heads, 128)
    own_part[...] = (own_prob.astype(BF16).astype(F32) * inverse).reshape(tokens, heads, 128)
    for t in range(tokens):
        for c in range(0, lat, 128):
            value = acc[t, :, c : c + 128] * old_part[t]
            key = keys[t : t + 1, c : c + 128].astype(F32)
            latent_out[t, :, c : c + 128] = (value + own_part[t] * key).astype(BF16)
    for sent, sem in (
        (send.at[pl.ds(0, experts - 1)], row_ssem),
        (ret_send.at[pl.ds(0, experts - 1)], ret_ssem),
        (hid_all.at[pl.ds(0, n_tp - 1)], hid_ssem),
        (gain_all.at[pl.ds(0, n_tp - 1)], gain_ssem),
        (rs_send.at[pl.ds(1, n_tp - 1)], rs_ssem),
        (key_recv.at[pl.ds(0, n_tp - 1)], key_ssem),
        (q_all.at[:, pl.ds(0, n_tp - 1)], q_ssem),
        (o_send.at[pl.ds(1, n_tp - 1)], o_ssem),
        (stat_send.at[pl.ds(1, n_tp - 1)], stat_ssem),
    ):
        arrival(sent, sem.at[0]).wait()


def put_out(hidden_in, latent_in, hidden_out, latent_out, sem):
    step = latent_in.shape[0] // 4
    copies = [pltpu.make_async_copy(hidden_in, hidden_out, sem.at[4])]
    for i in range(4):
        part = pl.ds(i * step, step)
        copies.append(
            pltpu.make_async_copy(latent_in.at[part], latent_out.at[part], sem.at[i])
        )
    for copy in copies:
        copy.start()
    for copy in copies:
        copy.wait()


def solution(mesh):
    n_tp, n_ep, n_mb = mesh.shape["tp"], mesh.shape["ep"], mesh.shape["mb"]
    experts = n_ep * n_mb

    def local(
        hidden,
        moe_gain,
        expert_ids,
        slots,
        affinity,
        w_gate,
        w_up,
        w_down,
        attn_gain,
        w_dkv,
        kv_gain,
        queries,
        cache,
        lengths,
    ):
        tokens, d_loc = hidden.shape
        d_all = d_loc * n_tp
        heads, kvc = queries.shape[1:]
        span = cache.shape[1]
        lat = kv_gain.shape[0]
        pairs = tokens // 2
        hid_dim = w_gate.shape[2]
        top = expert_ids.shape[1]
        wide = up(kvc + 3, 128)
        returns = n_tp - 1 + d_loc // piece_width(d_loc, d_all) if d_loc % 128 == 0 else 2
        any_space = pl.BlockSpec(memory_space=pl.ANY)
        vmem = pl.BlockSpec(memory_space=pltpu.VMEM)
        dma = pltpu.SemaphoreType.DMA
        results = pl.pallas_call(
            functools.partial(kernel, n_tp, n_ep, n_mb),
            out_shape=(
                pltpu.VMEM((tokens, d_loc), BF16),
                pltpu.VMEM((tokens, heads, lat), BF16),
            ),
            in_specs=[any_space] * 14,
            out_specs=(vmem, vmem),
            scratch_shapes=[
                pltpu.VMEM((n_tp, tokens, d_loc), BF16),
                pltpu.VMEM((n_tp, 1, d_loc), F32),
                pltpu.VMEM((experts, n_tp, CAP, d_loc), BF16),
                pltpu.VMEM((experts, n_tp, CAP, d_loc), BF16),
                pltpu.VMEM((d_all, hid_dim), BF16),
                pltpu.VMEM((d_all, hid_dim), BF16),
                pltpu.VMEM((hid_dim, d_all), BF16),
                pltpu.VMEM((kvc, d_loc), BF16),
                pltpu.VMEM((experts, CAP, d_all), BF16),
                pltpu.VMEM((experts, CAP, d_all), BF16),
                pltpu.VMEM((tokens, d_all), F32),
                pltpu.VMEM((n_tp, tokens, d_loc), BF16),
                pltpu.VMEM((n_tp, tokens, d_loc), BF16),
                pltpu.VMEM((tokens, wide), BF16),
                pltpu.VMEM((n_tp, tokens, wide), BF16),
                pltpu.VMEM((pairs, n_tp, heads, 2 * kvc), BF16),
                pltpu.VMEM((pairs, 2, heads, kvc - lat), BF16),
                pltpu.VMEM((pairs, 2, span, lat), BF16),
                pltpu.VMEM((pairs, 2, span, kvc - lat), BF16),
                pltpu.VMEM((pairs, 2 * span, 2 * (kvc - lat)), BF16),
                pltpu.VMEM((n_tp, pairs, 2, heads, lat), BF16),
                pltpu.VMEM((n_tp, pairs, 2, heads, lat), BF16),
                pltpu.VMEM((n_tp, heads, up(3 * tokens, 128)), F32),
                pltpu.VMEM((n_tp, heads, up(3 * tokens, 128)), BF16),
                pltpu.VMEM((n_tp, heads, up(3 * tokens, 128)), BF16),
                pltpu.VMEM((2, experts * CAP, hid_dim), F32),
                pltpu.VMEM((tokens, kvc), F32),
                pltpu.VMEM((1, d_loc), F32),
                pltpu.VMEM((tokens, heads, lat), F32),
                pltpu.VMEM((tokens, heads, 128), F32),
                pltpu.VMEM((tokens, heads, 128), F32),
                pltpu.VMEM((tokens, lat), BF16),
                pltpu.VMEM((tokens, heads, 128), F32),
                pltpu.VMEM((tokens, heads, 128), F32),
                pltpu.VMEM((d_loc,), F32),
                pltpu.VMEM((top, tokens), jnp.int32),
                pltpu.VMEM((top, tokens), jnp.int32),
                pltpu.VMEM((top, tokens), F32),
                pltpu.VMEM((d_loc,), F32),
                pltpu.VMEM((1, lat), F32),
                pltpu.SMEM((tokens,), jnp.int32),
                dma((7,)),
                pltpu.SemaphoreType.REGULAR((n_ep,)),
                dma((5,)),
                dma((3,)),
                dma((2,)),
                dma((1,)),
                dma((1,)),
                dma((1,)),
                dma((1,)),
                dma((1,)),
                dma((pairs,)),
                dma((1,)),
                dma((1,)),
                dma((1,)),
                dma((1,)),
                dma((1,)),
                dma((n_tp,)),
                dma((1,)),
                dma((returns,)),
                dma((1,)),
                dma((1,)),
                dma((1,)),
                dma((1,)),
            ],
            compiler_params=pltpu.CompilerParams(
                collective_id=0, has_side_effects=True, vmem_limit_bytes=60 * 1024 * 1024
            ),
        )(
            hidden,
            moe_gain,
            expert_ids.T,
            slots.T,
            affinity.T,
            w_gate,
            w_up,
            w_down,
            attn_gain,
            w_dkv.T,
            kv_gain[None],
            queries.reshape(pairs, 2, heads, kvc),
            cache.reshape(pairs, 2, span, kvc),
            lengths,
        )
        return pl.pallas_call(
            put_out,
            out_shape=(
                jax.ShapeDtypeStruct((tokens, d_loc), BF16),
                jax.ShapeDtypeStruct((tokens, heads, lat), BF16),
            ),
            in_specs=[vmem, vmem],
            out_specs=(any_space, any_space),
            scratch_shapes=[dma((5,))],
        )(*[pltpu.with_memory_space_constraint(r, pltpu.VMEM) for r in results])

    return jax.shard_map(
        local,
        mesh=mesh,
        in_specs=(
            P(("grp", "ep", "mb"), "tp"),
            P("tp"),
            P(("grp", "ep", "mb"), None),
            P(("grp", "ep", "mb"), None),
            P(("grp", "ep", "mb"), None),
            P(("ep", "mb"), None, "tp"),
            P(("ep", "mb"), None, "tp"),
            P(("ep", "mb"), "tp", None),
            P("tp"),
            P("tp", None),
            P(),
            P(("grp", "ep", "mb"), "tp", None),
            P(("grp", "ep", "mb"), "tp", None),
            P(("grp", "ep", "mb")),
        ),
        out_specs=(P(("grp", "ep", "mb"), "tp"), P(("grp", "ep", "mb"), "tp", None)),
        check_vma=False,
    )
```
